32 devices in a mesh: lat: 4 (over y, x), lon: 8 (over z, core).
Axes of the slice: x: 2, y: 2, z: 4, core: 2. Of those that a mesh axis runs over, the one named last changes fastest.
Arguments:
- state: float32 [64, 384, 1104], P('lat', 'lon'), may hold values from -6 to 6
- background: float32 [64, 384, 1104], P('lat', 'lon'), may hold values from -6 to 6
- inv_background: float32 [1104], replicated, may hold values from 0.1 to 1
- w_embed: bfloat16 [1104, 256], replicated, may hold values from -0.1875 to 0.1875
- norm_gain: float32 [2, 2, 256], replicated, may hold values from 0.25 to 1.75
- w_qkv: bfloat16 [2, 256, 768], replicated, may hold values from -0.375 to 0.375
- w_proj: bfloat16 [2, 256, 256], replicated, may hold values from -0.375 to 0.375
- head_scale: float32 [2, 8], replicated, may hold values from 2 to 12
- w_up: bfloat16 [2, 256, 1024], replicated, may hold values from -0.375 to 0.375
- w_down: bfloat16 [2, 1024, 256], replicated, may hold values from -0.1875 to 0.1875
- w_head: bfloat16 [256, 1104], replicated, may hold values from -0.375 to 0.375
- w_obs1: float32 [69, 256], replicated, may hold values from -0.75 to 0.75
- w_obs2: float32 [256, 256], replicated, may hold values from -0.375 to 0.375
- r_inverse: float32 [256, 256], replicated, as said below
- obs_values: float32 [65536, 256], P(('lat', 'lon')), may hold values from -6 to 6
- obs_owner: int32 [65536, 1], P(('lat', 'lon')), may hold values from 0 to 31; in each aligned block of 2048 rows (0 to 2047, 2048 to 4095, ...) at most 128 rows name the same one
- obs_point: int32 [65536], P(('lat', 'lon')), may hold values from 0 to 12287
- obs_count: int32 [32], P(('lat', 'lon')), may hold values from 1024 to 2048, as said below
Outputs:
- gradient: float32 [64, 384, 1104], P('lat', 'lon')
The draws below stay inside these ranges and needn't reach their ends.
Inputs may be any that keep to these rules, and one draw needn't show every extreme that they name: `r_inverse`: Symmetric, with a positive diagonal larger than the sum of magnitudes of the rest of its row. `obs_owner`: among the slots of one device, at most 128 name the same owner, and in some device exactly 128 do. `obs_count`: some device has all its slots live.
All inputs are finite; a program needn't handle non-finite values.
Results may differ from the reference program's by a relative error of at most 0.018.
Values may be sent and summed in bfloat16 or wider, within the bound.
No kernel may reach another device: no remote copies, remote signals or barrier semaphores. Data moves between devices by JAX's collectives and lax.ppermute only.
A program may use at most 192 MiB of HBM per device.

```python
import math
import jax
import jax.numpy as jnp
import numpy as np
from jax import lax

D = 256
HEADS = 8
FFN = 1024
VARS = 69
PIX = 16
CHAN = 256
HID_OBS = 256
WIN = 8
TLAT = 16
TLON = 48
OBS_DEV = 2048
SHIFT = 4
PV = 1104
NLAT = 64
NLON = 384
POINTS = 12288
OBS = 65536
CAP = 128
N_LAT = 4
N_LON = 8
DEVICES = 32


def draw_r_inverse(key, part):
    first, second = jax.random.split(jax.random.fold_in(key, 11))
    raw = 0.002 * jax.random.normal(first, (CHAN, CHAN), jnp.float32)
    sym = 0.5 * (raw + raw.T)
    extra = jnp.exp(jax.random.uniform(second, (CHAN,), jnp.float32, jnp.log(0.1), jnp.log(0.4)))
    off_part = sym - jnp.diag(jnp.diag(sym))
    return off_part + jnp.diag(jnp.sum(jnp.abs(off_part), 1) + extra)


def draw_obs_count(key, part):
    first, second = jax.random.split(jax.random.fold_in(key, 23))
    counts = jax.random.randint(first, (DEVICES,), OBS_DEV // 2, OBS_DEV + 1)
    chosen = jax.random.randint(second, (), 0, DEVICES)
    return jnp.where(jnp.arange(DEVICES) == chosen, OBS_DEV, counts).astype(jnp.int32)


def set_ends(values, key, smallest, top_value):
    shape = values.shape
    spot = [jax.random.randint(jax.random.fold_in(key, axis), (), 0, shape[axis]) for axis in range(len(shape))]
    values = values.at[tuple(spot)].set(smallest)
    longest = shape.index(max(shape))
    spot[longest] = (spot[longest] + 1) % shape[longest]
    return values.at[tuple(spot)].set(top_value)


def levels(stream_key, extent, cuts, smallest, top_value):
    def one(dim, shards_of):
        steps = jax.random.uniform(jax.random.fold_in(jax.random.fold_in(stream_key, 6), dim), (shards_of,), jnp.float32, smallest / len(cuts), top_value / len(cuts))
        return jnp.repeat(jnp.exp(steps), extent[dim] // shards_of).reshape((-1,) + (1,) * (len(extent) - dim - 1))

    loudness = one(*cuts[0])
    for cut in cuts[1:]:
        loudness = loudness * one(*cut)
    return loudness


def routed_block(key, own, number, rows, count, top, reach, slope):
    sequence = jax.random.permutation(key, count)
    packed, ordinary = shares(count, rows * top, reach, slope, True), shares(count, rows * top, reach, slope, False)
    places = jnp.arange(count)

    def named(tallies, rotation):
        used = int((tallies > 0).sum())
        fixed = max(1, used // 4)
        moved = fixed + (places - fixed + rotation * (used - fixed)) % max(1, count - fixed)
        return jnp.zeros((count,), jnp.int32).at[sequence[jnp.where(places < fixed, places, moved)]].set(jnp.asarray(tallies, jnp.int32))

    tallies = jnp.where(number % 4 == 0, named(packed, number // 4), named(ordinary, number - number // 4 - 1))
    mixed = jax.random.permutation(jax.random.fold_in(own, 3), count)
    donor, taker = mixed[0:count // 2 * 2:2], mixed[1:count // 2 * 2:2]
    room = jnp.minimum(tallies[donor] - 1, reach - tallies[taker]) // 2
    room = jnp.where((donor == sequence[0]) | (taker == sequence[0]) | (tallies[taker] == 0), 0, jnp.maximum(room, 0))
    moved = jax.random.randint(jax.random.fold_in(own, 4), (count // 2,), 0, 1 << 20) % (room + 1)
    tallies = tallies.at[donor].add(-moved).at[taker].add(moved)
    labels = jnp.searchsorted(jnp.cumsum(tallies), jnp.arange(rows * top), side="right").astype(jnp.int32)
    table = labels.reshape(top, rows).T
    table = table[jax.random.permutation(jax.random.fold_in(own, 1), rows)]
    rotation = jax.random.randint(jax.random.fold_in(own, 2), (rows, 1), 0, top)
    return jnp.take_along_axis(table, (jnp.arange(top)[None, :] + rotation) % top, axis=1)


def shares(amount, total, bound, lean, full):
    weights = [(1 << 20) // math.isqrt(standing ** lean) + 1 for standing in range(1, amount + 1)]
    largest = bound if full else min(bound, max(-(-total // amount), total * weights[0] // sum(weights)))
    least = 1 if total - largest >= amount - 1 else 0
    holding, rest = [largest] + [least] * (amount - 1), total - largest - least * (amount - 1)
    while rest > 0:
        movable = [i for i in range(1, amount) if holding[i] < largest] or [i for i in range(1, amount) if holding[i] < bound]
        pool, remaining = sum([weights[i] for i in movable]), rest
        for i in movable:
            more = min(bound - holding[i], max(1, remaining * weights[i] // pool), rest)
            holding[i] = holding[i] + more
            rest = rest - more
    return np.array(holding)


def bell_draw(stream_key, extent, scale, limit, cuts=(), held_as=jnp.bfloat16):
    values = scale * jax.random.normal(stream_key, extent, jnp.float32)
    if cuts:
        values = values * levels(stream_key, extent, cuts, -0.22, 0.18)
    return jnp.clip(values, -limit, limit).astype(held_as)


def setup_inputs(seed: int = 0) -> dict:
    seeds = jax.random.split(jax.random.key(seed), 19)
    state = bell_draw(seeds[0], (NLAT, NLON, PV), 1.0, 6.0, ((0, 4), (1, 8)), jnp.float32)
    background = bell_draw(seeds[1], (NLAT, NLON, PV), 1.0, 6.0, ((0, 4), (1, 8)), jnp.float32)
    inv_background = jnp.clip(jnp.exp(jax.random.uniform(seeds[2], (PV,), jnp.float32, math.log(0.1), math.log(1.0))), 0.1, 1.0)
    w_embed = bell_draw(seeds[3], (PV, D), PV ** -0.5, 0.1875)
    norm_gain = jnp.clip(1.0 + 0.15 * jax.random.normal(seeds[4], (2, 2, D), jnp.float32), 0.25, 1.75)
    w_qkv = bell_draw(seeds[5], (2, D, 3 * D), D ** -0.5, 0.375)
    w_proj = bell_draw(seeds[6], (2, D, D), D ** -0.5, 0.375)
    head_scale = jnp.clip(jnp.exp(jax.random.uniform(seeds[7], (2, HEADS), jnp.float32, math.log(2.0), math.log(12.0))), 2.0, 12.0)
    w_up = bell_draw(seeds[8], (2, D, FFN), D ** -0.5, 0.375)
    w_down = bell_draw(seeds[9], (2, FFN, D), FFN ** -0.5, 0.1875)
    w_head = bell_draw(seeds[10], (D, PV), D ** -0.5, 0.375)
    w_obs1 = bell_draw(seeds[11], (VARS, HID_OBS), VARS ** -0.5, 0.75, (), jnp.float32)
    w_obs2 = bell_draw(seeds[12], (HID_OBS, CHAN), HID_OBS ** -0.5, 0.375, (), jnp.float32)
    r_inverse = draw_r_inverse(jax.random.fold_in(seeds[18], 71), 0)
    obs_values = bell_draw(seeds[14], (OBS, CHAN), 1.0, 6.0, ((0, 32),), jnp.float32)
    obs_owner_keys = jax.random.split(jax.random.fold_in(seeds[15], 1), OBS // OBS_DEV)
    obs_owner_turns = jax.random.permutation(jax.random.fold_in(seeds[15], 3), OBS // OBS_DEV)
    obs_owner = jax.vmap(lambda own, number: routed_block(jax.random.fold_in(seeds[15], 2), own, number, OBS_DEV, DEVICES, 1, CAP, 2))(obs_owner_keys, obs_owner_turns).reshape((OBS, 1))
    obs_point = set_ends(jax.random.randint(seeds[16], (OBS,), 0, POINTS), jax.random.fold_in(seeds[16], 1), 0, POINTS - 1).astype(jnp.int32)
    obs_count = draw_obs_count(jax.random.fold_in(seeds[18], 71), 0)
    return {"state": state, "background": background, "inv_background": inv_background, "w_embed": w_embed, "norm_gain": norm_gain, "w_qkv": w_qkv, "w_proj": w_proj, "head_scale": head_scale, "w_up": w_up, "w_down": w_down, "w_head": w_head, "w_obs1": w_obs1, "w_obs2": w_obs2, "r_inverse": r_inverse, "obs_values": obs_values, "obs_owner": obs_owner, "obs_point": obs_point, "obs_count": obs_count}


EPS = 1e-05

def layer_norm(hidden, gain):
    mean = lax.optimization_barrier(jnp.mean(hidden, -1, keepdims=True))
    centred = hidden - mean
    spread = lax.optimization_barrier(jnp.mean(centred * centred, -1, keepdims=True))
    return (centred * lax.rsqrt(spread + EPS) * gain).astype(jnp.bfloat16)

def windows(field, width_win):
    rows, cols, width = field.shape
    field = field.reshape(rows // width_win, width_win, cols // width_win, width_win, width)
    return field.transpose(0, 2, 1, 3, 4).reshape(-1, width_win * width_win, width)

def unwindows(field, rows, cols, width_win):
    width = field.shape[-1]
    field = field.reshape(rows // width_win, cols // width_win, width_win, width_win, width)
    return field.transpose(0, 2, 1, 3, 4).reshape(rows, cols, width)

def attention(normed, w_qkv, w_proj, scales, row_start, total_rows, offset):
    rows, cols, width = normed.shape
    size = width // HEADS
    qkv = jnp.dot(normed.reshape(-1, width), w_qkv, preferred_element_type=jnp.float32).astype(jnp.bfloat16)
    qkv = windows(qkv.reshape(rows, cols, 3 * width), WIN)
    count = qkv.shape[0]
    query = qkv[:, :, :width].reshape(count, WIN * WIN, HEADS, size).astype(jnp.float32)
    keys = qkv[:, :, width:2 * width].reshape(count, WIN * WIN, HEADS, size).astype(jnp.float32)
    values = qkv[:, :, 2 * width:].reshape(count, WIN * WIN, HEADS, size).astype(jnp.float32)
    query = (query * lax.rsqrt(lax.optimization_barrier(jnp.sum(query * query, -1, keepdims=True)) + 1.0)).astype(jnp.bfloat16)
    keys = (keys * lax.rsqrt(lax.optimization_barrier(jnp.sum(keys * keys, -1, keepdims=True)) + 1.0)).astype(jnp.bfloat16)
    scores = jnp.einsum('wqhd,wkhd->whqk', query.astype(jnp.float32), keys.astype(jnp.float32))
    scores = scores * scales[None, :, None, None]
    expo = jnp.exp(scores)
    if offset > 0:
        row_index = row_start + jnp.arange(rows, dtype=jnp.int32)
        side = (row_index >= total_rows - offset).astype(jnp.float32)
        side = windows(jnp.broadcast_to(side[:, None, None], (rows, cols, 1)), WIN)[:, :, 0]
        allowed = (side[:, :, None] == side[:, None, :]).astype(jnp.float32)
        expo = expo * allowed[:, None, :, :]
    probs = (expo / lax.optimization_barrier(jnp.sum(expo, -1, keepdims=True))).astype(jnp.bfloat16)
    mixed = jnp.einsum('whqk,wkhd->wqhd', probs.astype(jnp.float32), values).astype(jnp.bfloat16)
    mixed = unwindows(mixed.reshape(count, WIN * WIN, width), rows, cols, WIN)
    out = jnp.dot(mixed.reshape(-1, width), w_proj, preferred_element_type=jnp.float32)
    return out.astype(jnp.bfloat16).reshape(rows, cols, width)

def mlp_residual(hidden, gain, w_up, w_down):
    width = hidden.shape[-1]
    normed = layer_norm(hidden, gain).reshape(-1, width)
    inner = jax.nn.gelu(jnp.dot(normed, w_up, preferred_element_type=jnp.float32)).astype(jnp.bfloat16)
    return hidden + jnp.dot(inner, w_down, preferred_element_type=jnp.float32).reshape(hidden.shape)

def propagate(state, w_embed, norm_gain, w_qkv, w_proj, head_scale, w_up, w_down, w_head):
    rows, cols, values = state.shape
    hidden = jnp.dot(state.astype(jnp.bfloat16).reshape(-1, values), w_embed, preferred_element_type=jnp.float32)
    hidden = hidden.reshape(rows, cols, -1)
    hidden = hidden + attention(layer_norm(hidden, norm_gain[0, 0]), w_qkv[0], w_proj[0], head_scale[0], 0, rows, 0)
    hidden = mlp_residual(hidden, norm_gain[0, 1], w_up[0], w_down[0])
    normed = layer_norm(hidden, norm_gain[1, 0])
    rolled = jnp.roll(normed, (-SHIFT, -SHIFT), (0, 1))
    answer = attention(rolled, w_qkv[1], w_proj[1], head_scale[1], 0, rows, SHIFT)
    hidden = hidden + jnp.roll(answer, (SHIFT, SHIFT), (0, 1))
    hidden = mlp_residual(hidden, norm_gain[1, 1], w_up[1], w_down[1])
    lifted = jnp.dot(hidden.astype(jnp.bfloat16).reshape(rows * cols, -1), w_head, preferred_element_type=jnp.float32)
    return state + lifted.reshape(state.shape)

def radiance_cost(columns, observed, live, w_obs1, w_obs2, r_inverse):
    best = lax.Precision.HIGHEST
    inner = jnp.tanh(jnp.dot(columns, w_obs1, precision=best))
    innovation = (jnp.dot(inner, w_obs2, precision=best) - observed) * live[:, None]
    return 0.5 * jnp.sum(innovation * jnp.dot(innovation, r_inverse, precision=best))

def reference(state, background, inv_background, w_embed, norm_gain, w_qkv, w_proj, head_scale, w_up, w_down, w_head, w_obs1, w_obs2, r_inverse, obs_values, obs_owner, obs_point, obs_count):

    def cost(initial):
        moved = propagate(initial, w_embed, norm_gain, w_qkv, w_proj, head_scale, w_up, w_down, w_head)
        grid = moved.reshape(N_LAT, TLAT, N_LON, TLON, PIX, VARS).transpose(0, 2, 1, 3, 4, 5)
        grid = grid.reshape(N_LAT * N_LON, TLAT * TLON * PIX, VARS)
        columns = grid[obs_owner[:, 0].astype(jnp.int32), obs_point.astype(jnp.int32)]
        slot_index = jnp.arange(OBS_DEV * N_LAT * N_LON, dtype=jnp.int32) % OBS_DEV
        live = (slot_index < jnp.repeat(obs_count, OBS_DEV)).astype(jnp.float32)
        differ = initial - background
        prior = 0.5 * jnp.sum(inv_background * differ * differ)
        return prior + radiance_cost(columns, obs_values, live, w_obs1, w_obs2, r_inverse)
    value, pull = jax.vjp(cost, state)
    return pull(jnp.ones_like(value))[0]
```

```python
import functools

import jax
import jax.numpy as jnp
from jax import lax
from jax.experimental import pallas as pl
from jax.experimental.pallas import tpu as pltpu
from jax.sharding import PartitionSpec as P

HEADS = 8
VARS = 69
PIX = 16
WIN = 8
SHIFT = 4
LANES = 128
EXTRA = 8
EPS = 1e-05
BF = jnp.bfloat16
F32 = jnp.float32
SQRT_2_OVER_PI = 0.7978845608028654
CUBIC = 0.044715

VMEM = pl.BlockSpec(memory_space=pltpu.VMEM)
SMEM = pl.BlockSpec(memory_space=pltpu.SMEM)


def nn(a, b):
    return lax.dot_general(a, b, (((1,), (0,)), ((), ())), preferred_element_type=F32)


def nt(a, b):
    return lax.dot_general(a, b, (((1,), (1,)), ((), ())), preferred_element_type=F32)


def tn(a, b):
    return lax.dot_general(a, b, (((0,), (0,)), ((), ())), preferred_element_type=F32)


def norm_parts(h):
    mean = jnp.mean(h, -1, keepdims=True)
    centred = h - mean
    spread = jnp.mean(centred * centred, -1, keepdims=True)
    rstd = lax.rsqrt(spread + EPS)
    return centred * rstd, rstd


def norm(h, gain):
    return (norm_parts(h)[0] * gain).astype(BF)


def norm_back(h, gain, cotangent):
    xhat, rstd = norm_parts(h)
    scaled = cotangent * gain
    m1 = jnp.mean(scaled, -1, keepdims=True)
    m2 = jnp.mean(scaled * xhat, -1, keepdims=True)
    return rstd * (scaled - m1 - xhat * m2)


def gelu_parts(u):
    square = u * u
    t = jnp.tanh(SQRT_2_OVER_PI * u * (1.0 + CUBIC * square))
    half = 0.5 * (1.0 + t)
    slope = half + 0.5 * u * (1.0 - t * t) * (
        SQRT_2_OVER_PI * (1.0 + 3.0 * CUBIC * square)
    )
    return u * half, slope


def head_ones(width, size):
    a = lax.broadcasted_iota(jnp.int32, (width, width), 0) // size
    b = lax.broadcasted_iota(jnp.int32, (width, width), 1) // size
    return (a == b).astype(F32).astype(BF)


def head_stack(heads, tokens, width):
    size = width // heads
    a = lax.broadcasted_iota(jnp.int32, (heads * tokens, width), 0) // tokens
    b = lax.broadcasted_iota(jnp.int32, (heads * tokens, width), 1) // size
    return (a == b).astype(F32).astype(BF)


def stacked(x, mask):
    return jnp.concatenate([x] * HEADS, axis=0) * mask


def side_mask(window_row, threshold, tokens):
    shape = (tokens, HEADS * tokens)
    a = lax.broadcasted_iota(jnp.int32, shape, 0) // WIN
    b = (lax.broadcasted_iota(jnp.int32, shape, 1) % tokens) // WIN
    first = (window_row * WIN + a) >= threshold
    second = (window_row * WIN + b) >= threshold
    return jnp.where(first == second, 1.0, 0.0).astype(F32)


def window(ref, i, w):
    block = ref[i, :, w, :, :]
    return block.reshape(block.shape[0] * block.shape[1], block.shape[2])


def attention_chunk(qkv, scale, ones_ref, mask_ref, allowed, e_ref, o_ref, count, tokens):
    width = qkv.shape[1] // 3
    q = qkv[:, :width].astype(F32)
    k = qkv[:, width : 2 * width].astype(F32)
    v = qkv[:, 2 * width :]
    ones = ones_ref[...]
    qs = (q * lax.rsqrt(nn((q * q).astype(BF), ones) + 1.0) * scale).astype(BF)
    kn = (k * lax.rsqrt(nn((k * k).astype(BF), ones) + 1.0)).astype(BF)
    mask = mask_ref[...]
    for w in range(count):
        part = slice(w * tokens, (w + 1) * tokens)
        expo = jnp.exp(nt(qs[part], stacked(kn[part], mask)))
        if allowed is not None:
            expo = expo * allowed
        expo = expo.astype(BF)
        e_ref[part] = expo
        o_ref[part] = nn(expo, stacked(v[part], mask))
    return (o_ref[...] / nn(e_ref[...], mask)).astype(BF)


def attention_chunk_back(
    qkv, d_out, scale, ones_ref, mask_ref, allowed, dq_ref, dk_ref, dv_ref, count, tokens
):
    width = qkv.shape[1] // 3
    size = width // HEADS
    q = qkv[:, :width].astype(F32)
    k = qkv[:, width : 2 * width].astype(F32)
    v = qkv[:, 2 * width :]
    ones = ones_ref[...]
    rq = lax.rsqrt(nn((q * q).astype(BF), ones) + 1.0)
    rk = lax.rsqrt(nn((k * k).astype(BF), ones) + 1.0)
    qs = (q * rq * scale).astype(BF)
    kn = (k * rk).astype(BF)
    mask = mask_ref[...]
    lane_head = lax.broadcasted_iota(jnp.int32, (1, LANES), 1) // size
    per_tile = LANES // size
    for w in range(count):
        part = slice(w * tokens, (w + 1) * tokens)
        kw = kn[part]
        qm = stacked(qs[part], mask)
        dm = stacked(d_out[part], mask)
        expo = jnp.exp(nt(kw, qm))
        if allowed is not None:
            expo = expo * allowed
        p = expo * (1.0 / jnp.sum(expo, 0, keepdims=True))
        dp = nt(v[part], dm)
        ds = (p * (dp - jnp.sum(p * dp, 0, keepdims=True))).astype(BF)
        dv_ref[part] = nn(p.astype(BF), dm)
        dk_ref[part] = nn(ds, qm)
        full = tn(ds, kw)
        tiles = []
        for tile in range(width // LANES):
            total = None
            for s in range(per_tile):
                h = tile * per_tile + s
                block = full[h * tokens : (h + 1) * tokens, tile * LANES : (tile + 1) * LANES]
                block = jnp.where(lane_head == s, block, 0.0)
                total = block if total is None else total + block
            tiles.append(total)
        dq_ref[part] = jnp.concatenate(tiles, axis=1)
    dqs = dq_ref[...]
    dkn = dk_ref[...]
    dq = scale * rq * (dqs - q * (rq * rq) * nn((q * dqs).astype(BF), ones))
    dk = rk * (dkn - k * (rk * rk) * nn((k * dkn).astype(BF), ones))
    return jnp.concatenate([dq.astype(BF), dk.astype(BF), dv_ref[...].astype(BF)], axis=1)


def route_kernel(
    cap, count_ref, owner_ref, point_ref, values_ref, r_ref, w2_ref,
    send_ref, mixed_ref, y_ref, buf_ref, tgt_ref, tgt_smem, sem,
):
    slots = owner_ref.shape[1]
    devices = send_ref.shape[0]
    stride = cap + EXTRA
    owner = owner_ref[...]
    live = lax.broadcasted_iota(jnp.int32, (1, slots), 1) < count_ref[0]
    match = lax.broadcasted_iota(jnp.int32, (devices, slots), 0) == owner
    match = jnp.where(match, 1.0, 0.0).astype(F32)
    a = lax.broadcasted_iota(jnp.int32, (LANES, LANES), 0)
    b = lax.broadcasted_iota(jnp.int32, (LANES, LANES), 1)
    upper = jnp.where(a < b, 1.0, 0.0).astype(BF)
    chunks = slots // LANES
    flat = jnp.concatenate(
        [match[:, c * LANES : (c + 1) * LANES] for c in range(chunks)], axis=0
    )
    before = nn(flat.astype(BF), upper)
    carry = jnp.zeros((devices, 1), F32)
    ranks = []
    for c in range(chunks):
        here = match[:, c * LANES : (c + 1) * LANES]
        seen = before[c * devices : (c + 1) * devices] + carry
        ranks.append(jnp.sum(here * seen, 0, keepdims=True))
        carry = carry + jnp.sum(here, 1, keepdims=True)
    rank = jnp.concatenate(ranks, axis=1).astype(jnp.int32)
    tgt_ref[...] = jnp.where(live, owner * stride + rank, devices * stride)
    copy = pltpu.make_async_copy(tgt_ref, tgt_smem, sem)
    copy.start()
    place = lax.broadcasted_iota(jnp.int32, (cap, slots), 0) == rank
    place = jnp.where(place & live, 1.0, 0.0).astype(BF)
    point = point_ref[...]
    high = (match * (point // LANES + 1).astype(F32)).astype(BF)
    low = (match * (point % LANES).astype(F32)).astype(BF)
    high = nt(high, place)
    low = nt(low, place)
    best = lax.Precision.HIGHEST
    dims = (((1,), (1,)), ((), ()))
    m2 = lax.dot_general(
        r_ref[...], w2_ref[...], dims, precision=best, preferred_element_type=F32
    )
    mixed_ref[...] = jnp.dot(
        w2_ref[...], m2, precision=best, preferred_element_type=F32
    ).astype(BF)
    y_ref[...] = nn(values_ref[...].astype(BF), m2.astype(BF))
    buf_ref[...] = jnp.zeros_like(buf_ref)
    copy.wait()
    unroll = 16

    def move(step, _):
        for u in range(unroll):
            j = step * unroll + u
            buf_ref[pl.ds(tgt_smem[0, j], 1), :] = y_ref[pl.ds(j, 1), :]
        return 0

    lax.fori_loop(0, slots // unroll, move, 0)
    for d in range(devices):
        send_ref[d, :, :] = buf_ref[d * stride : (d + 1) * stride, :].astype(BF)
    for d in range(devices):
        row = jnp.zeros((EXTRA, 2 * LANES), F32)
        row = jnp.concatenate(
            [
                jnp.pad(high[d : d + 1], ((0, 0), (0, LANES - cap))),
                jnp.pad(low[d : d + 1], ((0, 0), (0, LANES - cap))),
            ],
            axis=1,
        )
        send_ref[d, cap : cap + EXTRA, :] = jnp.broadcast_to(row, (EXTRA, 2 * LANES)).astype(BF)


def route(owner, point, count, values, r_inverse, w2, devices, cap):
    slots, channels = values.shape
    stride = cap + EXTRA
    return pl.pallas_call(
        functools.partial(route_kernel, cap),
        out_shape=(
            jax.ShapeDtypeStruct((devices, stride, channels), BF),
            jax.ShapeDtypeStruct(w2.shape, BF),
        ),
        in_specs=[SMEM, VMEM, VMEM, VMEM, VMEM, VMEM],
        out_specs=(VMEM, VMEM),
        scratch_shapes=[
            pltpu.VMEM((slots, channels), F32),
            pltpu.VMEM((devices * stride + EXTRA, channels), F32),
            pltpu.VMEM((1, slots), jnp.int32),
            pltpu.SMEM((1, slots), jnp.int32),
            pltpu.SemaphoreType.DMA,
        ],
        name="route",
    )(count, owner, point, values, r_inverse, w2)


def first_kernel(
    state_ref, we_ref, gain_ref, wqkv_ref, wproj_ref, scale_ref, wup_ref, wdown_ref,
    z1_ref, h1_ref, h0_ref, hm_ref, qkv_ref, gp_ref, top_ref, left_ref, corner_ref,
    ones_ref, mask_ref, e_ref, o_ref,
):
    rows, _, cols, _, _ = state_ref.shape
    width = we_ref.shape[1]
    tokens = WIN * WIN
    chunk = cols * tokens
    ones_ref[...] = head_ones(width, width // HEADS)
    mask_ref[...] = head_stack(HEADS, tokens, width)

    def body(i, _):
        x = jnp.concatenate([window(state_ref, i, w).astype(BF) for w in range(cols)], axis=0)
        h0 = nn(x, we_ref[...])
        here = pl.ds(pl.multiple_of(i * chunk, chunk), chunk)
        h0_ref[here, :] = h0
        qkv = nn(norm(h0, gain_ref[0:1]), wqkv_ref[0]).astype(BF)
        qkv_ref[here, :] = qkv
        mixed = attention_chunk(
            qkv, scale_ref[...], ones_ref, mask_ref, None, e_ref, o_ref, cols, tokens
        )
        hm = h0 + nn(mixed, wproj_ref[0]).astype(BF).astype(F32)
        hm_ref[here, :] = hm
        inner, slope = gelu_parts(nn(norm(hm, gain_ref[1:2]), wup_ref[0]))
        gp_ref[here, :] = slope.astype(BF)
        h1 = hm + nn(inner.astype(BF), wdown_ref[0])
        z1 = norm(h1, gain_ref[2:3]).astype(F32)
        for w in range(cols):
            part = slice(w * tokens, (w + 1) * tokens)
            h1_ref[i, :, w, :, :] = h1[part].reshape(WIN, WIN, width)
            z1_ref[i, :, w, :, :] = z1[part].reshape(WIN, WIN, width)
        return 0

    lax.fori_loop(0, rows, body, 0)
    top_ref[...] = z1_ref[0, 0:SHIFT, :, :, :].astype(BF)
    left_ref[...] = z1_ref[:, :, 0, 0:SHIFT, :].astype(BF)
    corner_ref[...] = z1_ref[0, 0:SHIFT, 0, 0:SHIFT, :].astype(BF)


def layer_spec(array, b):
    shape = (1,) + array.shape[1:]
    return pl.BlockSpec(shape, lambda *_: (b,) + (0,) * (array.ndim - 1))


def whole_spec(array):
    return pl.BlockSpec(array.shape, lambda *_: (0,) * array.ndim)


def first_block(state5, we, gains, wqkv, wproj, scale, wup, wdown):
    wr, _, wc, _, _ = state5.shape
    width = we.shape[1]
    tokens = wr * wc * WIN * WIN
    chunk = wc * WIN * WIN
    sh = jax.ShapeDtypeStruct
    outs = (
        sh((wr, WIN, wc, WIN, width), F32),
        sh((wr, WIN, wc, WIN, width), F32),
        sh((tokens, width), F32),
        sh((tokens, width), F32),
        sh((tokens, 3 * width), BF),
        sh((tokens, wup.shape[2]), BF),
        sh((SHIFT, wc, WIN, width), BF),
        sh((wr, WIN, SHIFT, width), BF),
        sh((SHIFT, SHIFT, width), BF),
    )
    return pl.pallas_call(
        first_kernel,
        grid=(1,),
        out_shape=outs,
        in_specs=[
            whole_spec(state5), whole_spec(we), whole_spec(gains), layer_spec(wqkv, 0),
            layer_spec(wproj, 0), whole_spec(scale), layer_spec(wup, 0), layer_spec(wdown, 0),
        ],
        out_specs=tuple(whole_spec(o) for o in outs),
        scratch_shapes=[
            pltpu.VMEM((width, width), BF),
            pltpu.VMEM((HEADS * WIN * WIN, width), BF),
            pltpu.VMEM((chunk, HEADS * WIN * WIN), BF),
            pltpu.VMEM((chunk, width), F32),
        ],
        name="first_block",
    )(state5, we, gains, wqkv, wproj, scale, wup, wdown)


def fill_ahead(pad_ref, own, right_ref, below_ref, corner_ref):
    rows, cols, _ = own.shape
    pad_ref[0:rows, 0:cols, :] = own
    pad_ref[0:rows, cols : cols + SHIFT, :] = right_ref[...].astype(F32)
    pad_ref[rows : rows + SHIFT, 0:cols, :] = below_ref[...].astype(F32)
    pad_ref[rows : rows + SHIFT, cols : cols + SHIFT, :] = corner_ref[...].astype(F32)


def rolled_window(pad_ref, i, w):
    block = pad_ref[
        pl.ds(i * WIN + SHIFT, WIN), SHIFT + w * WIN : SHIFT + (w + 1) * WIN, :
    ]
    return block.reshape(WIN * WIN, block.shape[2])


def emit_behind(out_ref, low_ref, east_ref, corner_ref):
    rows, cols, _ = out_ref.shape
    low_ref[...] = out_ref[rows - SHIFT : rows, :, :].astype(BF)
    east_ref[...] = out_ref[:, cols - SHIFT : cols, :].astype(BF)
    corner_ref[...] = out_ref[rows - SHIFT : rows, cols - SHIFT : cols, :].astype(BF)


def shifted_kernel(
    total_rows, start_ref, z1_ref, right_ref, below_ref, corner_ref, wqkv_ref, wproj_ref, scale_ref,
    ans_ref, low_ref, east_ref, last_ref, qkv_ref,
    pad_ref, ones_ref, mask_ref, e_ref, o_ref,
):
    rows, cols, width = z1_ref.shape
    wr, wc = rows // WIN, cols // WIN
    tokens = WIN * WIN
    chunk = wc * tokens
    ones_ref[...] = head_ones(width, width // HEADS)
    mask_ref[...] = head_stack(HEADS, tokens, width)
    fill_ahead(pad_ref, z1_ref[...], right_ref, below_ref, corner_ref)
    threshold = total_rows - SHIFT - start_ref[0]

    def body(i, _):
        z = jnp.concatenate([rolled_window(pad_ref, i, w).astype(BF) for w in range(wc)], axis=0)
        qkv = nn(z, wqkv_ref[0]).astype(BF)
        qkv_ref[pl.ds(pl.multiple_of(i * chunk, chunk), chunk), :] = qkv
        allowed = side_mask(i, threshold, tokens)
        mixed = attention_chunk(
            qkv, scale_ref[...], ones_ref, mask_ref, allowed, e_ref, o_ref, wc, tokens
        )
        answer = nn(mixed, wproj_ref[0]).astype(BF).astype(F32)
        for w in range(wc):
            ans_ref[pl.ds(i * WIN, WIN), w * WIN : (w + 1) * WIN, :] = answer[
                w * tokens : (w + 1) * tokens
            ].reshape(WIN, WIN, width)
        return 0

    lax.fori_loop(0, wr, body, 0)
    emit_behind(ans_ref, low_ref, east_ref, last_ref)


def behind_shapes(rows, cols, width):
    sh = jax.ShapeDtypeStruct
    return (
        sh((rows, cols, width), F32),
        sh((SHIFT, cols, width), BF),
        sh((rows, SHIFT, width), BF),
        sh((SHIFT, SHIFT, width), BF),
    )


def shifted_forward(start, z1, right, below, corner, wqkv, wproj, scale, total_rows):
    rows, cols, width = z1.shape
    tokens = rows * cols
    chunk = cols * WIN
    outs = behind_shapes(rows, cols, width) + (jax.ShapeDtypeStruct((tokens, 3 * width), BF),)
    return pl.pallas_call(
        functools.partial(shifted_kernel, total_rows),
        grid=(1,),
        out_shape=outs,
        in_specs=[SMEM]
        + [whole_spec(x) for x in (z1, right, below, corner)]
        + [layer_spec(wqkv, 1), layer_spec(wproj, 1), whole_spec(scale)],
        out_specs=tuple(whole_spec(o) for o in outs),
        scratch_shapes=[
            pltpu.VMEM((rows + SHIFT, cols + WIN, width), F32),
            pltpu.VMEM((width, width), BF),
            pltpu.VMEM((HEADS * WIN * WIN, width), BF),
            pltpu.VMEM((chunk, HEADS * WIN * WIN), BF),
            pltpu.VMEM((chunk, width), F32),
        ],
        name="shifted_forward",
    )(start, z1, right, below, corner, wqkv, wproj, scale)


def fill_behind(pad_ref, own, above_ref, west_ref, corner_ref):
    rows, cols, _ = own.shape
    pad_ref[SHIFT : SHIFT + rows, SHIFT : SHIFT + cols, :] = own
    pad_ref[0:SHIFT, SHIFT : SHIFT + cols, :] = above_ref[...].astype(F32)
    pad_ref[SHIFT : SHIFT + rows, 0:SHIFT, :] = west_ref[...].astype(F32)
    pad_ref[0:SHIFT, 0:SHIFT, :] = corner_ref[...].astype(F32)


def middle_kernel(
    cap, h1_ref, ans_ref, above_ref, west_ref, corner_ref, state_ref, obs_ref, mixed_ref,
    gain_ref, wup_ref, wdown_ref, whead_ref, w1_ref,
    out_ref, third_ref, top_ref, left_ref, edge_ref,
    pad_ref, h2_ref, gp_ref, table_ref, found_ref, idx_ref, cnt_ref, dup_ref,
    idx_smem, cnt_smem, dup_smem, sems,
):
    rows, cols, width = h1_ref.shape
    devices, stride, channels = obs_ref.shape
    tokens = rows * cols
    step = tokens // 2

    codes = obs_ref[:, cap : cap + EXTRA, :].astype(F32)[:, 0, :]
    high = codes[:, :LANES].astype(jnp.int32)
    low = codes[:, LANES : 2 * LANES].astype(jnp.int32)
    point = jnp.where(high > 0, (high - 1) * LANES + low, 0)
    lane = lax.broadcasted_iota(jnp.int32, (devices, LANES), 1)
    dump = PIX * tokens
    idx = jnp.where(
        high > 0, (point % PIX) * tokens + point // PIX, dump + lane % EXTRA
    )
    idx_ref[...] = idx
    cnt_ref[...] = jnp.broadcast_to(
        jnp.sum(jnp.where(high > 0, 1.0, 0.0), 1, keepdims=True), (devices, LANES)
    ).astype(jnp.int32)
    same = jnp.zeros((devices, LANES), jnp.int32)
    for s in range(1, EXTRA):
        hit = (pltpu.roll(idx, s, 1) == idx) & (lane % EXTRA >= s)
        same = jnp.maximum(same, jnp.where(hit, 1, 0))
    for s in (4, 2, 1):
        same = jnp.maximum(same, pltpu.roll(same, LANES - s, 1))
    dup_ref[...] = same
    copies = [
        pltpu.make_async_copy(a, b, sems.at[n])
        for n, (a, b) in enumerate(
            ((idx_ref, idx_smem), (cnt_ref, cnt_smem), (dup_ref, dup_smem))
        )
    ]
    for copy in copies:
        copy.start()

    fill_behind(pad_ref, ans_ref[...], above_ref, west_ref, corner_ref)
    h2_ref[...] = (h1_ref[...] + pad_ref[0:rows, 0:cols, :]).reshape(tokens, width)
    for s in range(PIX):
        table_ref[s * tokens : (s + 1) * tokens, :] = jnp.zeros((tokens, LANES), F32)
    table_ref[PIX * tokens :, :] = jnp.zeros((EXTRA, LANES), F32)

    def forward(i, _):
        here = pl.ds(pl.multiple_of(i * step, step), step)
        h2 = h2_ref[here, :]
        inner, slope = gelu_parts(nn(norm(h2, gain_ref[3:4]), wup_ref[0]))
        gp_ref[here, :] = slope.astype(BF)
        h3 = (h2 + nn(inner.astype(BF), wdown_ref[0])).astype(BF)
        for s in range(PIX):
            lifted = nn(h3, whead_ref[:, s * LANES : (s + 1) * LANES])
            there = pl.ds(pl.multiple_of(s * tokens + i * step, WIN), step)
            table_ref[there, 0:VARS] = (
                state_ref[here, s * VARS : (s + 1) * VARS] + lifted[:, 0:VARS]
            )
        return 0

    lax.fori_loop(0, 2, forward, 0)
    for copy in copies:
        copy.wait()

    group = 8

    def gather(d, _):
        def some(g, _):
            base = d * cap + g * group
            for u in range(group):
                found_ref[pl.ds(base + u, 1), :] = table_ref[
                    pl.ds(idx_smem[d, g * group + u], 1), :
                ]
            return 0

        lax.fori_loop(0, (cnt_smem[d, 0] + group - 1) // group, some, 0)
        return 0

    lax.fori_loop(0, devices, gather, 0)
    table_ref[...] = jnp.zeros_like(table_ref)

    def radiance(d, _):
        @pl.when(cnt_smem[d, 0] > 0)
        def _():
            here = pl.ds(pl.multiple_of(d * cap, cap), cap)
            t = jnp.tanh(nn(found_ref[here, :].astype(BF), w1_ref[...]))
            pulled = nn(t.astype(BF), mixed_ref[...]) - obs_ref[d, 0:cap, :].astype(F32)
            pulled = pulled * (1.0 - t * t)
            found_ref[here, :] = nt(pulled.astype(BF), w1_ref[...])

        return 0

    lax.fori_loop(0, devices, radiance, 0)

    def scatter(d, _):
        def some(g, _):
            base = d * cap + g * group
            spots = [idx_smem[d, g * group + u] for u in range(group)]

            @pl.when(dup_smem[d, g * group] == 0)
            def _():
                sums = [
                    table_ref[pl.ds(spots[u], 1), :] + found_ref[pl.ds(base + u, 1), :]
                    for u in range(group)
                ]
                for u in range(group):
                    table_ref[pl.ds(spots[u], 1), :] = sums[u]

            @pl.when(dup_smem[d, g * group] != 0)
            def _():
                for u in range(group):
                    table_ref[pl.ds(spots[u], 1), :] = (
                        table_ref[pl.ds(spots[u], 1), :] + found_ref[pl.ds(base + u, 1), :]
                    )

            return 0

        lax.fori_loop(0, (cnt_smem[d, 0] + group - 1) // group, some, 0)
        return 0

    lax.fori_loop(0, devices, scatter, 0)

    def backward(i, _):
        here = pl.ds(pl.multiple_of(i * step, step), step)
        grad = None
        for s in range(0, PIX, 2):
            both = []
            for n in (s, s + 1):
                there = pl.ds(pl.multiple_of(n * tokens + i * step, WIN), step)
                part = table_ref[there, :]
                out_ref[here, n * VARS : (n + 1) * VARS] = part[:, 0:VARS]
                both.append(part.astype(BF))
            add = nt(jnp.concatenate(both, axis=1), whead_ref[:, s * LANES : (s + 2) * LANES])
            grad = add if grad is None else grad + add
        grad = grad.astype(BF)
        d_inner = nt(grad, wdown_ref[0]) * gp_ref[here, :].astype(F32)
        d_normed = nt(d_inner.astype(BF), wup_ref[0])
        third = grad.astype(F32) + norm_back(h2_ref[here, :], gain_ref[3:4], d_normed)
        third_ref[pl.ds(i * (rows // 2), rows // 2), :, :] = third.reshape(rows // 2, cols, width)
        return 0

    lax.fori_loop(0, 2, backward, 0)
    top_ref[...] = third_ref[0:SHIFT, :, :].astype(BF)
    left_ref[...] = third_ref[:, 0:SHIFT, :].astype(BF)
    edge_ref[...] = third_ref[0:SHIFT, 0:SHIFT, :].astype(BF)


def middle(h1, ans, above, west, corner, state, obs, mixed, gains, wup, wdown, whead, w1):
    rows, cols, width = h1.shape
    tokens = rows * cols
    devices, stride, channels = obs.shape
    cap = stride - EXTRA
    sh = jax.ShapeDtypeStruct
    outs = (sh((tokens, state.shape[1]), F32),) + behind_shapes(rows, cols, width)
    args = (h1, ans, above, west, corner, state, obs, mixed, gains)
    return pl.pallas_call(
        functools.partial(middle_kernel, cap),
        grid=(1,),
        out_shape=outs,
        in_specs=[whole_spec(x) for x in args]
        + [layer_spec(wup, 1), layer_spec(wdown, 1), whole_spec(whead), whole_spec(w1)],
        out_specs=tuple(whole_spec(o) for o in outs),
        scratch_shapes=[
            pltpu.VMEM((rows + SHIFT, cols + WIN, width), F32),
            pltpu.VMEM((tokens, width), F32),
            pltpu.VMEM((tokens, wup.shape[2]), BF),
            pltpu.VMEM((PIX * tokens + EXTRA, LANES), F32),
            pltpu.VMEM((devices * cap, LANES), F32),
            pltpu.VMEM((devices, LANES), jnp.int32),
            pltpu.VMEM((devices, LANES), jnp.int32),
            pltpu.VMEM((devices, LANES), jnp.int32),
            pltpu.SMEM((devices, LANES), jnp.int32),
            pltpu.SMEM((devices, LANES), jnp.int32),
            pltpu.SMEM((devices, LANES), jnp.int32),
            pltpu.SemaphoreType.DMA((3,)),
        ],
        name="middle",
    )(*args, wup, wdown, whead, w1)


def shifted_back_kernel(
    total_rows, start_ref, third_ref, right_ref, below_ref, corner_ref, qkv_ref,
    wqkv_ref, wproj_ref, scale_ref,
    dz_ref, low_ref, east_ref, last_ref,
    pad_ref, ones_ref, mask_ref, dq_ref, dk_ref, dv_ref,
):
    rows, cols, width = third_ref.shape
    wr, wc = rows // WIN, cols // WIN
    tokens = WIN * WIN
    chunk = wc * tokens
    ones_ref[...] = head_ones(width, width // HEADS)
    mask_ref[...] = head_stack(HEADS, tokens, width)
    fill_ahead(pad_ref, third_ref[...], right_ref, below_ref, corner_ref)
    threshold = total_rows - SHIFT - start_ref[0]

    def body(i, _):
        d_answer = jnp.concatenate(
            [rolled_window(pad_ref, i, w).astype(BF) for w in range(wc)], axis=0
        )
        d_out = nt(d_answer, wproj_ref[0]).astype(BF)
        allowed = side_mask(i, threshold, tokens)
        qkv = qkv_ref[pl.ds(pl.multiple_of(i * chunk, chunk), chunk), :]
        d_qkv = attention_chunk_back(
            qkv, d_out, scale_ref[...], ones_ref, mask_ref, allowed,
            dq_ref, dk_ref, dv_ref, wc, tokens,
        )
        dz = nt(d_qkv, wqkv_ref[0]).astype(BF).astype(F32)
        for w in range(wc):
            dz_ref[pl.ds(i * WIN, WIN), w * WIN : (w + 1) * WIN, :] = dz[
                w * tokens : (w + 1) * tokens
            ].reshape(WIN, WIN, width)
        return 0

    lax.fori_loop(0, wr, body, 0)
    emit_behind(dz_ref, low_ref, east_ref, last_ref)


def shifted_backward(start, third, right, below, corner, qkv, wqkv, wproj, scale, total_rows):
    rows, cols, width = third.shape
    chunk = cols * WIN
    outs = behind_shapes(rows, cols, width)
    return pl.pallas_call(
        functools.partial(shifted_back_kernel, total_rows),
        grid=(1,),
        out_shape=outs,
        in_specs=[SMEM]
        + [whole_spec(x) for x in (third, right, below, corner, qkv)]
        + [layer_spec(wqkv, 1), layer_spec(wproj, 1), whole_spec(scale)],
        out_specs=tuple(whole_spec(o) for o in outs),
        scratch_shapes=[
            pltpu.VMEM((rows + SHIFT, cols + WIN, width), F32),
            pltpu.VMEM((width, width), BF),
            pltpu.VMEM((HEADS * WIN * WIN, width), BF),
        ]
        + [pltpu.VMEM((chunk, width), F32)] * 3,
        name="shifted_backward",
    )(start, third, right, below, corner, qkv, wqkv, wproj, scale)


def last_kernel(
    third_ref, dz_ref, above_ref, west_ref, corner_ref, h1_ref, h0_ref, hm_ref, qkv_ref, gp_ref,
    partial_ref, state_ref, back_ref, inv_ref, we_ref, gain_ref, wqkv_ref, wproj_ref, scale_ref,
    wup_ref, wdown_ref,
    out_ref,
    pad_ref, ones_ref, mask_ref, dq_ref, dk_ref, dv_ref,
):
    rows, cols, width = dz_ref.shape
    wr, wc = rows // WIN, cols // WIN
    tokens = WIN * WIN
    chunk = wc * tokens
    ones_ref[...] = head_ones(width, width // HEADS)
    mask_ref[...] = head_stack(HEADS, tokens, width)
    fill_behind(pad_ref, dz_ref[...], above_ref, west_ref, corner_ref)

    def body(i, _):
        here = pl.ds(pl.multiple_of(i * chunk, chunk), chunk)
        band = pl.ds(i * WIN, WIN)

        def take(ref):
            return jnp.concatenate(
                [
                    ref[band, w * WIN : (w + 1) * WIN, :].reshape(tokens, width)
                    for w in range(wc)
                ],
                axis=0,
            )

        second = take(third_ref) + norm_back(take(h1_ref), gain_ref[2:3], take(pad_ref))
        d_inner = nt(second.astype(BF), wdown_ref[0]) * gp_ref[here, :].astype(F32)
        d_normed = nt(d_inner.astype(BF), wup_ref[0])
        d_hm = second + norm_back(hm_ref[here, :], gain_ref[1:2], d_normed)
        d_out = nt(d_hm.astype(BF), wproj_ref[0]).astype(BF)
        d_qkv = attention_chunk_back(
            qkv_ref[here, :], d_out, scale_ref[...], ones_ref, mask_ref, None,
            dq_ref, dk_ref, dv_ref, wc, tokens,
        )
        dz = nt(d_qkv, wqkv_ref[0])
        d_h0 = (d_hm + norm_back(h0_ref[here, :], gain_ref[0:1], dz)).astype(BF)
        for w in range(wc):
            grad = nt(d_h0[w * tokens : (w + 1) * tokens], we_ref[...])
            grad = grad.reshape(WIN, WIN, grad.shape[1])
            spot = (band, slice(w * WIN, (w + 1) * WIN), slice(None))
            out_ref[spot] = (
                grad + partial_ref[spot] + inv_ref[...] * (state_ref[spot] - back_ref[spot])
            )
        return 0

    lax.fori_loop(0, wr, body, 0)


def last_block(
    third, dz, above, west, corner, h1, h0, hm, qkv, gp, partial, state, background, inv, we,
    gains, wqkv, wproj, scale, wup, wdown,
):
    rows, cols, width = dz.shape
    chunk = cols * WIN
    args = (
        third, dz, above, west, corner, h1, h0, hm, qkv, gp, partial, state, background, inv, we,
        gains,
    )
    out = jax.ShapeDtypeStruct(state.shape, F32)
    return pl.pallas_call(
        last_kernel,
        grid=(1,),
        out_shape=out,
        in_specs=[whole_spec(x) for x in args]
        + [layer_spec(wqkv, 0), layer_spec(wproj, 0), whole_spec(scale)]
        + [layer_spec(wup, 0), layer_spec(wdown, 0)],
        out_specs=whole_spec(out),
        scratch_shapes=[
            pltpu.VMEM((rows + SHIFT, cols + WIN, width), F32),
            pltpu.VMEM((width, width), BF),
            pltpu.VMEM((HEADS * WIN * WIN, width), BF),
        ]
        + [pltpu.VMEM((chunk, width), F32)] * 3,
        name="last_block",
    )(*args, wqkv, wproj, scale, wup, wdown)


def neighbour(x, by_lat, by_lon):
    lat, lon = lax.axis_size("lat"), lax.axis_size("lon")
    pairs = [
        (a * lon + b, ((a + by_lat) % lat) * lon + (b + by_lon) % lon)
        for a in range(lat)
        for b in range(lon)
    ]
    return lax.ppermute(x, ("lat", "lon"), pairs)


def local(
    state,
    background,
    inv_background,
    w_embed,
    norm_gain,
    w_qkv,
    w_proj,
    head_scale,
    w_up,
    w_down,
    w_head,
    w_obs1,
    w_obs2,
    r_inverse,
    obs_values,
    obs_owner,
    obs_point,
    obs_count,
):
    rows, cols, patch_values = state.shape
    width = w_embed.shape[1]
    total_rows = rows * lax.axis_size("lat")
    row_start = (lax.axis_index("lat") * rows).astype(jnp.int32).reshape(1)
    devices = lax.axis_size("lat") * lax.axis_size("lon")
    slots = obs_values.shape[0]
    cap = 2 * slots // devices

    send, mixed = route(
        obs_owner.reshape(1, slots), obs_point.reshape(1, slots), obs_count, obs_values,
        r_inverse, w_obs2, devices, cap,
    )
    obs = lax.all_to_all(send, ("lat", "lon"), split_axis=0, concat_axis=0, tiled=True)

    gains = norm_gain.reshape(-1, width)
    scales = jnp.repeat(head_scale, width // HEADS, axis=1)
    w1 = jnp.pad(w_obs1, ((0, LANES - VARS), (0, 0))).astype(BF)
    whead = jnp.pad(w_head.reshape(width, PIX, VARS), ((0, 0), (0, 0), (0, LANES - VARS)))
    whead = whead.reshape(width, PIX * LANES)

    state5 = state.reshape(rows // WIN, WIN, cols // WIN, WIN, patch_values)
    z1, h1, h0, hm, qkv0, gp0, top, left, corner = first_block(
        state5, w_embed, gains, w_qkv, w_proj, scales[0:1], w_up, w_down
    )
    z1 = z1.reshape(rows, cols, width)
    h1 = h1.reshape(rows, cols, width)
    below = neighbour(top.reshape(SHIFT, cols, width), -1, 0)
    right = neighbour(left.reshape(rows, SHIFT, width), 0, -1)
    corner = neighbour(corner, -1, -1)
    answer, low, east, last, qkv1 = shifted_forward(
        row_start, z1, right, below, corner, w_qkv, w_proj, scales[1:2], total_rows
    )
    above = neighbour(low, 1, 0)
    west = neighbour(east, 0, 1)
    last = neighbour(last, 1, 1)
    partial, third, top, left, corner = middle(
        h1, answer, above, west, last, state.reshape(rows * cols, patch_values), obs, mixed,
        gains, w_up, w_down, whead, w1,
    )
    below = neighbour(top, -1, 0)
    right = neighbour(left, 0, -1)
    corner = neighbour(corner, -1, -1)
    dz, low, east, last = shifted_backward(
        row_start, third, right, below, corner, qkv1, w_qkv, w_proj, scales[1:2], total_rows
    )
    above = neighbour(low, 1, 0)
    west = neighbour(east, 0, 1)
    last = neighbour(last, 1, 1)
    return last_block(
        third, dz, above, west, last, h1, h0, hm, qkv0, gp0,
        partial.reshape(state.shape), state, background, inv_background.reshape(1, 1, -1),
        w_embed, gains, w_qkv, w_proj, scales[0:1], w_up, w_down,
    )


def solution(mesh):
    placed = (
        P("lat", "lon", None),
        P("lat", "lon", None),
        P(),
        P(),
        P(),
        P(),
        P(),
        P(),
        P(),
        P(),
        P(),
        P(),
        P(),
        P(),
        P(("lat", "lon"), None),
        P(("lat", "lon"), None),
        P(("lat", "lon")),
        P(("lat", "lon")),
    )
    return jax.shard_map(
        local, mesh=mesh, in_specs=placed, out_specs=P("lat", "lon", None), check_vma=False
    )
```

```python
import functools

import jax
import jax.numpy as jnp
from jax import lax
from jax.experimental import pallas as pl
from jax.experimental.pallas import tpu as pltpu
from jax.sharding import PartitionSpec as P

HEADS = 8
VARS = 69
PIX = 16
WIN = 8
SHIFT = 4
LANES = 128
EXTRA = 8
EPS = 1e-05
BF = jnp.bfloat16
F32 = jnp.float32
SQRT_2_OVER_PI = 0.7978845608028654
CUBIC = 0.044715

VMEM = pl.BlockSpec(memory_space=pltpu.VMEM)
SMEM = pl.BlockSpec(memory_space=pltpu.SMEM)
ANY = pl.BlockSpec(memory_space=pl.ANY)
MIB = 1024 * 1024
LIMIT_ROUTE = 20 * MIB
LIMIT_FIRST = 24 * MIB
LIMIT_SHIFTED = 16 * MIB
LIMIT_FORECAST = 36 * MIB
LIMIT_ADJOINT = 32 * MIB
LIMIT_BACK = 16 * MIB
LIMIT_LAST = 24 * MIB


def limit(size):
    return pltpu.CompilerParams(vmem_limit_bytes=size)


def cost(flops):
    return pl.CostEstimate(flops=int(flops), bytes_accessed=8 * MIB, transcendentals=0)


def nn(a, b):
    return lax.dot_general(a, b, (((1,), (0,)), ((), ())), preferred_element_type=F32)


def nt(a, b):
    return lax.dot_general(a, b, (((1,), (1,)), ((), ())), preferred_element_type=F32)


def tn(a, b):
    return lax.dot_general(a, b, (((0,), (0,)), ((), ())), preferred_element_type=F32)


def norm_parts(h):
    mean = jnp.mean(h, -1, keepdims=True)
    centred = h - mean
    spread = jnp.mean(centred * centred, -1, keepdims=True)
    rstd = lax.rsqrt(spread + EPS)
    return centred * rstd, rstd


def norm(h, gain):
    return (norm_parts(h)[0] * gain).astype(BF)


def norm_back(h, gain, cotangent):
    xhat, rstd = norm_parts(h)
    scaled = cotangent * gain
    m1 = jnp.mean(scaled, -1, keepdims=True)
    m2 = jnp.mean(scaled * xhat, -1, keepdims=True)
    return rstd * (scaled - m1 - xhat * m2)


def gelu_parts(u):
    square = u * u
    t = jnp.tanh(SQRT_2_OVER_PI * u * (1.0 + CUBIC * square))
    half = 0.5 * (1.0 + t)
    slope = half + 0.5 * u * (1.0 - t * t) * (
        SQRT_2_OVER_PI * (1.0 + 3.0 * CUBIC * square)
    )
    return u * half, slope


def head_ones(width, size):
    a = lax.broadcasted_iota(jnp.int32, (width, width), 0) // size
    b = lax.broadcasted_iota(jnp.int32, (width, width), 1) // size
    return (a == b).astype(F32).astype(BF)


def head_stack(heads, tokens, width):
    size = width // heads
    a = lax.broadcasted_iota(jnp.int32, (heads * tokens, width), 0) // tokens
    b = lax.broadcasted_iota(jnp.int32, (heads * tokens, width), 1) // size
    return (a == b).astype(F32).astype(BF)


def stacked(x, mask):
    return jnp.concatenate([x] * HEADS, axis=0) * mask


def side_mask(window_row, threshold, tokens):
    shape = (tokens, HEADS * tokens)
    a = lax.broadcasted_iota(jnp.int32, shape, 0) // WIN
    b = (lax.broadcasted_iota(jnp.int32, shape, 1) % tokens) // WIN
    first = (window_row * WIN + a) >= threshold
    second = (window_row * WIN + b) >= threshold
    return jnp.where(first == second, 1.0, 0.0).astype(F32)


def window(ref, i, w):
    block = ref[i, :, w, :, :]
    return block.reshape(block.shape[0] * block.shape[1], block.shape[2])


def attention_chunk(qkv, scale, ones_ref, mask_ref, allowed, e_ref, o_ref, count, tokens):
    width = qkv.shape[1] // 3
    q = qkv[:, :width].astype(F32)
    k = qkv[:, width : 2 * width].astype(F32)
    v = qkv[:, 2 * width :]
    ones = ones_ref[...]
    qs = (q * lax.rsqrt(nn((q * q).astype(BF), ones) + 1.0) * scale).astype(BF)
    kn = (k * lax.rsqrt(nn((k * k).astype(BF), ones) + 1.0)).astype(BF)
    mask = mask_ref[...]
    for w in range(count):
        part = slice(w * tokens, (w + 1) * tokens)
        expo = jnp.exp(nt(qs[part], stacked(kn[part], mask)))
        if allowed is not None:
            expo = expo * allowed
        expo = expo.astype(BF)
        e_ref[part] = expo
        o_ref[part] = nn(expo, stacked(v[part], mask))
    return (o_ref[...] / nn(e_ref[...], mask)).astype(BF)


def attention_chunk_back(
    qkv, d_out, scale, ones_ref, mask_ref, allowed, dq_ref, dk_ref, dv_ref, count, tokens
):
    width = qkv.shape[1] // 3
    size = width // HEADS
    q = qkv[:, :width].astype(F32)
    k = qkv[:, width : 2 * width].astype(F32)
    v = qkv[:, 2 * width :]
    ones = ones_ref[...]
    rq = lax.rsqrt(nn((q * q).astype(BF), ones) + 1.0)
    rk = lax.rsqrt(nn((k * k).astype(BF), ones) + 1.0)
    qs = (q * rq * scale).astype(BF)
    kn = (k * rk).astype(BF)
    mask = mask_ref[...]
    lane_head = lax.broadcasted_iota(jnp.int32, (1, LANES), 1) // size
    per_tile = LANES // size
    for w in range(count):
        part = slice(w * tokens, (w + 1) * tokens)
        kw = kn[part]
        qm = stacked(qs[part], mask)
        dm = stacked(d_out[part], mask)
        expo = jnp.exp(nt(kw, qm))
        if allowed is not None:
            expo = expo * allowed
        p = expo * (1.0 / jnp.sum(expo, 0, keepdims=True))
        dp = nt(v[part], dm)
        ds = (p * (dp - jnp.sum(p * dp, 0, keepdims=True))).astype(BF)
        dv_ref[part] = nn(p.astype(BF), dm)
        dk_ref[part] = nn(ds, qm)
        full = tn(ds, kw)
        tiles = []
        for tile in range(width // LANES):
            total = None
            for s in range(per_tile):
                h = tile * per_tile + s
                block = full[h * tokens : (h + 1) * tokens, tile * LANES : (tile + 1) * LANES]
                block = jnp.where(lane_head == s, block, 0.0)
                total = block if total is None else total + block
            tiles.append(total)
        dq_ref[part] = jnp.concatenate(tiles, axis=1)
    dqs = dq_ref[...]
    dkn = dk_ref[...]
    dq = scale * rq * (dqs - q * (rq * rq) * nn((q * dqs).astype(BF), ones))
    dk = rk * (dkn - k * (rk * rk) * nn((k * dkn).astype(BF), ones))
    return jnp.concatenate([dq.astype(BF), dk.astype(BF), dv_ref[...].astype(BF)], axis=1)


def split(cap):
    first = max(8, cap // 4)
    return (first, first, cap - 2 * first), min(32, first)


def route_kernel(
    parts, count_ref, owner_ref, point_ref, values_ref, r_ref, w2_ref,
    send1_ref, send2_ref, send3_ref, mixed_ref, y_ref, buf_ref, tgt_ref, tgt_smem, sem,
):
    cap = sum(parts)
    slots = owner_ref.shape[1]
    devices = send1_ref.shape[0]
    owner = owner_ref[...]
    live = lax.broadcasted_iota(jnp.int32, (1, slots), 1) < count_ref[0]
    match = lax.broadcasted_iota(jnp.int32, (devices, slots), 0) == owner
    match = jnp.where(match, 1.0, 0.0).astype(F32)
    a = lax.broadcasted_iota(jnp.int32, (LANES, LANES), 0)
    b = lax.broadcasted_iota(jnp.int32, (LANES, LANES), 1)
    upper = jnp.where(a < b, 1.0, 0.0).astype(BF)
    chunks = slots // LANES
    flat = jnp.concatenate(
        [match[:, c * LANES : (c + 1) * LANES] for c in range(chunks)], axis=0
    )
    before = nn(flat.astype(BF), upper)
    carry = jnp.zeros((devices, 1), F32)
    ranks = []
    for c in range(chunks):
        here = match[:, c * LANES : (c + 1) * LANES]
        seen = before[c * devices : (c + 1) * devices] + carry
        ranks.append(jnp.sum(here * seen, 0, keepdims=True))
        carry = carry + jnp.sum(here, 1, keepdims=True)
    rank = jnp.concatenate(ranks, axis=1).astype(jnp.int32)
    tgt_ref[...] = jnp.where(live, owner * cap + rank, devices * cap)
    copy = pltpu.make_async_copy(tgt_ref, tgt_smem, sem)
    copy.start()
    place = lax.broadcasted_iota(jnp.int32, (cap, slots), 0) == rank
    place = jnp.where(place & live, 1.0, 0.0).astype(BF)
    point = point_ref[...]
    high = (match * (point // LANES + 1).astype(F32)).astype(BF)
    low = (match * (point % LANES).astype(F32)).astype(BF)
    high = nt(high, place)
    low = nt(low, place)
    best = lax.Precision.HIGHEST
    dims = (((1,), (1,)), ((), ()))
    m2 = lax.dot_general(
        r_ref[...], w2_ref[...], dims, precision=best, preferred_element_type=F32
    )
    mixed_ref[...] = jnp.dot(
        w2_ref[...], m2, precision=best, preferred_element_type=F32
    ).astype(BF)
    y = nn(values_ref[...].astype(BF), m2.astype(BF))
    y_ref[0, :, :] = y[:, :LANES]
    y_ref[1, :, :] = y[:, LANES:]
    buf_ref[...] = jnp.zeros_like(buf_ref)
    copy.wait()
    unroll = 32

    def move(step, _):
        spots = [tgt_smem[0, step * unroll + u] for u in range(unroll)]
        base = pl.multiple_of(step * unroll, unroll)
        for half in range(2):
            for u in range(unroll):
                buf_ref[half, pl.ds(spots[u], 1), :] = y_ref[half, pl.ds(base + u, 1), :]
        return 0

    lax.fori_loop(0, slots // unroll, move, 0)
    for d in range(devices):
        offset = d * cap
        for ref, size in zip((send1_ref, send2_ref, send3_ref), parts):
            for half in range(2):
                ref[d, 0:size, half * LANES : (half + 1) * LANES] = buf_ref[
                    half, offset : offset + size, :
                ].astype(BF)
            offset += size
    fill = ((0, 0), (0, LANES - cap))
    codes = jnp.concatenate([jnp.pad(high, fill), jnp.pad(low, fill)], axis=1)
    for d in range(devices):
        send1_ref[d, parts[0] : parts[0] + EXTRA, :] = jnp.broadcast_to(
            codes[d : d + 1], (EXTRA, 2 * LANES)
        ).astype(BF)


def route(owner, point, count, values, r_inverse, w2, devices, parts):
    slots, channels = values.shape
    cap = sum(parts)
    sizes = (parts[0] + EXTRA,) + tuple(parts[1:])
    return pl.pallas_call(
        functools.partial(route_kernel, parts),
        out_shape=tuple(jax.ShapeDtypeStruct((devices, n, channels), BF) for n in sizes)
        + (jax.ShapeDtypeStruct(w2.shape, BF),),
        in_specs=[SMEM, VMEM, VMEM, VMEM, VMEM, VMEM],
        out_specs=(VMEM,) * 4,
        scratch_shapes=[
            pltpu.VMEM((2, slots, LANES), F32),
            pltpu.VMEM((2, devices * cap + EXTRA, LANES), F32),
            pltpu.VMEM((1, slots), jnp.int32),
            pltpu.SMEM((1, slots), jnp.int32),
            pltpu.SemaphoreType.DMA,
        ],
        compiler_params=limit(LIMIT_ROUTE),
        cost_estimate=cost(1e9),
        name="route",
    )(count, owner, point, values, r_inverse, w2)


def first_kernel(
    state_ref, we_ref, gain_ref, wqkv_ref, wproj_ref, scale_ref, wup_ref, wdown_ref,
    z1_ref, h1_ref, h0_ref, hm_ref, qkv_ref, gp_ref, top_ref, left_ref, corner_ref,
    ones_ref, mask_ref, e_ref, o_ref,
):
    rows, _, cols, _, _ = state_ref.shape
    width = we_ref.shape[1]
    tokens = WIN * WIN
    chunk = cols * tokens
    ones_ref[...] = head_ones(width, width // HEADS)
    mask_ref[...] = head_stack(HEADS, tokens, width)

    def body(i, _):
        x = jnp.concatenate([window(state_ref, i, w).astype(BF) for w in range(cols)], axis=0)
        h0 = nn(x, we_ref[...])
        here = pl.ds(pl.multiple_of(i * chunk, chunk), chunk)
        h0_ref[here, :] = h0
        qkv = nn(norm(h0, gain_ref[0:1]), wqkv_ref[0]).astype(BF)
        qkv_ref[here, :] = qkv
        mixed = attention_chunk(
            qkv, scale_ref[...], ones_ref, mask_ref, None, e_ref, o_ref, cols, tokens
        )
        hm = h0 + nn(mixed, wproj_ref[0]).astype(BF).astype(F32)
        hm_ref[here, :] = hm
        inner, slope = gelu_parts(nn(norm(hm, gain_ref[1:2]), wup_ref[0]))
        gp_ref[here, :] = slope.astype(BF)
        h1 = hm + nn(inner.astype(BF), wdown_ref[0])
        z1 = norm(h1, gain_ref[2:3]).astype(F32)
        for w in range(cols):
            part = slice(w * tokens, (w + 1) * tokens)
            h1_ref[i, :, w, :, :] = h1[part].reshape(WIN, WIN, width)
            z1_ref[i, :, w, :, :] = z1[part].reshape(WIN, WIN, width)
        return 0

    lax.fori_loop(0, rows, body, 0)
    top_ref[...] = z1_ref[0, 0:SHIFT, :, :, :].astype(BF)
    left_ref[...] = z1_ref[:, :, 0, 0:SHIFT, :].astype(BF)
    corner_ref[...] = z1_ref[0, 0:SHIFT, 0, 0:SHIFT, :].astype(BF)


def first_block(state5, we, gains, wqkv, wproj, scale, wup, wdown):
    wr, _, wc, _, _ = state5.shape
    width = we.shape[1]
    tokens = wr * wc * WIN * WIN
    chunk = wc * WIN * WIN
    sh = jax.ShapeDtypeStruct
    outs = (
        sh((wr, WIN, wc, WIN, width), F32),
        sh((wr, WIN, wc, WIN, width), F32),
        sh((tokens, width), F32),
        sh((tokens, width), F32),
        sh((tokens, 3 * width), BF),
        sh((tokens, wup.shape[2]), BF),
        sh((SHIFT, wc, WIN, width), BF),
        sh((wr, WIN, SHIFT, width), BF),
        sh((SHIFT, SHIFT, width), BF),
    )
    return pl.pallas_call(
        first_kernel,
        out_shape=outs,
        in_specs=[VMEM] * 8,
        out_specs=(VMEM,) * len(outs),
        compiler_params=limit(LIMIT_FIRST),
        cost_estimate=cost(2e9),
        scratch_shapes=[
            pltpu.VMEM((width, width), BF),
            pltpu.VMEM((HEADS * WIN * WIN, width), BF),
            pltpu.VMEM((chunk, HEADS * WIN * WIN), BF),
            pltpu.VMEM((chunk, width), F32),
        ],
        name="first_block",
    )(state5, we, gains, wqkv, wproj, scale, wup, wdown)


def fill_ahead(pad_ref, own, right_ref, below_ref, corner_ref):
    rows, cols, _ = own.shape
    pad_ref[0:rows, 0:cols, :] = own
    pad_ref[0:rows, cols : cols + SHIFT, :] = right_ref[...].astype(F32)
    pad_ref[rows : rows + SHIFT, 0:cols, :] = below_ref[...].astype(F32)
    pad_ref[rows : rows + SHIFT, cols : cols + SHIFT, :] = corner_ref[...].astype(F32)


def rolled_window(pad_ref, i, w):
    block = pad_ref[
        pl.ds(i * WIN + SHIFT, WIN), SHIFT + w * WIN : SHIFT + (w + 1) * WIN, :
    ]
    return block.reshape(WIN * WIN, block.shape[2])


def emit_behind(out_ref, low_ref, east_ref, corner_ref):
    rows, cols, _ = out_ref.shape
    low_ref[...] = out_ref[rows - SHIFT : rows, :, :].astype(BF)
    east_ref[...] = out_ref[:, cols - SHIFT : cols, :].astype(BF)
    corner_ref[...] = out_ref[rows - SHIFT : rows, cols - SHIFT : cols, :].astype(BF)


def shifted_kernel(
    total_rows, start_ref, z1_ref, right_ref, below_ref, corner_ref, wqkv_ref, wproj_ref, scale_ref,
    ans_ref, low_ref, east_ref, last_ref, qkv_ref,
    pad_ref, ones_ref, mask_ref, e_ref, o_ref,
):
    rows, cols, width = z1_ref.shape
    wr, wc = rows // WIN, cols // WIN
    tokens = WIN * WIN
    chunk = wc * tokens
    ones_ref[...] = head_ones(width, width // HEADS)
    mask_ref[...] = head_stack(HEADS, tokens, width)
    fill_ahead(pad_ref, z1_ref[...], right_ref, below_ref, corner_ref)
    threshold = total_rows - SHIFT - start_ref[0]

    def body(i, _):
        z = jnp.concatenate([rolled_window(pad_ref, i, w).astype(BF) for w in range(wc)], axis=0)
        qkv = nn(z, wqkv_ref[1]).astype(BF)
        qkv_ref[pl.ds(pl.multiple_of(i * chunk, chunk), chunk), :] = qkv
        allowed = side_mask(i, threshold, tokens)
        mixed = attention_chunk(
            qkv, scale_ref[...], ones_ref, mask_ref, allowed, e_ref, o_ref, wc, tokens
        )
        answer = nn(mixed, wproj_ref[1]).astype(BF).astype(F32)
        for w in range(wc):
            ans_ref[pl.ds(i * WIN, WIN), w * WIN : (w + 1) * WIN, :] = answer[
                w * tokens : (w + 1) * tokens
            ].reshape(WIN, WIN, width)
        return 0

    lax.fori_loop(0, wr, body, 0)
    emit_behind(ans_ref, low_ref, east_ref, last_ref)


def behind_shapes(rows, cols, width):
    sh = jax.ShapeDtypeStruct
    return (
        sh((rows, cols, width), F32),
        sh((SHIFT, cols, width), BF),
        sh((rows, SHIFT, width), BF),
        sh((SHIFT, SHIFT, width), BF),
    )


def shifted_forward(start, z1, right, below, corner, wqkv, wproj, scale, total_rows):
    rows, cols, width = z1.shape
    tokens = rows * cols
    chunk = cols * WIN
    outs = behind_shapes(rows, cols, width) + (jax.ShapeDtypeStruct((tokens, 3 * width), BF),)
    return pl.pallas_call(
        functools.partial(shifted_kernel, total_rows),
        out_shape=outs,
        in_specs=[SMEM] + [VMEM] * 7,
        out_specs=(VMEM,) * len(outs),
        compiler_params=limit(LIMIT_SHIFTED),
        cost_estimate=cost(1e9),
        scratch_shapes=[
            pltpu.VMEM((rows + SHIFT, cols + WIN, width), F32),
            pltpu.VMEM((width, width), BF),
            pltpu.VMEM((HEADS * WIN * WIN, width), BF),
            pltpu.VMEM((chunk, HEADS * WIN * WIN), BF),
            pltpu.VMEM((chunk, width), F32),
        ],
        name="shifted_forward",
    )(start, z1, right, below, corner, wqkv, wproj, scale)


def fill_behind(pad_ref, own, above_ref, west_ref, corner_ref):
    rows, cols, _ = own.shape
    pad_ref[SHIFT : SHIFT + rows, SHIFT : SHIFT + cols, :] = own
    pad_ref[0:SHIFT, SHIFT : SHIFT + cols, :] = above_ref[...].astype(F32)
    pad_ref[SHIFT : SHIFT + rows, 0:SHIFT, :] = west_ref[...].astype(F32)
    pad_ref[0:SHIFT, 0:SHIFT, :] = corner_ref[...].astype(F32)


def group_jobs(cnt_smem, offset, size, group, body):
    devices = cnt_smem.shape[0]

    def each(d, _):
        valid = jnp.minimum(cnt_smem[d, 0] - offset, size)

        def some(g, _):
            body(d, offset + g * group, d * size + g * group)
            return 0

        lax.fori_loop(0, (jnp.maximum(valid, 0) + group - 1) // group, some, 0)
        return 0

    lax.fori_loop(0, devices, each, 0)


def gather_part(table_ref, found_ref, idx_smem, cnt_smem, offset, size, group):
    def body(d, slot, row):
        row = pl.multiple_of(row, group)
        for u in range(group):
            found_ref[pl.ds(row + u, 1), :] = table_ref[pl.ds(idx_smem[d, slot + u], 1), :]

    group_jobs(cnt_smem, offset, size, group, body)


def scatter_part(table_ref, found_ref, idx_smem, cnt_smem, dup_smem, offset, size, group):
    def body(d, slot, row):
        row = pl.multiple_of(row, group)
        spots = [idx_smem[d, slot + u] for u in range(group)]

        @pl.when(dup_smem[d, slot] == 0)
        def _():
            sums = [
                table_ref[pl.ds(spots[u], 1), :] + found_ref[pl.ds(row + u, 1), :]
                for u in range(group)
            ]
            for u in range(group):
                table_ref[pl.ds(spots[u], 1), :] = sums[u]

        @pl.when(dup_smem[d, slot] != 0)
        def _():
            for u in range(group):
                table_ref[pl.ds(spots[u], 1), :] = (
                    table_ref[pl.ds(spots[u], 1), :] + found_ref[pl.ds(row + u, 1), :]
                )

    group_jobs(cnt_smem, offset, size, group, body)


def radiance_part(found_ref, obs_ref, mixed_ref, w1_ref, size):
    devices, _, channels = obs_ref.shape
    batch = min(devices, max(1, 512 // size))

    def body(i, _):
        here = pl.ds(pl.multiple_of(i * batch * size, batch * size), batch * size)
        y = obs_ref[pl.ds(i * batch, batch), 0:size, :].astype(F32)
        y = y.reshape(batch * size, channels)
        t = jnp.tanh(nn(found_ref[here, :].astype(BF), w1_ref[...]))
        pulled = (nn(t.astype(BF), mixed_ref[...]) - y) * (1.0 - t * t)
        found_ref[here, :] = nt(pulled.astype(BF), w1_ref[...])
        return 0

    lax.fori_loop(0, devices // batch, body, 0)


def forecast_kernel(
    parts, group, h1_ref, ans_ref, above_ref, west_ref, corner_ref, state_ref, back_ref, inv_ref,
    obs1_ref, obs2_ref, mixed_ref, gain_ref, wup_ref, wdown_ref, whead_ref, w1_ref,
    h2_ref, gp_ref, prior_hbm, sums_hbm, found3_ref, idx_ref, cnt_ref, dup_ref,
    pad_ref, table_ref, found1_ref, found2_ref, prior_ref,
    idx_smem, cnt_smem, dup_smem, sems, prior_sem, sums_sem,
):
    rows, cols, width = h1_ref.shape
    devices = obs1_ref.shape[0]
    tokens = rows * cols
    step = tokens // 2

    codes = obs1_ref[:, parts[0] : parts[0] + EXTRA, :].astype(F32)[:, 0, :]
    high = codes[:, :LANES].astype(jnp.int32)
    low = codes[:, LANES : 2 * LANES].astype(jnp.int32)
    point = jnp.where(high > 0, (high - 1) * LANES + low, 0)
    lane = lax.broadcasted_iota(jnp.int32, (devices, LANES), 1)
    idx = jnp.where(
        high > 0, (point % PIX) * tokens + point // PIX, PIX * tokens + lane % group
    )
    idx_ref[...] = idx
    cnt_ref[...] = jnp.broadcast_to(
        jnp.sum(jnp.where(high > 0, 1.0, 0.0), 1, keepdims=True), (devices, LANES)
    ).astype(jnp.int32)
    same = jnp.zeros((devices, LANES), jnp.int32)
    for s in range(1, group):
        hit = (pltpu.roll(idx, s, 1) == idx) & (lane % group >= s)
        same = jnp.maximum(same, jnp.where(hit, 1, 0))
    s = group // 2
    while s:
        same = jnp.maximum(same, pltpu.roll(same, LANES - s, 1))
        s //= 2
    dup_ref[...] = same
    copies = [
        pltpu.make_async_copy(a, b, sems.at[n])
        for n, (a, b) in enumerate(
            ((idx_ref, idx_smem), (cnt_ref, cnt_smem), (dup_ref, dup_smem))
        )
    ]
    for copy in copies:
        copy.start()
    prior_ref[...] = inv_ref[...] * (state_ref[...] - back_ref[...])
    prior_copy = pltpu.make_async_copy(prior_ref, prior_hbm, prior_sem)
    prior_copy.start()

    fill_behind(pad_ref, ans_ref[...], above_ref, west_ref, corner_ref)
    h2_ref[...] = (h1_ref[...] + pad_ref[0:rows, 0:cols, :]).reshape(tokens, width)
    table_ref[...] = jnp.zeros_like(table_ref)

    def forward(i, _):
        here = pl.ds(pl.multiple_of(i * step, step), step)
        h2 = h2_ref[here, :]
        inner, slope = gelu_parts(nn(norm(h2, gain_ref[3:4]), wup_ref[1]))
        gp_ref[here, :] = slope.astype(BF)
        h3 = (h2 + nn(inner.astype(BF), wdown_ref[1])).astype(BF)
        for s in range(PIX):
            lifted = nn(h3, whead_ref[:, s * LANES : (s + 1) * LANES])
            there = pl.ds(pl.multiple_of(s * tokens + i * step, WIN), step)
            table_ref[there, 0:VARS] = (
                state_ref[here, s * VARS : (s + 1) * VARS] + lifted[:, 0:VARS]
            )
        return 0

    lax.fori_loop(0, 2, forward, 0)
    for copy in copies:
        copy.wait()
    offsets = (0, parts[0], parts[0] + parts[1])
    founds = (found1_ref, found2_ref, found3_ref)
    for offset, size, found in zip(offsets, parts, founds):
        gather_part(table_ref, found, idx_smem, cnt_smem, offset, size, group)
    table_ref[...] = jnp.zeros_like(table_ref)
    radiance_part(found1_ref, obs1_ref, mixed_ref, w1_ref, parts[0])
    scatter_part(table_ref, found1_ref, idx_smem, cnt_smem, dup_smem, 0, parts[0], group)
    radiance_part(found2_ref, obs2_ref, mixed_ref, w1_ref, parts[1])
    scatter_part(table_ref, found2_ref, idx_smem, cnt_smem, dup_smem, parts[0], parts[1], group)
    sums_copy = pltpu.make_async_copy(table_ref, sums_hbm, sums_sem)
    sums_copy.start()
    prior_copy.wait()
    sums_copy.wait()


def forecast(
    h1, ans, above, west, corner, state, background, inv, obs1, obs2, mixed, gains, wup, wdown,
    whead, w1, parts, group,
):
    rows, cols, width = h1.shape
    tokens = rows * cols
    devices = obs1.shape[0]
    sh = jax.ShapeDtypeStruct
    outs = (
        sh((tokens, width), F32),
        sh((tokens, wup.shape[2]), BF),
        sh(state.shape, F32),
        sh((PIX * tokens + group, LANES), F32),
        sh((devices * parts[2], LANES), F32),
    ) + (sh((devices, LANES), jnp.int32),) * 3
    return pl.pallas_call(
        functools.partial(forecast_kernel, parts, group),
        out_shape=outs,
        in_specs=[VMEM] * 16,
        out_specs=(VMEM, VMEM, ANY, ANY) + (VMEM,) * 4,
        scratch_shapes=[
            pltpu.VMEM((rows + SHIFT, cols + WIN, width), F32),
            pltpu.VMEM((PIX * tokens + group, LANES), F32),
            pltpu.VMEM((devices * parts[0], LANES), F32),
            pltpu.VMEM((devices * parts[1], LANES), F32),
            pltpu.VMEM(state.shape, F32),
        ]
        + [pltpu.SMEM((devices, LANES), jnp.int32)] * 3
        + [
            pltpu.SemaphoreType.DMA((3,)),
            pltpu.SemaphoreType.DMA,
            pltpu.SemaphoreType.DMA,
        ],
        compiler_params=limit(LIMIT_FORECAST),
        cost_estimate=cost(3e9),
        name="forecast",
    )(
        h1, ans, above, west, corner, state, background, inv, obs1, obs2, mixed, gains, wup,
        wdown, whead, w1,
    )


def adjoint_kernel(
    parts, group, idx_smem, cnt_smem, dup_smem, found_ref, obs3_ref, mixed_ref, w1_ref,
    h2_ref, gp_ref, gain_ref, wup_ref, wdown_ref, whead_ref, prior_hbm, sums_hbm,
    out_ref, third_ref, top_ref, left_ref, edge_ref,
    table_ref, work_ref, prior_ref, sums_sem, prior_sem,
):
    rows, cols, width = third_ref.shape
    tokens = rows * cols
    step = tokens // 2
    sums_copy = pltpu.make_async_copy(sums_hbm, table_ref, sums_sem)
    sums_copy.start()
    prior_copy = pltpu.make_async_copy(prior_hbm, prior_ref, prior_sem)
    prior_copy.start()
    work_ref[...] = found_ref[...]
    radiance_part(work_ref, obs3_ref, mixed_ref, w1_ref, parts[2])
    sums_copy.wait()
    scatter_part(
        table_ref, work_ref, idx_smem, cnt_smem, dup_smem, parts[0] + parts[1], parts[2], group
    )
    prior_copy.wait()

    def backward(i, _):
        here = pl.ds(pl.multiple_of(i * step, step), step)
        grad = None
        for s in range(0, PIX, 2):
            both = []
            for n in (s, s + 1):
                there = pl.ds(pl.multiple_of(n * tokens + i * step, WIN), step)
                part = table_ref[there, :]
                lanes = slice(n * VARS, (n + 1) * VARS)
                out_ref[here, lanes] = part[:, 0:VARS] + prior_ref[here, lanes]
                both.append(part.astype(BF))
            add = nt(jnp.concatenate(both, axis=1), whead_ref[:, s * LANES : (s + 2) * LANES])
            grad = add if grad is None else grad + add
        grad = grad.astype(BF)
        d_inner = nt(grad, wdown_ref[1]) * gp_ref[here, :].astype(F32)
        d_normed = nt(d_inner.astype(BF), wup_ref[1])
        third = grad.astype(F32) + norm_back(h2_ref[here, :], gain_ref[3:4], d_normed)
        third_ref[pl.ds(i * (rows // 2), rows // 2), :, :] = third.reshape(rows // 2, cols, width)
        return 0

    lax.fori_loop(0, 2, backward, 0)
    top_ref[...] = third_ref[0:SHIFT, :, :].astype(BF)
    left_ref[...] = third_ref[:, 0:SHIFT, :].astype(BF)
    edge_ref[...] = third_ref[0:SHIFT, 0:SHIFT, :].astype(BF)


def adjoint(
    idx, cnt, dup, found, obs3, mixed, w1, h2, gp, gains, wup, wdown, whead, prior, sums, parts,
    group, rows, cols,
):
    width = h2.shape[1]
    outs = (jax.ShapeDtypeStruct(prior.shape, F32),) + behind_shapes(rows, cols, width)
    return pl.pallas_call(
        functools.partial(adjoint_kernel, parts, group),
        out_shape=outs,
        in_specs=[SMEM] * 3 + [VMEM] * 10 + [ANY] * 2,
        out_specs=(VMEM,) * len(outs),
        scratch_shapes=[
            pltpu.VMEM(sums.shape, F32),
            pltpu.VMEM(found.shape, F32),
            pltpu.VMEM(prior.shape, F32),
            pltpu.SemaphoreType.DMA,
            pltpu.SemaphoreType.DMA,
        ],
        compiler_params=limit(LIMIT_ADJOINT),
        cost_estimate=cost(2e9),
        name="adjoint",
    )(idx, cnt, dup, found, obs3, mixed, w1, h2, gp, gains, wup, wdown, whead, prior, sums)


def shifted_back_kernel(
    total_rows, start_ref, third_ref, right_ref, below_ref, corner_ref, qkv_ref,
    wqkv_ref, wproj_ref, scale_ref,
    dz_ref, low_ref, east_ref, last_ref,
    pad_ref, ones_ref, mask_ref, dq_ref, dk_ref, dv_ref,
):
    rows, cols, width = third_ref.shape
    wr, wc = rows // WIN, cols // WIN
    tokens = WIN * WIN
    chunk = wc * tokens
    ones_ref[...] = head_ones(width, width // HEADS)
    mask_ref[...] = head_stack(HEADS, tokens, width)
    fill_ahead(pad_ref, third_ref[...], right_ref, below_ref, corner_ref)
    threshold = total_rows - SHIFT - start_ref[0]

    def body(i, _):
        d_answer = jnp.concatenate(
            [rolled_window(pad_ref, i, w).astype(BF) for w in range(wc)], axis=0
        )
        d_out = nt(d_answer, wproj_ref[1]).astype(BF)
        allowed = side_mask(i, threshold, tokens)
        qkv = qkv_ref[pl.ds(pl.multiple_of(i * chunk, chunk), chunk), :]
        d_qkv = attention_chunk_back(
            qkv, d_out, scale_ref[...], ones_ref, mask_ref, allowed,
            dq_ref, dk_ref, dv_ref, wc, tokens,
        )
        dz = nt(d_qkv, wqkv_ref[1]).astype(BF).astype(F32)
        for w in range(wc):
            dz_ref[pl.ds(i * WIN, WIN), w * WIN : (w + 1) * WIN, :] = dz[
                w * tokens : (w + 1) * tokens
            ].reshape(WIN, WIN, width)
        return 0

    lax.fori_loop(0, wr, body, 0)
    emit_behind(dz_ref, low_ref, east_ref, last_ref)


def shifted_backward(start, third, right, below, corner, qkv, wqkv, wproj, scale, total_rows):
    rows, cols, width = third.shape
    chunk = cols * WIN
    outs = behind_shapes(rows, cols, width)
    return pl.pallas_call(
        functools.partial(shifted_back_kernel, total_rows),
        out_shape=outs,
        in_specs=[SMEM] + [VMEM] * 8,
        out_specs=(VMEM,) * len(outs),
        compiler_params=limit(LIMIT_BACK),
        cost_estimate=cost(1e9),
        scratch_shapes=[
            pltpu.VMEM((rows + SHIFT, cols + WIN, width), F32),
            pltpu.VMEM((width, width), BF),
            pltpu.VMEM((HEADS * WIN * WIN, width), BF),
        ]
        + [pltpu.VMEM((chunk, width), F32)] * 3,
        name="shifted_backward",
    )(start, third, right, below, corner, qkv, wqkv, wproj, scale)


def last_kernel(
    third_ref, dz_ref, above_ref, west_ref, corner_ref, h1_ref, h0_ref, hm_ref, qkv_ref, gp_ref,
    we_ref, gain_ref, wqkv_ref, wproj_ref, scale_ref, wup_ref, wdown_ref, partial_hbm,
    out_hbm,
    pad_ref, ones_ref, mask_ref, dq_ref, dk_ref, dv_ref, out_ref, in_sems, out_sems,
):
    rows, cols, width = dz_ref.shape
    wr, wc = rows // WIN, cols // WIN
    tokens = WIN * WIN
    chunk = wc * tokens

    def rows_of(ref, i):
        return ref.at[pl.ds(i * WIN, WIN)]

    for i in range(wr):
        pltpu.make_async_copy(rows_of(partial_hbm, i), rows_of(out_ref, i), in_sems.at[i]).start()
    ones_ref[...] = head_ones(width, width // HEADS)
    mask_ref[...] = head_stack(HEADS, tokens, width)
    fill_behind(pad_ref, dz_ref[...], above_ref, west_ref, corner_ref)

    def body(i, _):
        here = pl.ds(pl.multiple_of(i * chunk, chunk), chunk)
        band = pl.ds(i * WIN, WIN)

        def take(ref):
            return jnp.concatenate(
                [
                    ref[band, w * WIN : (w + 1) * WIN, :].reshape(tokens, width)
                    for w in range(wc)
                ],
                axis=0,
            )

        second = take(third_ref) + norm_back(take(h1_ref), gain_ref[2:3], take(pad_ref))
        d_inner = nt(second.astype(BF), wdown_ref[0]) * gp_ref[here, :].astype(F32)
        d_normed = nt(d_inner.astype(BF), wup_ref[0])
        d_hm = second + norm_back(hm_ref[here, :], gain_ref[1:2], d_normed)
        d_out = nt(d_hm.astype(BF), wproj_ref[0]).astype(BF)
        d_qkv = attention_chunk_back(
            qkv_ref[here, :], d_out, scale_ref[...], ones_ref, mask_ref, None,
            dq_ref, dk_ref, dv_ref, wc, tokens,
        )
        dz = nt(d_qkv, wqkv_ref[0])
        d_h0 = (d_hm + norm_back(h0_ref[here, :], gain_ref[0:1], dz)).astype(BF)
        pltpu.make_async_copy(rows_of(partial_hbm, i), rows_of(out_ref, i), in_sems.at[i]).wait()
        for w in range(wc):
            grad = nt(d_h0[w * tokens : (w + 1) * tokens], we_ref[...])
            grad = grad.reshape(WIN, WIN, grad.shape[1])
            spot = (band, slice(w * WIN, (w + 1) * WIN), slice(None))
            out_ref[spot] = grad + out_ref[spot]
        pltpu.make_async_copy(rows_of(out_ref, i), rows_of(out_hbm, i), out_sems.at[i]).start()
        return 0

    lax.fori_loop(0, wr, body, 0)
    for i in range(wr):
        pltpu.make_async_copy(rows_of(out_ref, i), rows_of(out_hbm, i), out_sems.at[i]).wait()


def last_block(
    third, dz, above, west, corner, h1, h0, hm, qkv, gp, we, gains, wqkv, wproj, scale,
    wup, wdown, partial,
):
    rows, cols, width = dz.shape
    chunk = cols * WIN
    args = (
        third, dz, above, west, corner, h1, h0, hm, qkv, gp, we, gains, wqkv, wproj, scale,
        wup, wdown, partial,
    )
    out = jax.ShapeDtypeStruct(partial.shape, F32)
    return pl.pallas_call(
        last_kernel,
        out_shape=out,
        in_specs=[VMEM] * (len(args) - 1) + [ANY],
        out_specs=ANY,
        compiler_params=limit(LIMIT_LAST),
        cost_estimate=cost(2e9),
        scratch_shapes=[
            pltpu.VMEM((rows + SHIFT, cols + WIN, width), F32),
            pltpu.VMEM((width, width), BF),
            pltpu.VMEM((HEADS * WIN * WIN, width), BF),
        ]
        + [pltpu.VMEM((chunk, width), F32)] * 3
        + [
            pltpu.VMEM(partial.shape, F32),
            pltpu.SemaphoreType.DMA((rows // WIN,)),
            pltpu.SemaphoreType.DMA((rows // WIN,)),
        ],
        name="last_block",
    )(*args)


def neighbour(x, by_lat, by_lon):
    lat, lon = lax.axis_size("lat"), lax.axis_size("lon")
    pairs = [
        (a * lon + b, ((a + by_lat) % lat) * lon + (b + by_lon) % lon)
        for a in range(lat)
        for b in range(lon)
    ]
    return lax.ppermute(x, ("lat", "lon"), pairs)


def exchange(x):
    return lax.all_to_all(x, ("lat", "lon"), split_axis=0, concat_axis=0, tiled=True)


def local(
    state,
    background,
    inv_background,
    w_embed,
    norm_gain,
    w_qkv,
    w_proj,
    head_scale,
    w_up,
    w_down,
    w_head,
    w_obs1,
    w_obs2,
    r_inverse,
    obs_values,
    obs_owner,
    obs_point,
    obs_count,
):
    rows, cols, patch_values = state.shape
    width = w_embed.shape[1]
    total_rows = rows * lax.axis_size("lat")
    row_start = (lax.axis_index("lat") * rows).astype(jnp.int32).reshape(1)
    devices = lax.axis_size("lat") * lax.axis_size("lon")
    slots = obs_values.shape[0]
    cap = 2 * slots // devices

    parts, group = split(cap)

    send1, send2, send3, mixed = route(
        obs_owner.reshape(1, slots), obs_point.reshape(1, slots), obs_count, obs_values,
        r_inverse, w_obs2, devices, parts,
    )
    gains = norm_gain.reshape(-1, width)
    send1, gains = lax.optimization_barrier((send1, gains))
    obs1 = exchange(send1)
    scales = jnp.repeat(head_scale, width // HEADS, axis=1)
    w1 = jnp.pad(w_obs1, ((0, LANES - VARS), (0, 0))).astype(BF)
    whead = jnp.pad(w_head.reshape(width, PIX, VARS), ((0, 0), (0, 0), (0, LANES - VARS)))
    whead = whead.reshape(width, PIX * LANES)

    state5 = state.reshape(rows // WIN, WIN, cols // WIN, WIN, patch_values)
    z1, h1, h0, hm, qkv0, gp0, top, left, corner = first_block(
        state5, w_embed, gains, w_qkv, w_proj, scales[0:1], w_up, w_down
    )
    z1 = z1.reshape(rows, cols, width)
    h1 = h1.reshape(rows, cols, width)
    below = neighbour(top.reshape(SHIFT, cols, width), -1, 0)
    right = neighbour(left.reshape(rows, SHIFT, width), 0, -1)
    corner = neighbour(corner, -1, -1)
    below, right, corner, obs1, send2 = lax.optimization_barrier(
        (below, right, corner, obs1, send2)
    )
    obs2 = exchange(send2)
    answer, low, east, last, qkv1 = shifted_forward(
        row_start, z1, right, below, corner, w_qkv, w_proj, scales[1:2], total_rows
    )
    above = neighbour(low, 1, 0)
    west = neighbour(east, 0, 1)
    last = neighbour(last, 1, 1)
    above, west, last, obs2, send3 = lax.optimization_barrier((above, west, last, obs2, send3))
    obs3 = exchange(send3)
    flat = (rows * cols, patch_values)
    h2, gp1, prior, sums, found, idx, cnt, dup = forecast(
        h1, answer, above, west, last, state.reshape(flat), background.reshape(flat),
        inv_background.reshape(1, -1), obs1, obs2, mixed, gains, w_up, w_down, whead, w1,
        parts, group,
    )
    partial, third, top, left, corner = adjoint(
        idx, cnt, dup, found, obs3, mixed, w1, h2, gp1, gains, w_up, w_down, whead, prior, sums,
        parts, group, rows, cols,
    )
    below = neighbour(top, -1, 0)
    right = neighbour(left, 0, -1)
    corner = neighbour(corner, -1, -1)
    dz, low, east, last = shifted_backward(
        row_start, third, right, below, corner, qkv1, w_qkv, w_proj, scales[1:2], total_rows
    )
    above = neighbour(low, 1, 0)
    west = neighbour(east, 0, 1)
    last = neighbour(last, 1, 1)
    return last_block(
        third, dz, above, west, last, h1, h0, hm, qkv0, gp0, w_embed, gains, w_qkv, w_proj,
        scales[0:1], w_up, w_down, partial.reshape(state.shape),
    )


def solution(mesh):
    placed = (
        P("lat", "lon", None),
        P("lat", "lon", None),
        P(),
        P(),
        P(),
        P(),
        P(),
        P(),
        P(),
        P(),
        P(),
        P(),
        P(),
        P(),
        P(("lat", "lon"), None),
        P(("lat", "lon"), None),
        P(("lat", "lon")),
        P(("lat", "lon")),
    )
    return jax.shard_map(
        local, mesh=mesh, in_specs=placed, out_specs=P("lat", "lon", None), check_vma=False
    )
```

```python
import functools

import jax
import jax.numpy as jnp
from jax import lax
from jax.experimental import pallas as pl
from jax.experimental.pallas import tpu as pltpu
from jax.sharding import PartitionSpec as P

HEADS = 8
VARS = 69
PIX = 16
WIN = 8
SHIFT = 4
LANES = 128
EXTRA = 8
EPS = 1e-05
BF = jnp.bfloat16
F32 = jnp.float32
SQRT_2_OVER_PI = 0.7978845608028654
CUBIC = 0.044715

SMEM = pl.BlockSpec(memory_space=pltpu.SMEM)
HBM = pl.BlockSpec(memory_space=pltpu.HBM)
MIB = 1024 * 1024


class Stage:
    def __init__(self):
        self.inputs = {}
        self.outputs = {}
        self.waited = set()
        self.sent = set()

    def need(self, *refs):
        for ref in refs:
            if id(ref) not in self.waited:
                self.waited.add(id(ref))
                self.inputs[id(ref)].wait()

    def emit(self, *refs):
        for ref in refs:
            if id(ref) not in self.sent:
                self.sent.add(id(ref))
                self.outputs[id(ref)].start()

    def close(self):
        for key, copy in self.inputs.items():
            if key not in self.waited:
                copy.wait()
        for key, copy in self.outputs.items():
            if key not in self.sent:
                copy.start()
        for copy in self.outputs.values():
            copy.wait()


def staged(body, name, args, outs, scratch, flops, smem=(), raw=(), raw_outs=(), layer=None):
    layer = layer or {}
    count = len(args)
    in_buffers = []
    for i, x in enumerate(args):
        if i not in smem and i not in raw:
            shape = x.shape[1:] if i in layer else x.shape
            in_buffers.append((i, pltpu.VMEM(shape, x.dtype)))
    out_buffers = [
        (j, pltpu.VMEM(o.shape, o.dtype)) for j, o in enumerate(outs) if j not in raw_outs
    ]

    def kernel(*refs):
        ins = list(refs[:count])
        results = list(refs[count : count + len(outs)])
        rest = list(refs[count + len(outs) :])
        ins_vmem = rest[: len(in_buffers)]
        outs_vmem = rest[len(in_buffers) : len(in_buffers) + len(out_buffers)]
        in_sems, out_sems = rest[-2:]
        extra = rest[len(in_buffers) + len(out_buffers) : -2]
        stage = Stage()
        for n, ((i, _), buffer) in enumerate(zip(in_buffers, ins_vmem)):
            source = ins[i].at[layer[i]] if i in layer else ins[i]
            copy = pltpu.make_async_copy(source, buffer, in_sems.at[n])
            copy.start()
            stage.inputs[id(buffer)] = copy
            ins[i] = buffer
        for n, ((j, _), buffer) in enumerate(zip(out_buffers, outs_vmem)):
            stage.outputs[id(buffer)] = pltpu.make_async_copy(buffer, results[j], out_sems.at[n])
            results[j] = buffer
        body(stage, *ins, *results, *extra)
        stage.close()

    return pl.pallas_call(
        kernel,
        out_shape=tuple(outs),
        in_specs=[SMEM if i in smem else HBM for i in range(count)],
        out_specs=(HBM,) * len(outs),
        scratch_shapes=[b for _, b in in_buffers]
        + [b for _, b in out_buffers]
        + list(scratch)
        + [
            pltpu.SemaphoreType.DMA((max(1, len(in_buffers)),)),
            pltpu.SemaphoreType.DMA((max(1, len(out_buffers)),)),
        ],
        compiler_params=pltpu.CompilerParams(vmem_limit_bytes=60 * MIB),
        cost_estimate=pl.CostEstimate(
            flops=int(flops), bytes_accessed=8 * MIB, transcendentals=0
        ),
        name=name,
    )(*args)


def scale_lanes(scale_ref, block, width):
    head = lax.broadcasted_iota(jnp.int32, (1, width), 1) // (width // HEADS)
    row = jnp.zeros((1, width), F32)
    for h in range(HEADS):
        row = jnp.where(head == h, scale_ref[block, h], row)
    return row


def nn(a, b):
    return lax.dot_general(a, b, (((1,), (0,)), ((), ())), preferred_element_type=F32)


def nt(a, b):
    return lax.dot_general(a, b, (((1,), (1,)), ((), ())), preferred_element_type=F32)


def tn(a, b):
    return lax.dot_general(a, b, (((0,), (0,)), ((), ())), preferred_element_type=F32)


def norm_parts(h):
    mean = jnp.mean(h, -1, keepdims=True)
    centred = h - mean
    spread = jnp.mean(centred * centred, -1, keepdims=True)
    rstd = lax.rsqrt(spread + EPS)
    return centred * rstd, rstd


def norm(h, gain):
    return (norm_parts(h)[0] * gain).astype(BF)


def norm_back(h, gain, cotangent):
    xhat, rstd = norm_parts(h)
    scaled = cotangent * gain
    m1 = jnp.mean(scaled, -1, keepdims=True)
    m2 = jnp.mean(scaled * xhat, -1, keepdims=True)
    return rstd * (scaled - m1 - xhat * m2)


def gelu_parts(u):
    square = u * u
    t = jnp.tanh(SQRT_2_OVER_PI * u * (1.0 + CUBIC * square))
    half = 0.5 * (1.0 + t)
    slope = half + 0.5 * u * (1.0 - t * t) * (
        SQRT_2_OVER_PI * (1.0 + 3.0 * CUBIC * square)
    )
    return u * half, slope


def head_ones(width, size):
    a = lax.broadcasted_iota(jnp.int32, (width, width), 0) // size
    b = lax.broadcasted_iota(jnp.int32, (width, width), 1) // size
    return (a == b).astype(F32).astype(BF)


def head_stack(heads, tokens, width):
    size = width // heads
    a = lax.broadcasted_iota(jnp.int32, (heads * tokens, width), 0) // tokens
    b = lax.broadcasted_iota(jnp.int32, (heads * tokens, width), 1) // size
    return (a == b).astype(F32).astype(BF)


def stacked(x, mask):
    return jnp.concatenate([x] * HEADS, axis=0) * mask


def side_mask(window_row, threshold, tokens):
    shape = (tokens, HEADS * tokens)
    a = lax.broadcasted_iota(jnp.int32, shape, 0) // WIN
    b = (lax.broadcasted_iota(jnp.int32, shape, 1) % tokens) // WIN
    first = (window_row * WIN + a) >= threshold
    second = (window_row * WIN + b) >= threshold
    return jnp.where(first == second, 1.0, 0.0).astype(F32)


def window(ref, i, w):
    block = ref[i, :, w, :, :]
    return block.reshape(block.shape[0] * block.shape[1], block.shape[2])


def attention_chunk(qkv, scale, ones_ref, mask_ref, allowed, e_ref, o_ref, count, tokens):
    width = qkv.shape[1] // 3
    q = qkv[:, :width].astype(F32)
    k = qkv[:, width : 2 * width].astype(F32)
    v = qkv[:, 2 * width :]
    ones = ones_ref[...]
    qs = (q * lax.rsqrt(nn((q * q).astype(BF), ones) + 1.0) * scale).astype(BF)
    kn = (k * lax.rsqrt(nn((k * k).astype(BF), ones) + 1.0)).astype(BF)
    mask = mask_ref[...]
    for w in range(count):
        part = slice(w * tokens, (w + 1) * tokens)
        expo = jnp.exp(nt(qs[part], stacked(kn[part], mask)))
        if allowed is not None:
            expo = expo * allowed
        expo = expo.astype(BF)
        e_ref[part] = expo
        o_ref[part] = nn(expo, stacked(v[part], mask))
    return (o_ref[...] / nn(e_ref[...], mask)).astype(BF)


def attention_chunk_back(
    qkv, d_out, scale, ones_ref, mask_ref, allowed, dq_ref, dk_ref, dv_ref, count, tokens
):
    width = qkv.shape[1] // 3
    size = width // HEADS
    q = qkv[:, :width].astype(F32)
    k = qkv[:, width : 2 * width].astype(F32)
    v = qkv[:, 2 * width :]
    ones = ones_ref[...]
    rq = lax.rsqrt(nn((q * q).astype(BF), ones) + 1.0)
    rk = lax.rsqrt(nn((k * k).astype(BF), ones) + 1.0)
    qs = (q * rq * scale).astype(BF)
    kn = (k * rk).astype(BF)
    mask = mask_ref[...]
    lane_head = lax.broadcasted_iota(jnp.int32, (1, LANES), 1) // size
    per_tile = LANES // size
    for w in range(count):
        part = slice(w * tokens, (w + 1) * tokens)
        kw = kn[part]
        qm = stacked(qs[part], mask)
        dm = stacked(d_out[part], mask)
        expo = jnp.exp(nt(kw, qm))
        if allowed is not None:
            expo = expo * allowed
        p = expo * (1.0 / jnp.sum(expo, 0, keepdims=True))
        dp = nt(v[part], dm)
        ds = (p * (dp - jnp.sum(p * dp, 0, keepdims=True))).astype(BF)
        dv_ref[part] = nn(p.astype(BF), dm)
        dk_ref[part] = nn(ds, qm)
        full = tn(ds, kw)
        tiles = []
        for tile in range(width // LANES):
            total = None
            for s in range(per_tile):
                h = tile * per_tile + s
                block = full[h * tokens : (h + 1) * tokens, tile * LANES : (tile + 1) * LANES]
                block = jnp.where(lane_head == s, block, 0.0)
                total = block if total is None else total + block
            tiles.append(total)
        dq_ref[part] = jnp.concatenate(tiles, axis=1)
    dqs = dq_ref[...]
    dkn = dk_ref[...]
    dq = scale * rq * (dqs - q * (rq * rq) * nn((q * dqs).astype(BF), ones))
    dk = rk * (dkn - k * (rk * rk) * nn((k * dkn).astype(BF), ones))
    return jnp.concatenate([dq.astype(BF), dk.astype(BF), dv_ref[...].astype(BF)], axis=1)


def split(cap):
    first = max(8, cap // 4)
    return (first, first, cap - 2 * first), min(32, first)


def route_kernel(
    parts, stage, count_ref, owner_ref, point_ref, r_ref, w2_ref, values_ref,
    send1_ref, send2_ref, send3_ref, mixed_ref, y_ref, buf_ref, tgt_ref, tgt_smem, sem,
):
    cap = sum(parts)
    slots = owner_ref.shape[1]
    devices = send1_ref.shape[0]
    stage.need(owner_ref, point_ref)
    owner = owner_ref[...]
    live = lax.broadcasted_iota(jnp.int32, (1, slots), 1) < count_ref[0]
    match = lax.broadcasted_iota(jnp.int32, (devices, slots), 0) == owner
    match = jnp.where(match, 1.0, 0.0).astype(F32)
    a = lax.broadcasted_iota(jnp.int32, (LANES, LANES), 0)
    b = lax.broadcasted_iota(jnp.int32, (LANES, LANES), 1)
    upper = jnp.where(a < b, 1.0, 0.0).astype(BF)
    chunks = slots // LANES
    flat = jnp.concatenate(
        [match[:, c * LANES : (c + 1) * LANES] for c in range(chunks)], axis=0
    )
    before = nn(flat.astype(BF), upper)
    carry = jnp.zeros((devices, 1), F32)
    ranks = []
    for c in range(chunks):
        here = match[:, c * LANES : (c + 1) * LANES]
        seen = before[c * devices : (c + 1) * devices] + carry
        ranks.append(jnp.sum(here * seen, 0, keepdims=True))
        carry = carry + jnp.sum(here, 1, keepdims=True)
    rank = jnp.concatenate(ranks, axis=1).astype(jnp.int32)
    tgt_ref[...] = jnp.where(live, owner * cap + rank, devices * cap)
    copy = pltpu.make_async_copy(tgt_ref, tgt_smem, sem)
    copy.start()
    place = lax.broadcasted_iota(jnp.int32, (cap, slots), 0) == rank
    place = jnp.where(place & live, 1.0, 0.0).astype(BF)
    point = point_ref[...]
    high = (match * (point // LANES + 1).astype(F32)).astype(BF)
    low = (match * (point % LANES).astype(F32)).astype(BF)
    high = nt(high, place)
    low = nt(low, place)
    stage.need(r_ref, w2_ref, values_ref)
    best = lax.Precision.HIGHEST
    dims = (((1,), (1,)), ((), ()))
    m2 = lax.dot_general(
        r_ref[...], w2_ref[...], dims, precision=best, preferred_element_type=F32
    )
    mixed_ref[...] = jnp.dot(
        w2_ref[...], m2, precision=best, preferred_element_type=F32
    ).astype(BF)
    y = nn(values_ref[...].astype(BF), m2.astype(BF))
    y_ref[0, :, :] = y[:, :LANES]
    y_ref[1, :, :] = y[:, LANES:]
    buf_ref[...] = jnp.zeros_like(buf_ref)
    copy.wait()
    unroll = 32

    def move(step, _):
        spots = [tgt_smem[0, step * unroll + u] for u in range(unroll)]
        base = pl.multiple_of(step * unroll, unroll)
        for half in range(2):
            for u in range(unroll):
                buf_ref[half, pl.ds(spots[u], 1), :] = y_ref[half, pl.ds(base + u, 1), :]
        return 0

    lax.fori_loop(0, slots // unroll, move, 0)
    for d in range(devices):
        offset = d * cap
        for ref, size in zip((send1_ref, send2_ref, send3_ref), parts):
            for half in range(2):
                ref[d, 0:size, half * LANES : (half + 1) * LANES] = buf_ref[
                    half, offset : offset + size, :
                ].astype(BF)
            offset += size
    fill = ((0, 0), (0, LANES - cap))
    codes = jnp.concatenate([jnp.pad(high, fill), jnp.pad(low, fill)], axis=1)
    for d in range(devices):
        send1_ref[d, parts[0] : parts[0] + EXTRA, :] = jnp.broadcast_to(
            codes[d : d + 1], (EXTRA, 2 * LANES)
        ).astype(BF)


def route(owner, point, count, values, r_inverse, w2, devices, parts):
    slots, channels = values.shape
    cap = sum(parts)
    sizes = (parts[0] + EXTRA,) + tuple(parts[1:])
    return staged(
        functools.partial(route_kernel, parts),
        "route",
        (count, owner, point, r_inverse, w2, values),
        tuple(jax.ShapeDtypeStruct((devices, n, channels), BF) for n in sizes)
        + (jax.ShapeDtypeStruct(w2.shape, BF),),
        [
            pltpu.VMEM((2, slots, LANES), F32),
            pltpu.VMEM((2, devices * cap + EXTRA, LANES), F32),
            pltpu.VMEM((1, slots), jnp.int32),
            pltpu.SMEM((1, slots), jnp.int32),
            pltpu.SemaphoreType.DMA,
        ],
        1e9,
        smem=(0,),
    )


def first_kernel(
    stage, scale_ref, order_ref, state_hbm, we_ref, gain_ref, wqkv_ref, wproj_ref, wup_ref, wdown_ref,
    top_ref, left_ref, corner_ref, z1_ref, h1_ref, h0_ref, hm_ref, qkv_ref, gp_ref,
    state_ref, ones_ref, mask_ref, e_ref, o_ref, sems,
):
    rows, _, cols, _, _ = state_ref.shape
    width = we_ref.shape[1]
    tokens = WIN * WIN
    chunk = cols * tokens

    def load(i):
        return pltpu.make_async_copy(state_hbm.at[i], state_ref.at[i], sems.at[i])

    for i in range(rows):
        load(i).start()
    ones_ref[...] = head_ones(width, width // HEADS)
    mask_ref[...] = head_stack(HEADS, tokens, width)
    scale = scale_lanes(scale_ref, 0, width)
    stage.need(we_ref, gain_ref, wqkv_ref, wproj_ref, wup_ref, wdown_ref)

    def body(i, _):
        load(i).wait()
        x = jnp.concatenate([window(state_ref, i, w).astype(BF) for w in range(cols)], axis=0)
        h0 = nn(x, we_ref[...])
        here = pl.ds(pl.multiple_of(i * chunk, chunk), chunk)
        h0_ref[here, :] = h0
        qkv = nn(norm(h0, gain_ref[0, 0:1]), wqkv_ref[...]).astype(BF)
        qkv_ref[here, :] = qkv
        mixed = attention_chunk(qkv, scale, ones_ref, mask_ref, None, e_ref, o_ref, cols, tokens)
        hm = h0 + nn(mixed, wproj_ref[...]).astype(BF).astype(F32)
        hm_ref[here, :] = hm
        inner, slope = gelu_parts(nn(norm(hm, gain_ref[0, 1:2]), wup_ref[...]))
        gp_ref[here, :] = slope.astype(BF)
        h1 = hm + nn(inner.astype(BF), wdown_ref[...])
        z1 = norm(h1, gain_ref[1, 0:1]).astype(F32)
        for w in range(cols):
            part = slice(w * tokens, (w + 1) * tokens)
            h1_ref[i, :, w, :, :] = h1[part].reshape(WIN, WIN, width)
            z1_ref[i, :, w, :, :] = z1[part].reshape(WIN, WIN, width)
        return 0

    lax.fori_loop(0, rows, body, 0)
    top_ref[...] = z1_ref[0, 0:SHIFT, :, :, :].astype(BF)
    left_ref[...] = z1_ref[:, :, 0, 0:SHIFT, :].astype(BF)
    corner_ref[...] = z1_ref[0, 0:SHIFT, 0, 0:SHIFT, :].astype(BF)


def first_block(order, state5, we, gains, wqkv, wproj, scale, wup, wdown):
    wr, _, wc, _, _ = state5.shape
    width = we.shape[1]
    tokens = wr * wc * WIN * WIN
    chunk = wc * WIN * WIN
    sh = jax.ShapeDtypeStruct
    outs = (
        sh((SHIFT, wc, WIN, width), BF),
        sh((wr, WIN, SHIFT, width), BF),
        sh((SHIFT, SHIFT, width), BF),
        sh((wr, WIN, wc, WIN, width), F32),
        sh((wr, WIN, wc, WIN, width), F32),
        sh((tokens, width), F32),
        sh((tokens, width), F32),
        sh((tokens, 3 * width), BF),
        sh((tokens, wup.shape[2]), BF),
    )
    return staged(
        first_kernel,
        "first_block",
        (scale, order, state5, we, gains, wqkv, wproj, wup, wdown),
        outs,
        [
            pltpu.VMEM(state5.shape, F32),
            pltpu.VMEM((width, width), BF),
            pltpu.VMEM((HEADS * WIN * WIN, width), BF),
            pltpu.VMEM((chunk, HEADS * WIN * WIN), BF),
            pltpu.VMEM((chunk, width), F32),
            pltpu.SemaphoreType.DMA((wr,)),
        ],
        2e9,
        smem=(0,),
        raw=(1, 2),
        layer={5: 0, 6: 0, 7: 0, 8: 0},
    )


def fill_ahead(pad_ref, own, right_ref, below_ref, corner_ref):
    rows, cols, _ = own.shape
    pad_ref[0:rows, 0:cols, :] = own
    pad_ref[0:rows, cols : cols + SHIFT, :] = right_ref[...].astype(F32)
    pad_ref[rows : rows + SHIFT, 0:cols, :] = below_ref[...].astype(F32)
    pad_ref[rows : rows + SHIFT, cols : cols + SHIFT, :] = corner_ref[...].astype(F32)


def rolled_window(pad_ref, i, w):
    block = pad_ref[
        pl.ds(i * WIN + SHIFT, WIN), SHIFT + w * WIN : SHIFT + (w + 1) * WIN, :
    ]
    return block.reshape(WIN * WIN, block.shape[2])


def emit_behind(out_ref, low_ref, east_ref, corner_ref):
    rows, cols, _ = out_ref.shape
    low_ref[...] = out_ref[rows - SHIFT : rows, :, :].astype(BF)
    east_ref[...] = out_ref[:, cols - SHIFT : cols, :].astype(BF)
    corner_ref[...] = out_ref[rows - SHIFT : rows, cols - SHIFT : cols, :].astype(BF)


def shifted_kernel(
    total_rows, stage, start_ref, scale_ref, z1_ref, right_ref, below_ref, corner_ref, wqkv_ref,
    wproj_ref, ans_ref, low_ref, east_ref, last_ref, qkv_ref,
    pad_ref, ones_ref, mask_ref, e_ref, o_ref,
):
    rows, cols, width = z1_ref.shape
    wr, wc = rows // WIN, cols // WIN
    tokens = WIN * WIN
    chunk = wc * tokens
    ones_ref[...] = head_ones(width, width // HEADS)
    mask_ref[...] = head_stack(HEADS, tokens, width)
    scale = scale_lanes(scale_ref, 1, width)
    stage.need(z1_ref, right_ref, below_ref, corner_ref, wqkv_ref, wproj_ref)
    fill_ahead(pad_ref, z1_ref[...], right_ref, below_ref, corner_ref)
    threshold = total_rows - SHIFT - start_ref[0]

    def body(i, _):
        z = jnp.concatenate([rolled_window(pad_ref, i, w).astype(BF) for w in range(wc)], axis=0)
        qkv = nn(z, wqkv_ref[...]).astype(BF)
        qkv_ref[pl.ds(pl.multiple_of(i * chunk, chunk), chunk), :] = qkv
        allowed = side_mask(i, threshold, tokens)
        mixed = attention_chunk(qkv, scale, ones_ref, mask_ref, allowed, e_ref, o_ref, wc, tokens)
        answer = nn(mixed, wproj_ref[...]).astype(BF).astype(F32)
        for w in range(wc):
            ans_ref[pl.ds(i * WIN, WIN), w * WIN : (w + 1) * WIN, :] = answer[
                w * tokens : (w + 1) * tokens
            ].reshape(WIN, WIN, width)
        return 0

    lax.fori_loop(0, wr, body, 0)
    emit_behind(ans_ref, low_ref, east_ref, last_ref)


def behind_shapes(rows, cols, width):
    sh = jax.ShapeDtypeStruct
    return (
        sh((rows, cols, width), F32),
        sh((SHIFT, cols, width), BF),
        sh((rows, SHIFT, width), BF),
        sh((SHIFT, SHIFT, width), BF),
    )


def shifted_forward(start, z1, right, below, corner, wqkv, wproj, scale, total_rows):
    rows, cols, width = z1.shape
    tokens = rows * cols
    chunk = cols * WIN
    outs = behind_shapes(rows, cols, width) + (jax.ShapeDtypeStruct((tokens, 3 * width), BF),)
    return staged(
        functools.partial(shifted_kernel, total_rows),
        "shifted_forward",
        (start, scale, z1, right, below, corner, wqkv, wproj),
        outs,
        [
            pltpu.VMEM((rows + SHIFT, cols + WIN, width), F32),
            pltpu.VMEM((width, width), BF),
            pltpu.VMEM((HEADS * WIN * WIN, width), BF),
            pltpu.VMEM((chunk, HEADS * WIN * WIN), BF),
            pltpu.VMEM((chunk, width), F32),
        ],
        1e9,
        smem=(0, 1),
        layer={6: 1, 7: 1},
    )


def fill_behind(pad_ref, own, above_ref, west_ref, corner_ref):
    rows, cols, _ = own.shape
    pad_ref[SHIFT : SHIFT + rows, SHIFT : SHIFT + cols, :] = own
    pad_ref[0:SHIFT, SHIFT : SHIFT + cols, :] = above_ref[...].astype(F32)
    pad_ref[SHIFT : SHIFT + rows, 0:SHIFT, :] = west_ref[...].astype(F32)
    pad_ref[0:SHIFT, 0:SHIFT, :] = corner_ref[...].astype(F32)


def group_jobs(cnt_smem, offset, size, group, body):
    devices = cnt_smem.shape[0]

    def each(d, _):
        valid = jnp.minimum(cnt_smem[d, 0] - offset, size)

        def some(g, _):
            body(d, offset + g * group, d * size + g * group)
            return 0

        lax.fori_loop(0, (jnp.maximum(valid, 0) + group - 1) // group, some, 0)
        return 0

    lax.fori_loop(0, devices, each, 0)


def gather_part(table_ref, found_ref, idx_smem, cnt_smem, offset, size, group):
    def body(d, slot, row):
        row = pl.multiple_of(row, group)
        for u in range(group):
            found_ref[pl.ds(row + u, 1), :] = table_ref[pl.ds(idx_smem[d, slot + u], 1), :]

    group_jobs(cnt_smem, offset, size, group, body)


def scatter_part(table_ref, found_ref, idx_smem, cnt_smem, dup_smem, offset, size, group):
    def body(d, slot, row):
        row = pl.multiple_of(row, group)
        spots = [idx_smem[d, slot + u] for u in range(group)]

        @pl.when(dup_smem[d, slot] == 0)
        def _():
            sums = [
                table_ref[pl.ds(spots[u], 1), :] + found_ref[pl.ds(row + u, 1), :]
                for u in range(group)
            ]
            for u in range(group):
                table_ref[pl.ds(spots[u], 1), :] = sums[u]

        @pl.when(dup_smem[d, slot] != 0)
        def _():
            for u in range(group):
                table_ref[pl.ds(spots[u], 1), :] = (
                    table_ref[pl.ds(spots[u], 1), :] + found_ref[pl.ds(row + u, 1), :]
                )

    group_jobs(cnt_smem, offset, size, group, body)


def radiance_part(found_ref, obs_ref, mixed_ref, w1_ref, size):
    devices, _, channels = obs_ref.shape
    batch = min(devices, max(1, 512 // size))

    def body(i, _):
        here = pl.ds(pl.multiple_of(i * batch * size, batch * size), batch * size)
        y = obs_ref[pl.ds(i * batch, batch), 0:size, :].astype(F32)
        y = y.reshape(batch * size, channels)
        t = jnp.tanh(nn(found_ref[here, :].astype(BF), w1_ref[...].astype(BF)))
        pulled = (nn(t.astype(BF), mixed_ref[...]) - y) * (1.0 - t * t)
        found_ref[here, :] = nt(pulled.astype(BF), w1_ref[...].astype(BF))
        return 0

    lax.fori_loop(0, devices // batch, body, 0)


def forecast_kernel(
    parts, group, stage, obs1_ref, h1_ref, ans_ref, above_ref, west_ref, corner_ref, gain_ref,
    wup_ref, wdown_ref, whead_ref, state_ref, w1_in_ref, mixed_ref, obs2_ref, back_ref, inv_ref,
    h2_ref, gp_ref, prior_ref, found3_ref, idx_ref, cnt_ref, dup_ref, table_out_ref, w1_ref,
    pad_ref, table_ref, found1_ref, found2_ref, idx_smem, cnt_smem, dup_smem, sems,
):
    rows, cols, width = h1_ref.shape
    devices = obs1_ref.shape[0]
    tokens = rows * cols
    step = tokens // 2

    stage.need(obs1_ref)
    codes = obs1_ref[:, parts[0] : parts[0] + EXTRA, :].astype(F32)[:, 0, :]
    high = codes[:, :LANES].astype(jnp.int32)
    low = codes[:, LANES : 2 * LANES].astype(jnp.int32)
    point = jnp.where(high > 0, (high - 1) * LANES + low, 0)
    lane = lax.broadcasted_iota(jnp.int32, (devices, LANES), 1)
    idx = jnp.where(
        high > 0, (point % PIX) * tokens + point // PIX, PIX * tokens + lane % group
    )
    idx_ref[...] = idx
    cnt_ref[...] = jnp.broadcast_to(
        jnp.sum(jnp.where(high > 0, 1.0, 0.0), 1, keepdims=True), (devices, LANES)
    ).astype(jnp.int32)
    same = jnp.zeros((devices, LANES), jnp.int32)
    for s in range(1, group):
        hit = (pltpu.roll(idx, s, 1) == idx) & (lane % group >= s)
        same = jnp.maximum(same, jnp.where(hit, 1, 0))
    s = group // 2
    while s:
        same = jnp.maximum(same, pltpu.roll(same, LANES - s, 1))
        s //= 2
    dup_ref[...] = same
    copies = [
        pltpu.make_async_copy(a, b, sems.at[n])
        for n, (a, b) in enumerate(
            ((idx_ref, idx_smem), (cnt_ref, cnt_smem), (dup_ref, dup_smem))
        )
    ]
    for copy in copies:
        copy.start()
    stage.need(h1_ref, ans_ref, above_ref, west_ref, corner_ref)
    fill_behind(pad_ref, ans_ref[...], above_ref, west_ref, corner_ref)
    h2_ref[...] = (h1_ref[...] + pad_ref[0:rows, 0:cols, :]).reshape(tokens, width)
    table_ref[...] = jnp.zeros_like(table_ref)
    stage.need(gain_ref, wup_ref, wdown_ref, whead_ref, state_ref)

    def forward(i, _):
        here = pl.ds(pl.multiple_of(i * step, step), step)
        h2 = h2_ref[here, :]
        inner, slope = gelu_parts(nn(norm(h2, gain_ref[1, 1:2]), wup_ref[...]))
        gp_ref[here, :] = slope.astype(BF)
        h3 = (h2 + nn(inner.astype(BF), wdown_ref[...])).astype(BF)
        moved = state_ref[here, :] + nn(h3, whead_ref[...])
        for s in range(PIX):
            there = pl.ds(pl.multiple_of(s * tokens + i * step, WIN), step)
            table_ref[there, 0:VARS] = moved[:, s * VARS : (s + 1) * VARS]
        return 0

    lax.fori_loop(0, 2, forward, 0)
    stage.emit(h2_ref, gp_ref, idx_ref, cnt_ref, dup_ref)
    stage.need(back_ref, inv_ref, w1_in_ref, mixed_ref, obs2_ref)
    prior_ref[...] = inv_ref[...] * (state_ref[...] - back_ref[...])
    stage.emit(prior_ref)
    w1_ref[...] = jnp.zeros_like(w1_ref)
    w1_ref[0:VARS, :] = w1_in_ref[...]
    w1_ref[...] = w1_ref[...].astype(BF).astype(F32)
    for copy in copies:
        copy.wait()
    offsets = (0, parts[0], parts[0] + parts[1])
    founds = (found1_ref, found2_ref, found3_ref)
    for offset, size, found in zip(offsets, parts, founds):
        gather_part(table_ref, found, idx_smem, cnt_smem, offset, size, group)
    stage.emit(found3_ref)
    table_ref = table_out_ref
    table_ref[...] = jnp.zeros_like(table_ref)
    radiance_part(found1_ref, obs1_ref, mixed_ref, w1_ref, parts[0])
    scatter_part(table_ref, found1_ref, idx_smem, cnt_smem, dup_smem, 0, parts[0], group)
    radiance_part(found2_ref, obs2_ref, mixed_ref, w1_ref, parts[1])
    scatter_part(table_ref, found2_ref, idx_smem, cnt_smem, dup_smem, parts[0], parts[1], group)


def forecast(
    h1, ans, above, west, corner, state, background, inv, obs1, obs2, mixed, gains, wup, wdown,
    whead, w1, parts, group,
):
    rows, cols, width = h1.shape
    tokens = rows * cols
    devices = obs1.shape[0]
    sh = jax.ShapeDtypeStruct
    outs = (
        sh((tokens, width), F32),
        sh((tokens, wup.shape[2]), BF),
        sh(state.shape, F32),
        sh((devices * parts[2], LANES), F32),
        sh((devices, LANES), jnp.int32),
        sh((devices, LANES), jnp.int32),
        sh((devices, LANES), jnp.int32),
        sh((PIX * tokens + group, LANES), F32),
        sh((LANES, w1.shape[1]), F32),
    )
    return staged(
        functools.partial(forecast_kernel, parts, group),
        "forecast",
        (
            obs1, h1, ans, above, west, corner, gains, wup, wdown, whead, state, w1, mixed, obs2,
            background, inv,
        ),
        outs,
        [
            pltpu.VMEM((rows + SHIFT, cols + WIN, width), F32),
            pltpu.VMEM((PIX * tokens + group, LANES), F32),
            pltpu.VMEM((devices * parts[0], LANES), F32),
            pltpu.VMEM((devices * parts[1], LANES), F32),
        ]
        + [pltpu.SMEM((devices, LANES), jnp.int32)] * 3
        + [pltpu.SemaphoreType.DMA((3,))],
        3e9,
        layer={7: 1, 8: 1},
    )


def adjoint_kernel(
    parts, group, stage, idx_smem, cnt_smem, dup_smem, w1_ref, mixed_ref, work_ref, obs3_ref,
    table_ref, prior_ref, whead_ref, wdown_ref, gp_ref, wup_ref, h2_ref, gain_ref,
    top_ref, left_ref, edge_ref, third_ref, out_ref, moved_ref,
):
    rows, cols, width = third_ref.shape
    tokens = rows * cols
    step = tokens // 2
    stage.need(w1_ref, mixed_ref, work_ref, obs3_ref)
    radiance_part(work_ref, obs3_ref, mixed_ref, w1_ref, parts[2])
    stage.need(table_ref)
    scatter_part(
        table_ref, work_ref, idx_smem, cnt_smem, dup_smem, parts[0] + parts[1], parts[2], group
    )
    stage.need(prior_ref, whead_ref, wdown_ref, gp_ref, wup_ref, h2_ref, gain_ref)

    def backward(i, _):
        here = pl.ds(pl.multiple_of(i * step, step), step)
        for s in range(PIX):
            there = pl.ds(pl.multiple_of(s * tokens + i * step, WIN), step)
            moved_ref[:, s * VARS : (s + 1) * VARS] = table_ref[there, 0:VARS]
        moved = moved_ref[...]
        out_ref[here, :] = moved + prior_ref[here, :]
        grad = nt(moved.astype(BF), whead_ref[...]).astype(BF)
        d_inner = nt(grad, wdown_ref[...]) * gp_ref[here, :].astype(F32)
        d_normed = nt(d_inner.astype(BF), wup_ref[...])
        third = grad.astype(F32) + norm_back(h2_ref[here, :], gain_ref[1, 1:2], d_normed)
        third_ref[pl.ds(i * (rows // 2), rows // 2), :, :] = third.reshape(rows // 2, cols, width)
        return 0

    lax.fori_loop(0, 2, backward, 0)
    top_ref[...] = third_ref[0:SHIFT, :, :].astype(BF)
    left_ref[...] = third_ref[:, 0:SHIFT, :].astype(BF)
    edge_ref[...] = third_ref[0:SHIFT, 0:SHIFT, :].astype(BF)


def adjoint(
    idx, cnt, dup, found, obs3, mixed, w1, h2, gp, gains, wup, wdown, whead, prior, sums, parts,
    group, rows, cols,
):
    width = h2.shape[1]
    third, top, left, edge = behind_shapes(rows, cols, width)
    outs = (top, left, edge, third, jax.ShapeDtypeStruct(prior.shape, F32))
    return staged(
        functools.partial(adjoint_kernel, parts, group),
        "adjoint",
        (idx, cnt, dup, w1, mixed, found, obs3, sums, prior, whead, wdown, gp, wup, h2, gains),
        outs,
        [pltpu.VMEM((prior.shape[0] // 2, prior.shape[1]), F32)],
        2e9,
        smem=(0, 1, 2),
        layer={10: 1, 12: 1},
    )


def shifted_back_kernel(
    total_rows, stage, start_ref, scale_ref, third_ref, right_ref, below_ref, corner_ref,
    wproj_ref, qkv_ref, wqkv_ref, dz_ref, low_ref, east_ref, last_ref,
    pad_ref, ones_ref, mask_ref, dq_ref, dk_ref, dv_ref,
):
    rows, cols, width = third_ref.shape
    wr, wc = rows // WIN, cols // WIN
    tokens = WIN * WIN
    chunk = wc * tokens
    ones_ref[...] = head_ones(width, width // HEADS)
    mask_ref[...] = head_stack(HEADS, tokens, width)
    scale = scale_lanes(scale_ref, 1, width)
    stage.need(third_ref, right_ref, below_ref, corner_ref, wproj_ref, qkv_ref, wqkv_ref)
    fill_ahead(pad_ref, third_ref[...], right_ref, below_ref, corner_ref)
    threshold = total_rows - SHIFT - start_ref[0]

    def body(i, _):
        d_answer = jnp.concatenate(
            [rolled_window(pad_ref, i, w).astype(BF) for w in range(wc)], axis=0
        )
        d_out = nt(d_answer, wproj_ref[...]).astype(BF)
        allowed = side_mask(i, threshold, tokens)
        qkv = qkv_ref[pl.ds(pl.multiple_of(i * chunk, chunk), chunk), :]
        d_qkv = attention_chunk_back(
            qkv, d_out, scale, ones_ref, mask_ref, allowed,
            dq_ref, dk_ref, dv_ref, wc, tokens,
        )
        dz = nt(d_qkv, wqkv_ref[...]).astype(BF).astype(F32)
        for w in range(wc):
            dz_ref[pl.ds(i * WIN, WIN), w * WIN : (w + 1) * WIN, :] = dz[
                w * tokens : (w + 1) * tokens
            ].reshape(WIN, WIN, width)
        return 0

    lax.fori_loop(0, wr, body, 0)
    emit_behind(dz_ref, low_ref, east_ref, last_ref)


def shifted_backward(start, third, right, below, corner, qkv, wqkv, wproj, scale, total_rows):
    rows, cols, width = third.shape
    chunk = cols * WIN
    outs = behind_shapes(rows, cols, width)
    return staged(
        functools.partial(shifted_back_kernel, total_rows),
        "shifted_backward",
        (start, scale, third, right, below, corner, wproj, qkv, wqkv),
        outs,
        [
            pltpu.VMEM((rows + SHIFT, cols + WIN, width), F32),
            pltpu.VMEM((width, width), BF),
            pltpu.VMEM((HEADS * WIN * WIN, width), BF),
        ]
        + [pltpu.VMEM((chunk, width), F32)] * 3,
        1e9,
        smem=(0, 1),
        layer={6: 1, 8: 1},
    )


def last_kernel(
    stage, scale_ref, partial_hbm, dz_ref, above_ref, west_ref, corner_ref, third_ref, h1_ref,
    gain_ref, wdown_ref, gp_ref, wup_ref, hm_ref, wproj_ref, qkv_ref, wqkv_ref, h0_ref, we_ref,
    out_hbm,
    pad_ref, ones_ref, mask_ref, dq_ref, dk_ref, dv_ref, out_ref, in_sems, out_sems,
):
    rows, cols, width = dz_ref.shape
    wr, wc = rows // WIN, cols // WIN
    tokens = WIN * WIN
    chunk = wc * tokens

    def rows_of(ref, i):
        return ref.at[pl.ds(i * WIN, WIN)]

    for i in range(wr):
        pltpu.make_async_copy(rows_of(partial_hbm, i), rows_of(out_ref, i), in_sems.at[i]).start()
    ones_ref[...] = head_ones(width, width // HEADS)
    mask_ref[...] = head_stack(HEADS, tokens, width)
    scale = scale_lanes(scale_ref, 0, width)
    stage.need(dz_ref, above_ref, west_ref, corner_ref, third_ref, h1_ref, gain_ref, wdown_ref)
    stage.need(gp_ref, wup_ref, hm_ref, wproj_ref, qkv_ref, wqkv_ref, h0_ref, we_ref)
    fill_behind(pad_ref, dz_ref[...], above_ref, west_ref, corner_ref)

    def body(i, _):
        here = pl.ds(pl.multiple_of(i * chunk, chunk), chunk)
        band = pl.ds(i * WIN, WIN)

        def take(ref):
            return jnp.concatenate(
                [
                    ref[band, w * WIN : (w + 1) * WIN, :].reshape(tokens, width)
                    for w in range(wc)
                ],
                axis=0,
            )

        second = take(third_ref) + norm_back(take(h1_ref), gain_ref[1, 0:1], take(pad_ref))
        d_inner = nt(second.astype(BF), wdown_ref[...]) * gp_ref[here, :].astype(F32)
        d_normed = nt(d_inner.astype(BF), wup_ref[...])
        d_hm = second + norm_back(hm_ref[here, :], gain_ref[0, 1:2], d_normed)
        d_out = nt(d_hm.astype(BF), wproj_ref[...]).astype(BF)
        d_qkv = attention_chunk_back(
            qkv_ref[here, :], d_out, scale, ones_ref, mask_ref, None,
            dq_ref, dk_ref, dv_ref, wc, tokens,
        )
        dz = nt(d_qkv, wqkv_ref[...])
        d_h0 = (d_hm + norm_back(h0_ref[here, :], gain_ref[0, 0:1], dz)).astype(BF)
        pltpu.make_async_copy(rows_of(partial_hbm, i), rows_of(out_ref, i), in_sems.at[i]).wait()
        for w in range(wc):
            grad = nt(d_h0[w * tokens : (w + 1) * tokens], we_ref[...])
            grad = grad.reshape(WIN, WIN, grad.shape[1])
            spot = (band, slice(w * WIN, (w + 1) * WIN), slice(None))
            out_ref[spot] = grad + out_ref[spot]
        pltpu.make_async_copy(rows_of(out_ref, i), rows_of(out_hbm, i), out_sems.at[i]).start()
        return 0

    lax.fori_loop(0, wr, body, 0)
    for i in range(wr):
        pltpu.make_async_copy(rows_of(out_ref, i), rows_of(out_hbm, i), out_sems.at[i]).wait()


def last_block(
    third, dz, above, west, corner, h1, h0, hm, qkv, gp, we, gains, wqkv, wproj, scale,
    wup, wdown, partial,
):
    rows, cols, width = dz.shape
    chunk = cols * WIN
    (result,) = staged(
        last_kernel,
        "last_block",
        (
            scale, partial, dz, above, west, corner, third, h1, gains, wdown, gp, wup, hm, wproj,
            qkv, wqkv, h0, we,
        ),
        (jax.ShapeDtypeStruct(partial.shape, F32),),
        [
            pltpu.VMEM((rows + SHIFT, cols + WIN, width), F32),
            pltpu.VMEM((width, width), BF),
            pltpu.VMEM((HEADS * WIN * WIN, width), BF),
        ]
        + [pltpu.VMEM((chunk, width), F32)] * 3
        + [
            pltpu.VMEM(partial.shape, F32),
            pltpu.SemaphoreType.DMA((rows // WIN,)),
            pltpu.SemaphoreType.DMA((rows // WIN,)),
        ],
        2e9,
        smem=(0,),
        raw=(1,),
        raw_outs=(0,),
        layer={9: 0, 11: 0, 13: 0, 15: 0},
    )
    return result


def neighbour(x, by_lat, by_lon):
    lat, lon = lax.axis_size("lat"), lax.axis_size("lon")
    pairs = [
        (a * lon + b, ((a + by_lat) % lat) * lon + (b + by_lon) % lon)
        for a in range(lat)
        for b in range(lon)
    ]
    return lax.ppermute(x, ("lat", "lon"), pairs)


def exchange(x):
    return lax.all_to_all(x, ("lat", "lon"), split_axis=0, concat_axis=0, tiled=True)


def local(
    state,
    background,
    inv_background,
    w_embed,
    norm_gain,
    w_qkv,
    w_proj,
    head_scale,
    w_up,
    w_down,
    w_head,
    w_obs1,
    w_obs2,
    r_inverse,
    obs_values,
    obs_owner,
    obs_point,
    obs_count,
):
    rows, cols, patch_values = state.shape
    width = w_embed.shape[1]
    total_rows = rows * lax.axis_size("lat")
    row_start = (lax.axis_index("lat") * rows).astype(jnp.int32).reshape(1)
    devices = lax.axis_size("lat") * lax.axis_size("lon")
    slots = obs_values.shape[0]
    cap = 2 * slots // devices

    parts, group = split(cap)

    send1, send2, send3, mixed = route(
        obs_owner.reshape(1, slots), obs_point.reshape(1, slots), obs_count, obs_values,
        r_inverse, w_obs2, devices, parts,
    )
    obs1 = exchange(send1)
    state5 = state.reshape(rows // WIN, WIN, cols // WIN, WIN, patch_values)
    top, left, corner, z1, h1, h0, hm, qkv0, gp0 = first_block(
        mixed, state5, w_embed, norm_gain, w_qkv, w_proj, head_scale, w_up, w_down
    )
    z1 = z1.reshape(rows, cols, width)
    h1 = h1.reshape(rows, cols, width)
    below = neighbour(top.reshape(SHIFT, cols, width), -1, 0)
    right = neighbour(left.reshape(rows, SHIFT, width), 0, -1)
    corner = neighbour(corner, -1, -1)
    below, right, corner, obs1, send2 = lax.optimization_barrier(
        (below, right, corner, obs1, send2)
    )
    obs2 = exchange(send2)
    answer, low, east, last, qkv1 = shifted_forward(
        row_start, z1, right, below, corner, w_qkv, w_proj, head_scale, total_rows
    )
    above = neighbour(low, 1, 0)
    west = neighbour(east, 0, 1)
    last = neighbour(last, 1, 1)
    above, west, last, obs2, send3 = lax.optimization_barrier((above, west, last, obs2, send3))
    obs3 = exchange(send3)
    flat = (rows * cols, patch_values)
    h2, gp1, prior, found, idx, cnt, dup, sums, w1 = forecast(
        h1, answer, above, west, last, state.reshape(flat), background.reshape(flat),
        inv_background.reshape(1, -1), obs1, obs2, mixed, norm_gain, w_up, w_down, w_head,
        w_obs1, parts, group,
    )
    top, left, corner, third, partial = adjoint(
        idx, cnt, dup, found, obs3, mixed, w1, h2, gp1, norm_gain, w_up, w_down, w_head, prior,
        sums,
        parts, group, rows, cols,
    )
    below = neighbour(top, -1, 0)
    right = neighbour(left, 0, -1)
    corner = neighbour(corner, -1, -1)
    dz, low, east, last = shifted_backward(
        row_start, third, right, below, corner, qkv1, w_qkv, w_proj, head_scale, total_rows
    )
    above = neighbour(low, 1, 0)
    west = neighbour(east, 0, 1)
    last = neighbour(last, 1, 1)
    return last_block(
        third, dz, above, west, last, h1, h0, hm, qkv0, gp0, w_embed, norm_gain, w_qkv, w_proj,
        head_scale, w_up, w_down, partial.reshape(state.shape),
    )


def solution(mesh):
    placed = (
        P("lat", "lon", None),
        P("lat", "lon", None),
        P(),
        P(),
        P(),
        P(),
        P(),
        P(),
        P(),
        P(),
        P(),
        P(),
        P(),
        P(),
        P(("lat", "lon"), None),
        P(("lat", "lon"), None),
        P(("lat", "lon")),
        P(("lat", "lon")),
    )
    return jax.shard_map(
        local, mesh=mesh, in_specs=placed, out_specs=P("lat", "lon", None), check_vma=False
    )
```

```python
import functools

import jax
import jax.numpy as jnp
from jax import lax
from jax.experimental import pallas as pl
from jax.experimental.pallas import tpu as pltpu
from jax.sharding import PartitionSpec as P

HEADS = 8
VARS = 69
PIX = 16
WIN = 8
SHIFT = 4
LANES = 128
EXTRA = 8
EPS = 1e-05
BF = jnp.bfloat16
F32 = jnp.float32
SQRT_2_OVER_PI = 0.7978845608028654
CUBIC = 0.044715

SMEM = pl.BlockSpec(memory_space=pltpu.SMEM)
VMEM = pl.BlockSpec(memory_space=pltpu.VMEM)
HBM = pl.BlockSpec(memory_space=pltpu.HBM)
MIB = 1024 * 1024


class Stage:
    def __init__(self):
        self.inputs = {}
        self.outputs = {}
        self.waited = set()
        self.sent = set()

    def need(self, *refs):
        for ref in refs:
            if id(ref) not in self.waited:
                self.waited.add(id(ref))
                self.inputs[id(ref)].wait()

    def need_at(self, first, *refs):
        pending = [ref for ref in refs if id(ref) not in self.waited]
        self.waited.update(id(ref) for ref in pending)

        @pl.when(first)
        def _():
            for ref in pending:
                self.inputs[id(ref)].wait()

    def emit_part(self, part, *refs):
        for ref in refs:
            self.sent.add(id(ref))
            self.outputs[id(ref)].part(part).start()

    def emit(self, *refs):
        for ref in refs:
            if id(ref) not in self.sent:
                self.sent.add(id(ref))
                self.outputs[id(ref)].start()

    def close(self):
        for key, copy in self.inputs.items():
            if key not in self.waited:
                copy.wait()
        for key, copy in self.outputs.items():
            if key not in self.sent:
                copy.start()
        for copy in self.outputs.values():
            copy.wait()


class Outgoing:
    def __init__(self, source, target, sem):
        self.refs = (source, target, sem)

    def part(self, part):
        source, target, sem = self.refs
        return pltpu.make_async_copy(source.at[part], target.at[part], sem)

    def start(self):
        pltpu.make_async_copy(*self.refs).start()

    def wait(self):
        pltpu.make_async_copy(*self.refs).wait()


def staged(
    body, name, args, outs, scratch, flops, smem=(), raw=(), raw_outs=(), layer=None, vmem=()
):
    layer = layer or {}
    count = len(args)
    in_buffers = []
    for i, x in enumerate(args):
        if i not in smem and i not in raw and i not in vmem:
            shape = x.shape[1:] if i in layer else x.shape
            in_buffers.append((i, pltpu.VMEM(shape, x.dtype)))
    out_buffers = [
        (j, pltpu.VMEM(o.shape, o.dtype)) for j, o in enumerate(outs) if j not in raw_outs
    ]

    def kernel(*refs):
        ins = list(refs[:count])
        results = list(refs[count : count + len(outs)])
        rest = list(refs[count + len(outs) :])
        ins_vmem = rest[: len(in_buffers)]
        outs_vmem = rest[len(in_buffers) : len(in_buffers) + len(out_buffers)]
        in_sems, out_sems = rest[-2:]
        extra = rest[len(in_buffers) + len(out_buffers) : -2]
        stage = Stage()
        stage.waited.update(id(ins[i]) for i in vmem)
        for n, ((i, _), buffer) in enumerate(zip(in_buffers, ins_vmem)):
            source = ins[i].at[layer[i]] if i in layer else ins[i]
            copy = pltpu.make_async_copy(source, buffer, in_sems.at[n])
            copy.start()
            stage.inputs[id(buffer)] = copy
            ins[i] = buffer
        for n, ((j, _), buffer) in enumerate(zip(out_buffers, outs_vmem)):
            stage.outputs[id(buffer)] = Outgoing(buffer, results[j], out_sems.at[n])
            results[j] = buffer
        body(stage, *ins, *results, *extra)
        stage.close()

    return pl.pallas_call(
        kernel,
        out_shape=tuple(outs),
        in_specs=[
            SMEM if i in smem else VMEM if i in vmem else HBM for i in range(count)
        ],
        out_specs=(HBM,) * len(outs),
        scratch_shapes=[b for _, b in in_buffers]
        + [b for _, b in out_buffers]
        + list(scratch)
        + [
            pltpu.SemaphoreType.DMA((max(1, len(in_buffers)),)),
            pltpu.SemaphoreType.DMA((max(1, len(out_buffers)),)),
        ],
        compiler_params=pltpu.CompilerParams(vmem_limit_bytes=60 * MIB),
        cost_estimate=pl.CostEstimate(
            flops=int(flops), bytes_accessed=8 * MIB, transcendentals=0
        ),
        name=name,
    )(*args)


def scale_lanes(scale_ref, block, width):
    head = lax.broadcasted_iota(jnp.int32, (1, width), 1) // (width // HEADS)
    row = jnp.zeros((1, width), F32)
    for h in range(HEADS):
        row = jnp.where(head == h, scale_ref[block, h], row)
    return row


def nn(a, b):
    return lax.dot_general(a, b, (((1,), (0,)), ((), ())), preferred_element_type=F32)


def nt(a, b):
    return lax.dot_general(a, b, (((1,), (1,)), ((), ())), preferred_element_type=F32)


def tn(a, b):
    return lax.dot_general(a, b, (((0,), (0,)), ((), ())), preferred_element_type=F32)


def norm_parts(h):
    mean = jnp.mean(h, -1, keepdims=True)
    centred = h - mean
    spread = jnp.mean(centred * centred, -1, keepdims=True)
    rstd = lax.rsqrt(spread + EPS)
    return centred * rstd, rstd


def norm(h, gain):
    return (norm_parts(h)[0] * gain).astype(BF)


def norm_back(h, gain, cotangent):
    xhat, rstd = norm_parts(h)
    scaled = cotangent * gain
    m1 = jnp.mean(scaled, -1, keepdims=True)
    m2 = jnp.mean(scaled * xhat, -1, keepdims=True)
    return rstd * (scaled - m1 - xhat * m2)


def gelu_parts(u):
    square = u * u
    t = jnp.tanh(SQRT_2_OVER_PI * u * (1.0 + CUBIC * square))
    half = 0.5 * (1.0 + t)
    slope = half + 0.5 * u * (1.0 - t * t) * (
        SQRT_2_OVER_PI * (1.0 + 3.0 * CUBIC * square)
    )
    return u * half, slope


def head_ones(width, size):
    a = lax.broadcasted_iota(jnp.int32, (width, width), 0) // size
    b = lax.broadcasted_iota(jnp.int32, (width, width), 1) // size
    return (a == b).astype(F32).astype(BF)


def head_stack(heads, tokens, width):
    size = width // heads
    a = lax.broadcasted_iota(jnp.int32, (heads * tokens, width), 0) // tokens
    b = lax.broadcasted_iota(jnp.int32, (heads * tokens, width), 1) // size
    return (a == b).astype(F32).astype(BF)


def stacked(x, mask):
    return jnp.concatenate([x] * HEADS, axis=0) * mask


def side_mask(window_row, threshold, tokens):
    shape = (tokens, HEADS * tokens)
    a = lax.broadcasted_iota(jnp.int32, shape, 0) // WIN
    b = (lax.broadcasted_iota(jnp.int32, shape, 1) % tokens) // WIN
    first = (window_row * WIN + a) >= threshold
    second = (window_row * WIN + b) >= threshold
    return jnp.where(first == second, 1.0, 0.0).astype(F32)


def window(ref, i, w):
    block = ref[i, :, w, :, :]
    return block.reshape(block.shape[0] * block.shape[1], block.shape[2])


def attention_chunk(qkv, scale, ones_ref, mask_ref, allowed, e_ref, o_ref, count, tokens):
    width = qkv.shape[1] // 3
    q = qkv[:, :width].astype(F32)
    k = qkv[:, width : 2 * width].astype(F32)
    v = qkv[:, 2 * width :]
    ones = ones_ref[...]
    qs = (q * lax.rsqrt(nn((q * q).astype(BF), ones) + 1.0) * scale).astype(BF)
    kn = (k * lax.rsqrt(nn((k * k).astype(BF), ones) + 1.0)).astype(BF)
    mask = mask_ref[...]
    for w in range(count):
        part = slice(w * tokens, (w + 1) * tokens)
        expo = jnp.exp(nt(qs[part], stacked(kn[part], mask)))
        if allowed is not None:
            expo = expo * allowed
        expo = expo.astype(BF)
        e_ref[part] = expo
        o_ref[part] = nn(expo, stacked(v[part], mask))
    return (o_ref[...] / nn(e_ref[...], mask)).astype(BF)


def attention_chunk_back(
    qkv, d_out, scale, ones_ref, mask_ref, allowed, dq_ref, dk_ref, dv_ref, count, tokens
):
    width = qkv.shape[1] // 3
    size = width // HEADS
    q = qkv[:, :width].astype(F32)
    k = qkv[:, width : 2 * width].astype(F32)
    v = qkv[:, 2 * width :]
    ones = ones_ref[...]
    rq = lax.rsqrt(nn((q * q).astype(BF), ones) + 1.0)
    rk = lax.rsqrt(nn((k * k).astype(BF), ones) + 1.0)
    qs = (q * rq * scale).astype(BF)
    kn = (k * rk).astype(BF)
    mask = mask_ref[...]
    lane_head = lax.broadcasted_iota(jnp.int32, (1, LANES), 1) // size
    per_tile = LANES // size
    for w in range(count):
        part = slice(w * tokens, (w + 1) * tokens)
        kw = kn[part]
        qm = stacked(qs[part], mask)
        dm = stacked(d_out[part], mask)
        expo = jnp.exp(nt(kw, qm))
        if allowed is not None:
            expo = expo * allowed
        p = expo * (1.0 / jnp.sum(expo, 0, keepdims=True))
        dp = nt(v[part], dm)
        ds = (p * (dp - jnp.sum(p * dp, 0, keepdims=True))).astype(BF)
        dv_ref[part] = nn(p.astype(BF), dm)
        dk_ref[part] = nn(ds, qm)
        full = tn(ds, kw)
        tiles = []
        for tile in range(width // LANES):
            total = None
            for s in range(per_tile):
                h = tile * per_tile + s
                block = full[h * tokens : (h + 1) * tokens, tile * LANES : (tile + 1) * LANES]
                block = jnp.where(lane_head == s, block, 0.0)
                total = block if total is None else total + block
            tiles.append(total)
        dq_ref[part] = jnp.concatenate(tiles, axis=1)
    dqs = dq_ref[...]
    dkn = dk_ref[...]
    dq = scale * rq * (dqs - q * (rq * rq) * nn((q * dqs).astype(BF), ones))
    dk = rk * (dkn - k * (rk * rk) * nn((k * dkn).astype(BF), ones))
    return jnp.concatenate([dq.astype(BF), dk.astype(BF), dv_ref[...].astype(BF)], axis=1)


def split(cap):
    first = max(8, cap // 4)
    return (first, first, cap - 2 * first), min(16, first)


def route_kernel(
    parts, stage, count_ref, owner_ref, point_ref, r_ref, w2_ref, values_ref,
    send1_ref, send2_ref, send3_ref, mixed_ref, y_ref, buf_ref, tgt_ref, tgt_smem, sem,
):
    cap = sum(parts)
    slots = owner_ref.shape[1]
    devices = send1_ref.shape[0]
    stage.need(owner_ref, point_ref)
    owner = owner_ref[...]
    live = lax.broadcasted_iota(jnp.int32, (1, slots), 1) < count_ref[0]
    match = lax.broadcasted_iota(jnp.int32, (devices, slots), 0) == owner
    match = jnp.where(match, 1.0, 0.0).astype(F32)
    a = lax.broadcasted_iota(jnp.int32, (LANES, LANES), 0)
    b = lax.broadcasted_iota(jnp.int32, (LANES, LANES), 1)
    upper = jnp.where(a < b, 1.0, 0.0).astype(BF)
    chunks = slots // LANES
    flat = jnp.concatenate(
        [match[:, c * LANES : (c + 1) * LANES] for c in range(chunks)], axis=0
    )
    before = nn(flat.astype(BF), upper)
    carry = jnp.zeros((devices, 1), F32)
    ranks = []
    dump = devices * cap
    for c in range(chunks):
        here = match[:, c * LANES : (c + 1) * LANES]
        seen = before[c * devices : (c + 1) * devices] + carry
        ranks.append(jnp.sum(here * seen, 0, keepdims=True))
        span = slice(c * LANES, (c + 1) * LANES)
        spot = owner[:, span] * cap + ranks[-1].astype(jnp.int32)
        tgt_ref[c : c + 1, :] = jnp.where(live[:, span], spot, dump)
        carry = carry + jnp.sum(here, 1, keepdims=True)
    rank = jnp.concatenate(ranks, axis=1).astype(jnp.int32)
    copy = pltpu.make_async_copy(tgt_ref, tgt_smem, sem)
    copy.start()
    place = lax.broadcasted_iota(jnp.int32, (cap, slots), 0) == rank
    place = jnp.where(place & live, 1.0, 0.0).astype(BF)
    point = point_ref[...]
    high = (match * (point // LANES + 1).astype(F32)).astype(BF)
    low = (match * (point % LANES).astype(F32)).astype(BF)
    high = nt(high, place)
    low = nt(low, place)
    stage.need(r_ref, w2_ref, values_ref)
    best = lax.Precision.HIGHEST
    dims = (((1,), (1,)), ((), ()))
    m2 = lax.dot_general(
        r_ref[...], w2_ref[...], dims, precision=best, preferred_element_type=F32
    )
    mixed_ref[...] = jnp.dot(
        w2_ref[...], m2, precision=best, preferred_element_type=F32
    ).astype(BF)
    y = nn(values_ref[...].astype(BF), m2.astype(BF))
    y_ref[0, :, :] = y[:, :LANES]
    y_ref[1, :, :] = y[:, LANES:]
    buf_ref[...] = jnp.zeros_like(buf_ref)
    copy.wait()
    unroll = 16

    def move(c, _):
        base = pl.multiple_of(c * LANES, LANES)
        for start in range(0, LANES, unroll):
            spots = [tgt_smem[c, start + u] for u in range(unroll)]
            for half in range(2):
                for u in range(unroll):
                    buf_ref[half, pl.ds(spots[u], 1), :] = y_ref[
                        half, pl.ds(base + start + u, 1), :
                    ]
        return 0

    lax.fori_loop(0, chunks, move, 0)
    for d in range(devices):
        offset = d * cap
        for ref, size in zip((send1_ref, send2_ref, send3_ref), parts):
            for half in range(2):
                ref[d, 0:size, half * LANES : (half + 1) * LANES] = buf_ref[
                    half, offset : offset + size, :
                ].astype(BF)
            offset += size
    fill = ((0, 0), (0, LANES - cap))
    codes = jnp.concatenate([jnp.pad(high, fill), jnp.pad(low, fill)], axis=1)
    for d in range(devices):
        send1_ref[d, parts[0] : parts[0] + EXTRA, :] = jnp.broadcast_to(
            codes[d : d + 1], (EXTRA, 2 * LANES)
        ).astype(BF)


def route(owner, point, count, values, r_inverse, w2, devices, parts):
    slots, channels = values.shape
    cap = sum(parts)
    sizes = (parts[0] + EXTRA,) + tuple(parts[1:])
    return staged(
        functools.partial(route_kernel, parts),
        "route",
        (count, owner, point, r_inverse, w2, values),
        tuple(jax.ShapeDtypeStruct((devices, n, channels), BF) for n in sizes)
        + (jax.ShapeDtypeStruct(w2.shape, BF),),
        [
            pltpu.VMEM((2, slots, LANES), F32),
            pltpu.VMEM((2, devices * cap + EXTRA, LANES), F32),
            pltpu.VMEM((slots // LANES, LANES), jnp.int32),
            pltpu.SMEM((slots // LANES, LANES), jnp.int32),
            pltpu.SemaphoreType.DMA,
        ],
        1e9,
        smem=(0,),
    )


def first_kernel(
    stage, scale_ref, order_ref, state_hbm, we_ref, gain_ref, wqkv_ref, wproj_ref, wup_ref, wdown_ref,
    top_ref, left_ref, corner_ref, z1_ref, h1_ref, h0_ref, hm_ref, qkv_ref, gp_ref,
    state_ref, ones_ref, mask_ref, e_ref, o_ref, sems,
):
    rows, _, cols, _, _ = state_ref.shape
    width = we_ref.shape[1]
    tokens = WIN * WIN
    chunk = cols * tokens

    def load(i):
        return pltpu.make_async_copy(state_hbm.at[i], state_ref.at[i], sems.at[i])

    for i in range(rows):
        load(i).start()
    ones_ref[...] = head_ones(width, width // HEADS)
    mask_ref[...] = head_stack(HEADS, tokens, width)
    scale = scale_lanes(scale_ref, 0, width)
    stage.need(we_ref, gain_ref)

    def body(i, _):
        load(i).wait()
        x = jnp.concatenate([window(state_ref, i, w).astype(BF) for w in range(cols)], axis=0)
        h0 = nn(x, we_ref[...])
        here = pl.ds(pl.multiple_of(i * chunk, chunk), chunk)
        h0_ref[here, :] = h0
        stage.emit_part(here, h0_ref)
        stage.need_at(i == 0, wqkv_ref)
        qkv = nn(norm(h0, gain_ref[0, 0:1]), wqkv_ref[...]).astype(BF)
        qkv_ref[here, :] = qkv
        stage.emit_part(here, qkv_ref)
        mixed = attention_chunk(qkv, scale, ones_ref, mask_ref, None, e_ref, o_ref, cols, tokens)
        stage.need_at(i == 0, wproj_ref, wup_ref, wdown_ref)
        hm = h0 + nn(mixed, wproj_ref[...]).astype(BF).astype(F32)
        hm_ref[here, :] = hm
        stage.emit_part(here, hm_ref)
        inner, slope = gelu_parts(nn(norm(hm, gain_ref[0, 1:2]), wup_ref[...]))
        gp_ref[here, :] = slope.astype(BF)
        stage.emit_part(here, gp_ref)
        h1 = hm + nn(inner.astype(BF), wdown_ref[...])
        z1 = norm(h1, gain_ref[1, 0:1]).astype(F32)
        for w in range(cols):
            part = slice(w * tokens, (w + 1) * tokens)
            h1_ref[i, :, w, :, :] = h1[part].reshape(WIN, WIN, width)
            z1_ref[i, :, w, :, :] = z1[part].reshape(WIN, WIN, width)
        stage.emit_part(i, z1_ref, h1_ref)
        return 0

    lax.fori_loop(0, rows, body, 0)
    top_ref[...] = z1_ref[0, 0:SHIFT, :, :, :].astype(BF)
    left_ref[...] = z1_ref[:, :, 0, 0:SHIFT, :].astype(BF)
    corner_ref[...] = z1_ref[0, 0:SHIFT, 0, 0:SHIFT, :].astype(BF)


def first_block(order, state5, we, gains, wqkv, wproj, scale, wup, wdown):
    wr, _, wc, _, _ = state5.shape
    width = we.shape[1]
    tokens = wr * wc * WIN * WIN
    chunk = wc * WIN * WIN
    sh = jax.ShapeDtypeStruct
    outs = (
        sh((SHIFT, wc, WIN, width), BF),
        sh((wr, WIN, SHIFT, width), BF),
        sh((SHIFT, SHIFT, width), BF),
        sh((wr, WIN, wc, WIN, width), F32),
        sh((wr, WIN, wc, WIN, width), F32),
        sh((tokens, width), F32),
        sh((tokens, width), F32),
        sh((tokens, 3 * width), BF),
        sh((tokens, wup.shape[2]), BF),
    )
    return staged(
        first_kernel,
        "first_block",
        (scale, order, state5, we, gains, wqkv, wproj, wup, wdown),
        outs,
        [
            pltpu.VMEM(state5.shape, F32),
            pltpu.VMEM((width, width), BF),
            pltpu.VMEM((HEADS * WIN * WIN, width), BF),
            pltpu.VMEM((chunk, HEADS * WIN * WIN), BF),
            pltpu.VMEM((chunk, width), F32),
            pltpu.SemaphoreType.DMA((wr,)),
        ],
        2e9,
        smem=(0,),
        raw=(1, 2),
        layer={5: 0, 6: 0, 7: 0, 8: 0},
    )


def fill_ahead(pad_ref, own, right_ref, below_ref, corner_ref):
    rows, cols, _ = own.shape
    pad_ref[0:rows, 0:cols, :] = own
    pad_ref[0:rows, cols : cols + SHIFT, :] = right_ref[...].astype(F32)
    pad_ref[rows : rows + SHIFT, 0:cols, :] = below_ref[...].astype(F32)
    pad_ref[rows : rows + SHIFT, cols : cols + SHIFT, :] = corner_ref[...].astype(F32)


def rolled_window(pad_ref, i, w):
    block = pad_ref[
        pl.ds(i * WIN + SHIFT, WIN), SHIFT + w * WIN : SHIFT + (w + 1) * WIN, :
    ]
    return block.reshape(WIN * WIN, block.shape[2])


def emit_behind(out_ref, low_ref, east_ref, corner_ref):
    rows, cols, _ = out_ref.shape
    low_ref[...] = out_ref[rows - SHIFT : rows, :, :].astype(BF)
    east_ref[...] = out_ref[:, cols - SHIFT : cols, :].astype(BF)
    corner_ref[...] = out_ref[rows - SHIFT : rows, cols - SHIFT : cols, :].astype(BF)


def shifted_kernel(
    total_rows, stage, start_ref, scale_ref, z1_ref, right_ref, below_ref, corner_ref, wqkv_ref,
    wproj_ref, ans_ref, low_ref, east_ref, last_ref, qkv_ref,
    pad_ref, ones_ref, mask_ref, e_ref, o_ref,
):
    rows, cols, width = z1_ref.shape
    wr, wc = rows // WIN, cols // WIN
    tokens = WIN * WIN
    chunk = wc * tokens
    ones_ref[...] = head_ones(width, width // HEADS)
    mask_ref[...] = head_stack(HEADS, tokens, width)
    scale = scale_lanes(scale_ref, 1, width)
    stage.need(z1_ref, right_ref, below_ref, corner_ref)
    fill_ahead(pad_ref, z1_ref[...], right_ref, below_ref, corner_ref)
    threshold = total_rows - SHIFT - start_ref[0]

    def body(i, _):
        z = jnp.concatenate([rolled_window(pad_ref, i, w).astype(BF) for w in range(wc)], axis=0)
        stage.need_at(i == 0, wqkv_ref, wproj_ref)
        qkv = nn(z, wqkv_ref[...]).astype(BF)
        here = pl.ds(pl.multiple_of(i * chunk, chunk), chunk)
        qkv_ref[here, :] = qkv
        stage.emit_part(here, qkv_ref)
        allowed = side_mask(i, threshold, tokens)
        mixed = attention_chunk(qkv, scale, ones_ref, mask_ref, allowed, e_ref, o_ref, wc, tokens)
        answer = nn(mixed, wproj_ref[...]).astype(BF).astype(F32)
        for w in range(wc):
            ans_ref[pl.ds(i * WIN, WIN), w * WIN : (w + 1) * WIN, :] = answer[
                w * tokens : (w + 1) * tokens
            ].reshape(WIN, WIN, width)
        stage.emit_part(pl.ds(i * WIN, WIN), ans_ref)
        return 0

    lax.fori_loop(0, wr, body, 0)
    emit_behind(ans_ref, low_ref, east_ref, last_ref)


def behind_shapes(rows, cols, width):
    sh = jax.ShapeDtypeStruct
    return (
        sh((rows, cols, width), F32),
        sh((SHIFT, cols, width), BF),
        sh((rows, SHIFT, width), BF),
        sh((SHIFT, SHIFT, width), BF),
    )


def shifted_forward(start, z1, right, below, corner, wqkv, wproj, scale, total_rows):
    rows, cols, width = z1.shape
    tokens = rows * cols
    chunk = cols * WIN
    outs = behind_shapes(rows, cols, width) + (jax.ShapeDtypeStruct((tokens, 3 * width), BF),)
    return staged(
        functools.partial(shifted_kernel, total_rows),
        "shifted_forward",
        (start, scale, z1, right, below, corner, wqkv, wproj),
        outs,
        [
            pltpu.VMEM((rows + SHIFT, cols + WIN, width), F32),
            pltpu.VMEM((width, width), BF),
            pltpu.VMEM((HEADS * WIN * WIN, width), BF),
            pltpu.VMEM((chunk, HEADS * WIN * WIN), BF),
            pltpu.VMEM((chunk, width), F32),
        ],
        1e9,
        smem=(0, 1),
        layer={6: 1, 7: 1},
    )


def fill_behind(pad_ref, own, above_ref, west_ref, corner_ref):
    rows, cols, _ = own.shape
    pad_ref[SHIFT : SHIFT + rows, SHIFT : SHIFT + cols, :] = own
    pad_ref[0:SHIFT, SHIFT : SHIFT + cols, :] = above_ref[...].astype(F32)
    pad_ref[SHIFT : SHIFT + rows, 0:SHIFT, :] = west_ref[...].astype(F32)
    pad_ref[0:SHIFT, 0:SHIFT, :] = corner_ref[...].astype(F32)


def group_jobs(cnt_smem, offset, size, group, body):
    devices = cnt_smem.shape[0]

    def each(d, _):
        valid = cnt_smem[d, 0] - offset
        for g in range(0, size, group):

            @pl.when(valid > g)
            def _():
                body(d, offset + g, pl.multiple_of(d * size + g, group))

        return 0

    lax.fori_loop(0, devices, each, 0)


def gather_part(table_ref, found_ref, idx_smem, cnt_smem, offset, size, group):
    def body(d, slot, row):
        for u in range(group):
            found_ref[pl.ds(row + u, 1), :] = table_ref[pl.ds(idx_smem[d, slot + u], 1), :]

    group_jobs(cnt_smem, offset, size, group, body)


def scatter_part(table_ref, found_ref, idx_smem, cnt_smem, dup_smem, offset, size, group):
    def body(d, slot, row):
        @pl.when(dup_smem[d, slot] == 0)
        def _():
            spots = [idx_smem[d, slot + u] for u in range(group)]
            sums = [
                table_ref[pl.ds(spots[u], 1), :] + found_ref[pl.ds(row + u, 1), :]
                for u in range(group)
            ]
            for u in range(group):
                table_ref[pl.ds(spots[u], 1), :] = sums[u]

        @pl.when(dup_smem[d, slot] != 0)
        def _():
            def one(u, _):
                spot = pl.ds(idx_smem[d, slot + u], 1)
                table_ref[spot, :] = table_ref[spot, :] + found_ref[pl.ds(row + u, 1), :]
                return 0

            lax.fori_loop(0, group, one, 0)

    group_jobs(cnt_smem, offset, size, group, body)


def radiance_part(found_ref, obs_ref, mixed_ref, w1_ref, size):
    devices, _, channels = obs_ref.shape
    batch = min(devices, max(1, 512 // size))

    def body(i, _):
        here = pl.ds(pl.multiple_of(i * batch * size, batch * size), batch * size)
        y = obs_ref[pl.ds(i * batch, batch), 0:size, :].astype(F32)
        y = y.reshape(batch * size, channels)
        t = jnp.tanh(nn(found_ref[here, :].astype(BF), w1_ref[...].astype(BF)))
        pulled = (nn(t.astype(BF), mixed_ref[...]) - y) * (1.0 - t * t)
        found_ref[here, :] = nt(pulled.astype(BF), w1_ref[...].astype(BF))
        return 0

    lax.fori_loop(0, devices // batch, body, 0)


def forecast_kernel(
    parts, group, stage, obs1_ref, h1_ref, ans_ref, above_ref, west_ref, corner_ref, gain_ref,
    wup_ref, wdown_ref, whead_ref, state_ref, w1_in_ref, mixed_ref, obs2_ref, back_ref, inv_ref,
    h2_ref, gp_ref, prior_ref, found3_ref, idx_ref, cnt_ref, dup_ref, table_out_ref, w1_ref,
    pad_ref, table_ref, found1_ref, found2_ref, idx_smem, cnt_smem, dup_smem, sems,
):
    rows, cols, width = h1_ref.shape
    devices = obs1_ref.shape[0]
    tokens = rows * cols
    step = tokens // 2

    stage.need(obs1_ref)
    codes = obs1_ref[:, parts[0] : parts[0] + EXTRA, :].astype(F32)[:, 0, :]
    high = codes[:, :LANES].astype(jnp.int32)
    low = codes[:, LANES : 2 * LANES].astype(jnp.int32)
    point = jnp.where(high > 0, (high - 1) * LANES + low, 0)
    lane = lax.broadcasted_iota(jnp.int32, (devices, LANES), 1)
    idx = jnp.where(
        high > 0, (point % PIX) * tokens + point // PIX, PIX * tokens + lane % group
    )
    idx_ref[...] = idx
    cnt_ref[...] = jnp.broadcast_to(
        jnp.sum(jnp.where(high > 0, 1.0, 0.0), 1, keepdims=True), (devices, LANES)
    ).astype(jnp.int32)
    same = jnp.zeros((devices, LANES), jnp.int32)
    for s in range(1, group):
        hit = (pltpu.roll(idx, s, 1) == idx) & (lane % group >= s)
        same = jnp.maximum(same, jnp.where(hit, 1, 0))
    s = group // 2
    while s:
        same = jnp.maximum(same, pltpu.roll(same, LANES - s, 1))
        s //= 2
    dup_ref[...] = same
    copies = [
        pltpu.make_async_copy(a, b, sems.at[n])
        for n, (a, b) in enumerate(
            ((idx_ref, idx_smem), (cnt_ref, cnt_smem), (dup_ref, dup_smem))
        )
    ]
    for copy in copies:
        copy.start()
    stage.need(h1_ref, ans_ref, above_ref, west_ref, corner_ref)
    fill_behind(pad_ref, ans_ref[...], above_ref, west_ref, corner_ref)
    h2_ref[...] = (h1_ref[...] + pad_ref[0:rows, 0:cols, :]).reshape(tokens, width)
    table_ref[...] = jnp.zeros_like(table_ref)
    stage.need(gain_ref, wup_ref, wdown_ref)

    def forward(i, _):
        here = pl.ds(pl.multiple_of(i * step, step), step)
        h2 = h2_ref[here, :]
        inner, slope = gelu_parts(nn(norm(h2, gain_ref[1, 1:2]), wup_ref[...]))
        gp_ref[here, :] = slope.astype(BF)
        h3 = (h2 + nn(inner.astype(BF), wdown_ref[...])).astype(BF)
        stage.need_at(i == 0, whead_ref, state_ref)
        moved = state_ref[here, :] + nt(h3, whead_ref[...])
        for s in range(PIX):
            there = pl.ds(pl.multiple_of(s * tokens + i * step, WIN), step)
            table_ref[there, 0:VARS] = moved[:, s * VARS : (s + 1) * VARS]
        return 0

    lax.fori_loop(0, 2, forward, 0)
    stage.emit(h2_ref, gp_ref, idx_ref, cnt_ref, dup_ref)
    stage.need(back_ref, inv_ref, w1_in_ref, mixed_ref, obs2_ref)
    prior_ref[...] = inv_ref[...] * (state_ref[...] - back_ref[...])
    stage.emit(prior_ref)
    w1_ref[...] = jnp.zeros_like(w1_ref)
    w1_ref[0:VARS, :] = w1_in_ref[...]
    w1_ref[...] = w1_ref[...].astype(BF).astype(F32)
    for copy in copies:
        copy.wait()
    offsets = (0, parts[0], parts[0] + parts[1])
    founds = (found1_ref, found2_ref, found3_ref)
    for offset, size, found in zip(offsets, parts, founds):
        gather_part(table_ref, found, idx_smem, cnt_smem, offset, size, group)
    stage.emit(found3_ref)
    table_ref = table_out_ref
    table_ref[...] = jnp.zeros_like(table_ref)
    radiance_part(found1_ref, obs1_ref, mixed_ref, w1_ref, parts[0])
    scatter_part(table_ref, found1_ref, idx_smem, cnt_smem, dup_smem, 0, parts[0], group)
    radiance_part(found2_ref, obs2_ref, mixed_ref, w1_ref, parts[1])
    scatter_part(table_ref, found2_ref, idx_smem, cnt_smem, dup_smem, parts[0], parts[1], group)


def forecast(
    h1, ans, above, west, corner, state, background, inv, obs1, obs2, mixed, gains, wup, wdown,
    whead, w1, parts, group,
):
    rows, cols, width = h1.shape
    tokens = rows * cols
    devices = obs1.shape[0]
    sh = jax.ShapeDtypeStruct
    outs = (
        sh((tokens, width), F32),
        sh((tokens, wup.shape[2]), BF),
        sh(state.shape, F32),
        sh((devices * parts[2], LANES), F32),
        sh((devices, LANES), jnp.int32),
        sh((devices, LANES), jnp.int32),
        sh((devices, LANES), jnp.int32),
        sh((PIX * tokens + group, LANES), F32),
        sh((LANES, w1.shape[1]), F32),
    )
    return staged(
        functools.partial(forecast_kernel, parts, group),
        "forecast",
        (
            obs1, h1, ans, above, west, corner, gains, wup, wdown, whead, state, w1, mixed, obs2,
            background, inv,
        ),
        outs,
        [
            pltpu.VMEM((rows + SHIFT, cols + WIN, width), F32),
            pltpu.VMEM((PIX * tokens + group, LANES), F32),
            pltpu.VMEM((devices * parts[0], LANES), F32),
            pltpu.VMEM((devices * parts[1], LANES), F32),
        ]
        + [pltpu.SMEM((devices, LANES), jnp.int32)] * 3
        + [pltpu.SemaphoreType.DMA((3,))],
        3e9,
        layer={7: 1, 8: 1},
    )


def adjoint_kernel(
    parts, group, stage, idx_smem, cnt_smem, dup_smem, w1_ref, mixed_ref, work_ref, obs3_ref,
    table_ref, prior_ref, whead_ref, wdown_ref, gp_ref, wup_ref, h2_ref, gain_ref,
    top_ref, left_ref, edge_ref, third_ref, out_ref, moved_ref,
):
    rows, cols, width = third_ref.shape
    tokens = rows * cols
    step = tokens // 2
    stage.need(w1_ref, mixed_ref, work_ref, obs3_ref)
    radiance_part(work_ref, obs3_ref, mixed_ref, w1_ref, parts[2])
    stage.need(table_ref)
    scatter_part(
        table_ref, work_ref, idx_smem, cnt_smem, dup_smem, parts[0] + parts[1], parts[2], group
    )
    stage.need(prior_ref, whead_ref, wdown_ref, gp_ref, wup_ref, h2_ref, gain_ref)
    half = rows // 2

    def backward(i, _):
        here = pl.ds(pl.multiple_of(i * step, step), step)
        for s in range(PIX):
            there = pl.ds(pl.multiple_of(s * tokens + i * step, WIN), step)
            moved_ref[:, s * VARS : (s + 1) * VARS] = table_ref[there, 0:VARS]
        moved = moved_ref[...]
        out_ref[here, :] = moved + prior_ref[here, :]
        stage.emit_part(here, out_ref)
        grad = nn(moved.astype(BF), whead_ref[...]).astype(BF)
        d_inner = nt(grad, wdown_ref[...]) * gp_ref[here, :].astype(F32)
        d_normed = nt(d_inner.astype(BF), wup_ref[...])
        third = grad.astype(F32) + norm_back(h2_ref[here, :], gain_ref[1, 1:2], d_normed)
        third_ref[pl.ds(i * half, half), :, :] = third.reshape(half, cols, width)
        stage.emit_part(pl.ds(i * half, half), third_ref)
        return 0

    lax.fori_loop(0, 2, backward, 0)
    top_ref[...] = third_ref[0:SHIFT, :, :].astype(BF)
    left_ref[...] = third_ref[:, 0:SHIFT, :].astype(BF)
    edge_ref[...] = third_ref[0:SHIFT, 0:SHIFT, :].astype(BF)


def adjoint(
    idx, cnt, dup, found, obs3, mixed, w1, h2, gp, gains, wup, wdown, whead, prior, sums, parts,
    group, rows, cols,
):
    width = h2.shape[1]
    third, top, left, edge = behind_shapes(rows, cols, width)
    outs = (top, left, edge, third, jax.ShapeDtypeStruct(prior.shape, F32))
    return staged(
        functools.partial(adjoint_kernel, parts, group),
        "adjoint",
        (idx, cnt, dup, w1, mixed, found, obs3, sums, prior, whead, wdown, gp, wup, h2, gains),
        outs,
        [pltpu.VMEM((prior.shape[0] // 2, prior.shape[1]), F32)],
        2e9,
        smem=(0, 1, 2),
        layer={10: 1, 12: 1},
    )


def shifted_back_kernel(
    total_rows, stage, start_ref, scale_ref, third_ref, right_ref, below_ref, corner_ref,
    wproj_ref, qkv_ref, wqkv_ref, dz_ref, low_ref, east_ref, last_ref,
    pad_ref, ones_ref, mask_ref, dq_ref, dk_ref, dv_ref,
):
    rows, cols, width = third_ref.shape
    wr, wc = rows // WIN, cols // WIN
    tokens = WIN * WIN
    chunk = wc * tokens
    ones_ref[...] = head_ones(width, width // HEADS)
    mask_ref[...] = head_stack(HEADS, tokens, width)
    scale = scale_lanes(scale_ref, 1, width)
    stage.need(third_ref, right_ref, below_ref, corner_ref)
    fill_ahead(pad_ref, third_ref[...], right_ref, below_ref, corner_ref)
    threshold = total_rows - SHIFT - start_ref[0]

    def body(i, _):
        d_answer = jnp.concatenate(
            [rolled_window(pad_ref, i, w).astype(BF) for w in range(wc)], axis=0
        )
        stage.need_at(i == 0, wproj_ref, qkv_ref, wqkv_ref)
        d_out = nt(d_answer, wproj_ref[...]).astype(BF)
        allowed = side_mask(i, threshold, tokens)
        qkv = qkv_ref[pl.ds(pl.multiple_of(i * chunk, chunk), chunk), :]
        d_qkv = attention_chunk_back(
            qkv, d_out, scale, ones_ref, mask_ref, allowed,
            dq_ref, dk_ref, dv_ref, wc, tokens,
        )
        dz = nt(d_qkv, wqkv_ref[...]).astype(BF).astype(F32)
        for w in range(wc):
            dz_ref[pl.ds(i * WIN, WIN), w * WIN : (w + 1) * WIN, :] = dz[
                w * tokens : (w + 1) * tokens
            ].reshape(WIN, WIN, width)
        stage.emit_part(pl.ds(i * WIN, WIN), dz_ref)
        return 0

    lax.fori_loop(0, wr, body, 0)
    emit_behind(dz_ref, low_ref, east_ref, last_ref)


def shifted_backward(start, third, right, below, corner, qkv, wqkv, wproj, scale, total_rows):
    rows, cols, width = third.shape
    chunk = cols * WIN
    outs = behind_shapes(rows, cols, width)
    return staged(
        functools.partial(shifted_back_kernel, total_rows),
        "shifted_backward",
        (start, scale, third, right, below, corner, wproj, qkv, wqkv),
        outs,
        [
            pltpu.VMEM((rows + SHIFT, cols + WIN, width), F32),
            pltpu.VMEM((width, width), BF),
            pltpu.VMEM((HEADS * WIN * WIN, width), BF),
        ]
        + [pltpu.VMEM((chunk, width), F32)] * 3,
        1e9,
        smem=(0, 1),
        layer={6: 1, 8: 1},
    )


def last_kernel(
    stage, scale_ref, partial_hbm, dz_ref, above_ref, west_ref, corner_ref, third_ref, h1_ref,
    gain_ref, wdown_ref, gp_ref, wup_ref, hm_ref, wproj_ref, qkv_ref, wqkv_ref, h0_ref, we_ref,
    out_hbm,
    pad_ref, ones_ref, mask_ref, dq_ref, dk_ref, dv_ref, out_ref, in_sems, out_sems,
):
    rows, cols, width = dz_ref.shape
    wr, wc = rows // WIN, cols // WIN
    tokens = WIN * WIN
    chunk = wc * tokens

    def rows_of(ref, i):
        return ref.at[pl.ds(i * WIN, WIN)]

    ones_ref[...] = head_ones(width, width // HEADS)
    mask_ref[...] = head_stack(HEADS, tokens, width)
    scale = scale_lanes(scale_ref, 0, width)
    for i in range(wr):
        pltpu.make_async_copy(rows_of(partial_hbm, i), rows_of(out_ref, i), in_sems.at[i]).start()
    stage.need(dz_ref, above_ref, west_ref, corner_ref)
    fill_behind(pad_ref, dz_ref[...], above_ref, west_ref, corner_ref)

    def body(i, _):
        here = pl.ds(pl.multiple_of(i * chunk, chunk), chunk)
        band = pl.ds(i * WIN, WIN)

        def take(ref):
            return jnp.concatenate(
                [
                    ref[band, w * WIN : (w + 1) * WIN, :].reshape(tokens, width)
                    for w in range(wc)
                ],
                axis=0,
            )

        stage.need_at(i == 0, third_ref, h1_ref, gain_ref, wdown_ref, gp_ref, wup_ref)
        second = take(third_ref) + norm_back(take(h1_ref), gain_ref[1, 0:1], take(pad_ref))
        d_inner = nt(second.astype(BF), wdown_ref[...]) * gp_ref[here, :].astype(F32)
        d_normed = nt(d_inner.astype(BF), wup_ref[...])
        stage.need_at(i == 0, hm_ref, wproj_ref, qkv_ref, wqkv_ref, h0_ref, we_ref)
        d_hm = second + norm_back(hm_ref[here, :], gain_ref[0, 1:2], d_normed)
        d_out = nt(d_hm.astype(BF), wproj_ref[...]).astype(BF)
        d_qkv = attention_chunk_back(
            qkv_ref[here, :], d_out, scale, ones_ref, mask_ref, None,
            dq_ref, dk_ref, dv_ref, wc, tokens,
        )
        dz = nt(d_qkv, wqkv_ref[...])
        d_h0 = (d_hm + norm_back(h0_ref[here, :], gain_ref[0, 0:1], dz)).astype(BF)
        pltpu.make_async_copy(rows_of(partial_hbm, i), rows_of(out_ref, i), in_sems.at[i]).wait()
        for w in range(wc):
            grad = nt(d_h0[w * tokens : (w + 1) * tokens], we_ref[...])
            grad = grad.reshape(WIN, WIN, grad.shape[1])
            spot = (band, slice(w * WIN, (w + 1) * WIN), slice(None))
            out_ref[spot] = grad + out_ref[spot]
        pltpu.make_async_copy(rows_of(out_ref, i), rows_of(out_hbm, i), out_sems.at[i]).start()
        return 0

    lax.fori_loop(0, wr, body, 0)
    for i in range(wr):
        pltpu.make_async_copy(rows_of(out_ref, i), rows_of(out_hbm, i), out_sems.at[i]).wait()


def last_block(
    third, dz, above, west, corner, h1, h0, hm, qkv, gp, we, gains, wqkv, wproj, scale,
    wup, wdown, partial,
):
    rows, cols, width = dz.shape
    chunk = cols * WIN
    (result,) = staged(
        last_kernel,
        "last_block",
        (
            scale, partial, dz, above, west, corner, third, h1, gains, wdown, gp, wup, hm, wproj,
            qkv, wqkv, h0, we,
        ),
        (jax.ShapeDtypeStruct(partial.shape, F32),),
        [
            pltpu.VMEM((rows + SHIFT, cols + WIN, width), F32),
            pltpu.VMEM((width, width), BF),
            pltpu.VMEM((HEADS * WIN * WIN, width), BF),
        ]
        + [pltpu.VMEM((chunk, width), F32)] * 3
        + [
            pltpu.VMEM(partial.shape, F32),
            pltpu.SemaphoreType.DMA((rows // WIN,)),
            pltpu.SemaphoreType.DMA((rows // WIN,)),
        ],
        2e9,
        smem=(0,),
        raw=(1,),
        raw_outs=(0,),
        layer={9: 0, 11: 0, 13: 0, 15: 0},
    )
    return result


def neighbour(x, by_lat, by_lon):
    lat, lon = lax.axis_size("lat"), lax.axis_size("lon")
    pairs = [
        (a * lon + b, ((a + by_lat) % lat) * lon + (b + by_lon) % lon)
        for a in range(lat)
        for b in range(lon)
    ]
    return lax.ppermute(x, ("lat", "lon"), pairs)


def exchange(x):
    return lax.all_to_all(x, ("lat", "lon"), split_axis=0, concat_axis=0, tiled=True)


def local(
    state,
    background,
    inv_background,
    w_embed,
    norm_gain,
    w_qkv,
    w_proj,
    head_scale,
    w_up,
    w_down,
    w_head,
    w_obs1,
    w_obs2,
    r_inverse,
    obs_values,
    obs_owner,
    obs_point,
    obs_count,
):
    rows, cols, patch_values = state.shape
    width = w_embed.shape[1]
    total_rows = rows * lax.axis_size("lat")
    row_start = (lax.axis_index("lat") * rows).astype(jnp.int32).reshape(1)
    devices = lax.axis_size("lat") * lax.axis_size("lon")
    slots = obs_values.shape[0]
    cap = 2 * slots // devices

    parts, group = split(cap)

    send1, send2, send3, mixed = route(
        obs_owner.reshape(1, slots), obs_point.reshape(1, slots), obs_count, obs_values,
        r_inverse, w_obs2, devices, parts,
    )
    obs1 = exchange(send1)
    state5 = state.reshape(rows // WIN, WIN, cols // WIN, WIN, patch_values)
    top, left, corner, z1, h1, h0, hm, qkv0, gp0 = first_block(
        mixed, state5, w_embed, norm_gain, w_qkv, w_proj, head_scale, w_up, w_down
    )
    z1 = z1.reshape(rows, cols, width)
    h1 = h1.reshape(rows, cols, width)
    below = neighbour(top.reshape(SHIFT, cols, width), -1, 0)
    right = neighbour(left.reshape(rows, SHIFT, width), 0, -1)
    corner = neighbour(corner, -1, -1)
    below, right, corner, obs1, send2 = lax.optimization_barrier(
        (below, right, corner, obs1, send2)
    )
    obs2 = exchange(send2)
    answer, low, east, last, qkv1 = shifted_forward(
        row_start, z1, right, below, corner, w_qkv, w_proj, head_scale, total_rows
    )
    above = neighbour(low, 1, 0)
    west = neighbour(east, 0, 1)
    last = neighbour(last, 1, 1)
    above, west, last, obs2, send3 = lax.optimization_barrier((above, west, last, obs2, send3))
    obs3 = exchange(send3)
    flat = (rows * cols, patch_values)
    h2, gp1, prior, found, idx, cnt, dup, sums, w1 = forecast(
        h1, answer, above, west, last, state.reshape(flat), background.reshape(flat),
        inv_background.reshape(1, -1), obs1, obs2, mixed, norm_gain, w_up, w_down, w_head.T,
        w_obs1, parts, group,
    )
    top, left, corner, third, partial = adjoint(
        idx, cnt, dup, found, obs3, mixed, w1, h2, gp1, norm_gain, w_up, w_down, w_head.T, prior,
        sums,
        parts, group, rows, cols,
    )
    below = neighbour(top, -1, 0)
    right = neighbour(left, 0, -1)
    corner = neighbour(corner, -1, -1)
    dz, low, east, last = shifted_backward(
        row_start, third, right, below, corner, qkv1, w_qkv, w_proj, head_scale, total_rows
    )
    above = neighbour(low, 1, 0)
    west = neighbour(east, 0, 1)
    last = neighbour(last, 1, 1)
    return last_block(
        third, dz, above, west, last, h1, h0, hm, qkv0, gp0, w_embed, norm_gain, w_qkv, w_proj,
        head_scale, w_up, w_down, partial.reshape(state.shape),
    )


def solution(mesh):
    placed = (
        P("lat", "lon", None),
        P("lat", "lon", None),
        P(),
        P(),
        P(),
        P(),
        P(),
        P(),
        P(),
        P(),
        P(),
        P(),
        P(),
        P(),
        P(("lat", "lon"), None),
        P(("lat", "lon"), None),
        P(("lat", "lon")),
        P(("lat", "lon")),
    )
    return jax.shard_map(
        local, mesh=mesh, in_specs=placed, out_specs=P("lat", "lon", None), check_vma=False
    )
```

```python
import functools

import jax
import jax.numpy as jnp
from jax import lax
from jax.experimental import pallas as pl
from jax.experimental.pallas import tpu as pltpu
from jax.sharding import PartitionSpec as P

HEADS = 8
VARS = 69
PIX = 16
WIN = 8
SHIFT = 4
LANES = 128
EXTRA = 8
EPS = 1e-05
BF = jnp.bfloat16
F32 = jnp.float32
SQRT_2_OVER_PI = 0.7978845608028654
CUBIC = 0.044715

SMEM = pl.BlockSpec(memory_space=pltpu.SMEM)
VMEM = pl.BlockSpec(memory_space=pltpu.VMEM)
HBM = pl.BlockSpec(memory_space=pltpu.HBM)
MIB = 1024 * 1024


class Stage:
    def __init__(self):
        self.inputs = {}
        self.outputs = {}
        self.waited = set()
        self.sent = set()

    def need(self, *refs):
        for ref in refs:
            if id(ref) not in self.waited:
                self.waited.add(id(ref))
                self.inputs[id(ref)].wait()

    def need_at(self, first, *refs):
        pending = [ref for ref in refs if id(ref) not in self.waited]
        self.waited.update(id(ref) for ref in pending)

        @pl.when(first)
        def _():
            for ref in pending:
                self.inputs[id(ref)].wait()

    def emit_part(self, part, *refs):
        for ref in refs:
            self.sent.add(id(ref))
            self.outputs[id(ref)].part(part).start()

    def emit(self, *refs):
        for ref in refs:
            if id(ref) not in self.sent:
                self.sent.add(id(ref))
                self.outputs[id(ref)].start()

    def close(self):
        for key, copy in self.inputs.items():
            if key not in self.waited:
                copy.wait()
        for key, copy in self.outputs.items():
            if key not in self.sent:
                copy.start()
        for copy in self.outputs.values():
            copy.wait()


class Outgoing:
    def __init__(self, source, target, sem):
        self.refs = (source, target, sem)

    def part(self, part):
        source, target, sem = self.refs
        return pltpu.make_async_copy(source.at[part], target.at[part], sem)

    def start(self):
        pltpu.make_async_copy(*self.refs).start()

    def wait(self):
        pltpu.make_async_copy(*self.refs).wait()


def staged(
    body, name, args, outs, scratch, flops, smem=(), raw=(), raw_outs=(), layer=None, vmem=()
):
    layer = layer or {}
    count = len(args)
    in_buffers = []
    for i, x in enumerate(args):
        if i not in smem and i not in raw and i not in vmem:
            shape = x.shape[1:] if i in layer else x.shape
            in_buffers.append((i, pltpu.VMEM(shape, x.dtype)))
    out_buffers = [
        (j, pltpu.VMEM(o.shape, o.dtype)) for j, o in enumerate(outs) if j not in raw_outs
    ]

    def kernel(*refs):
        ins = list(refs[:count])
        results = list(refs[count : count + len(outs)])
        rest = list(refs[count + len(outs) :])
        ins_vmem = rest[: len(in_buffers)]
        outs_vmem = rest[len(in_buffers) : len(in_buffers) + len(out_buffers)]
        in_sems, out_sems = rest[-2:]
        extra = rest[len(in_buffers) + len(out_buffers) : -2]
        stage = Stage()
        stage.waited.update(id(ins[i]) for i in vmem)
        for n, ((i, _), buffer) in enumerate(zip(in_buffers, ins_vmem)):
            source = ins[i].at[layer[i]] if i in layer else ins[i]
            copy = pltpu.make_async_copy(source, buffer, in_sems.at[n])
            copy.start()
            stage.inputs[id(buffer)] = copy
            ins[i] = buffer
        for n, ((j, _), buffer) in enumerate(zip(out_buffers, outs_vmem)):
            stage.outputs[id(buffer)] = Outgoing(buffer, results[j], out_sems.at[n])
            results[j] = buffer
        body(stage, *ins, *results, *extra)
        stage.close()

    return pl.pallas_call(
        kernel,
        out_shape=tuple(outs),
        in_specs=[
            SMEM if i in smem else VMEM if i in vmem else HBM for i in range(count)
        ],
        out_specs=(HBM,) * len(outs),
        scratch_shapes=[b for _, b in in_buffers]
        + [b for _, b in out_buffers]
        + list(scratch)
        + [
            pltpu.SemaphoreType.DMA((max(1, len(in_buffers)),)),
            pltpu.SemaphoreType.DMA((max(1, len(out_buffers)),)),
        ],
        compiler_params=pltpu.CompilerParams(vmem_limit_bytes=60 * MIB),
        cost_estimate=pl.CostEstimate(
            flops=int(flops), bytes_accessed=8 * MIB, transcendentals=0
        ),
        name=name,
    )(*args)


def scale_lanes(scale_ref, block, width):
    head = lax.broadcasted_iota(jnp.int32, (1, width), 1) // (width // HEADS)
    row = jnp.zeros((1, width), F32)
    for h in range(HEADS):
        row = jnp.where(head == h, scale_ref[block, h], row)
    return row


def nn(a, b):
    return lax.dot_general(a, b, (((1,), (0,)), ((), ())), preferred_element_type=F32)


def nt(a, b):
    return lax.dot_general(a, b, (((1,), (1,)), ((), ())), preferred_element_type=F32)


def tn(a, b):
    return lax.dot_general(a, b, (((0,), (0,)), ((), ())), preferred_element_type=F32)


def norm_parts(h):
    mean = jnp.mean(h, -1, keepdims=True)
    centred = h - mean
    spread = jnp.mean(centred * centred, -1, keepdims=True)
    rstd = lax.rsqrt(spread + EPS)
    return centred * rstd, rstd


def norm(h, gain):
    return (norm_parts(h)[0] * gain).astype(BF)


def norm_back(h, gain, cotangent):
    xhat, rstd = norm_parts(h)
    scaled = cotangent * gain
    m1 = jnp.mean(scaled, -1, keepdims=True)
    m2 = jnp.mean(scaled * xhat, -1, keepdims=True)
    return rstd * (scaled - m1 - xhat * m2)


def gelu_parts(u):
    square = u * u
    t = jnp.tanh(u * (SQRT_2_OVER_PI + SQRT_2_OVER_PI * CUBIC * square))
    half = 0.5 + 0.5 * t
    value = u * half
    rate = 2.0 * SQRT_2_OVER_PI + 6.0 * SQRT_2_OVER_PI * CUBIC * square
    return value, half + value * (1.0 - half) * rate


def head_ones(width, size):
    a = lax.broadcasted_iota(jnp.int32, (width, width), 0) // size
    b = lax.broadcasted_iota(jnp.int32, (width, width), 1) // size
    return (a == b).astype(F32).astype(BF)


def head_stack(tokens, size):
    heads = LANES // size
    a = lax.broadcasted_iota(jnp.int32, (heads * tokens, LANES), 0) // tokens
    b = lax.broadcasted_iota(jnp.int32, (heads * tokens, LANES), 1) // size
    return (a == b).astype(F32).astype(BF)


def stacked(x, mask):
    copies = mask.shape[0] // x.shape[0]
    return [
        jnp.concatenate([x[:, t : t + LANES]] * copies, axis=0) * mask
        for t in range(0, x.shape[1], LANES)
    ]


def scores_of(x, blocks):
    return jnp.concatenate(
        [nt(x[:, t * LANES : (t + 1) * LANES], b) for t, b in enumerate(blocks)], axis=1
    )


def mix_of(p, blocks):
    rows = blocks[0].shape[0]
    return jnp.concatenate(
        [nn(p[:, t * rows : (t + 1) * rows], b) for t, b in enumerate(blocks)], axis=1
    )


def side_mask(window_row, threshold, tokens):
    shape = (tokens, HEADS * tokens)
    a = lax.broadcasted_iota(jnp.int32, shape, 0) // WIN
    b = (lax.broadcasted_iota(jnp.int32, shape, 1) % tokens) // WIN
    first = (window_row * WIN + a) >= threshold
    second = (window_row * WIN + b) >= threshold
    return jnp.where(first == second, 1.0, 0.0).astype(F32)


def window(ref, i, w):
    block = ref[i, :, w, :, :]
    return block.reshape(block.shape[0] * block.shape[1], block.shape[2])


def attention_chunk(qkv, scale, ones_ref, mask_ref, allowed, e_ref, o_ref, count, tokens):
    width = qkv.shape[1] // 3
    q = qkv[:, :width].astype(F32)
    k = qkv[:, width : 2 * width].astype(F32)
    v = qkv[:, 2 * width :]
    ones = ones_ref[...]
    qs = (q * lax.rsqrt(nn((q * q).astype(BF), ones) + 1.0) * scale).astype(BF)
    kn = (k * lax.rsqrt(nn((k * k).astype(BF), ones) + 1.0)).astype(BF)
    mask = mask_ref[...]
    for w in range(count):
        part = slice(w * tokens, (w + 1) * tokens)
        expo = jnp.exp(scores_of(qs[part], stacked(kn[part], mask)))
        if allowed is not None:
            expo = expo * allowed
        expo = expo.astype(BF)
        e_ref[part] = expo
        o_ref[part] = mix_of(expo, stacked(v[part], mask))
    total = mix_of(e_ref[...], [mask] * (width // LANES))
    return (o_ref[...] / total).astype(BF)


def attention_chunk_back(
    qkv, d_out, scale, ones_ref, mask_ref, allowed, dq_ref, dk_ref, dv_ref, count, tokens
):
    width = qkv.shape[1] // 3
    size = width // HEADS
    q = qkv[:, :width].astype(F32)
    k = qkv[:, width : 2 * width].astype(F32)
    v = qkv[:, 2 * width :]
    ones = ones_ref[...]
    rq = lax.rsqrt(nn((q * q).astype(BF), ones) + 1.0)
    rk = lax.rsqrt(nn((k * k).astype(BF), ones) + 1.0)
    qs = (q * rq * scale).astype(BF)
    kn = (k * rk).astype(BF)
    mask = mask_ref[...]
    lane_head = lax.broadcasted_iota(jnp.int32, (1, LANES), 1) // size
    per_tile = LANES // size
    for w in range(count):
        part = slice(w * tokens, (w + 1) * tokens)
        kw = kn[part]
        qm = stacked(qs[part], mask)
        dm = stacked(d_out[part], mask)
        expo = jnp.exp(scores_of(kw, qm))
        if allowed is not None:
            expo = expo * allowed
        p = expo * (1.0 / jnp.sum(expo, 0, keepdims=True))
        dp = scores_of(v[part], dm)
        ds = (p * (dp - jnp.sum(p * dp, 0, keepdims=True))).astype(BF)
        dv_ref[part] = mix_of(p.astype(BF), dm)
        dk_ref[part] = mix_of(ds, qm)
        tiles = []
        for tile in range(width // LANES):
            span = per_tile * tokens
            full = tn(
                ds[:, tile * span : (tile + 1) * span], kw[:, tile * LANES : (tile + 1) * LANES]
            )
            total = None
            for s in range(per_tile):
                block = full[s * tokens : (s + 1) * tokens]
                block = jnp.where(lane_head == s, block, 0.0)
                total = block if total is None else total + block
            tiles.append(total)
        dq_ref[part] = jnp.concatenate(tiles, axis=1)
    dqs = dq_ref[...]
    dkn = dk_ref[...]
    dq = scale * rq * (dqs - q * (rq * rq) * nn((q * dqs).astype(BF), ones))
    dk = rk * (dkn - k * (rk * rk) * nn((k * dkn).astype(BF), ones))
    return jnp.concatenate([dq.astype(BF), dk.astype(BF), dv_ref[...].astype(BF)], axis=1)


def split(cap):
    first = max(8, cap // 4)
    return (first, first, cap - 2 * first), min(16, first)


def route_kernel(
    parts, stage, count_ref, owner_ref, point_ref, r_ref, w2_ref, values_ref,
    send1_ref, send2_ref, send3_ref, mixed_ref, y_ref, buf_ref, tgt_ref, tgt_smem, sem,
):
    cap = sum(parts)
    slots = owner_ref.shape[1]
    devices = send1_ref.shape[0]
    stage.need(owner_ref, point_ref)
    owner = owner_ref[...]
    live = lax.broadcasted_iota(jnp.int32, (1, slots), 1) < count_ref[0]
    match = lax.broadcasted_iota(jnp.int32, (devices, slots), 0) == owner
    match = jnp.where(match, 1.0, 0.0).astype(F32)
    a = lax.broadcasted_iota(jnp.int32, (LANES, LANES), 0)
    b = lax.broadcasted_iota(jnp.int32, (LANES, LANES), 1)
    upper = jnp.where(a < b, 1.0, 0.0).astype(BF)
    chunks = slots // LANES
    flat = jnp.concatenate(
        [match[:, c * LANES : (c + 1) * LANES] for c in range(chunks)], axis=0
    )
    before = nn(flat.astype(BF), upper)
    carry = jnp.zeros((devices, 1), F32)
    ranks = []
    dump = devices * cap
    for c in range(chunks):
        here = match[:, c * LANES : (c + 1) * LANES]
        seen = before[c * devices : (c + 1) * devices] + carry
        ranks.append(jnp.sum(here * seen, 0, keepdims=True))
        span = slice(c * LANES, (c + 1) * LANES)
        spot = owner[:, span] * cap + ranks[-1].astype(jnp.int32)
        tgt_ref[c : c + 1, :] = jnp.where(live[:, span], spot, dump)
        carry = carry + jnp.sum(here, 1, keepdims=True)
    rank = jnp.concatenate(ranks, axis=1).astype(jnp.int32)
    copy = pltpu.make_async_copy(tgt_ref, tgt_smem, sem)
    copy.start()
    place = lax.broadcasted_iota(jnp.int32, (cap, slots), 0) == rank
    place = jnp.where(place & live, 1.0, 0.0).astype(BF)
    point = point_ref[...]
    high = (match * (point // LANES + 1).astype(F32)).astype(BF)
    low = (match * (point % LANES).astype(F32)).astype(BF)
    high = nt(high, place)
    low = nt(low, place)
    stage.need(r_ref, w2_ref, values_ref)
    best = lax.Precision.HIGHEST
    dims = (((1,), (1,)), ((), ()))
    m2 = lax.dot_general(
        r_ref[...], w2_ref[...], dims, precision=best, preferred_element_type=F32
    )
    mixed_ref[...] = jnp.dot(
        w2_ref[...], m2, precision=best, preferred_element_type=F32
    ).astype(BF)
    y = nn(values_ref[...].astype(BF), m2.astype(BF))
    y_ref[0, :, :] = y[:, :LANES]
    y_ref[1, :, :] = y[:, LANES:]
    buf_ref[...] = jnp.zeros_like(buf_ref)
    copy.wait()
    unroll = 16

    def move(c, _):
        base = pl.multiple_of(c * LANES, LANES)
        for start in range(0, LANES, unroll):
            spots = [tgt_smem[c, start + u] for u in range(unroll)]
            for half in range(2):
                for u in range(unroll):
                    buf_ref[half, pl.ds(spots[u], 1), :] = y_ref[
                        half, pl.ds(base + start + u, 1), :
                    ]
        return 0

    lax.fori_loop(0, chunks, move, 0)
    for d in range(devices):
        offset = d * cap
        for ref, size in zip((send1_ref, send2_ref, send3_ref), parts):
            for half in range(2):
                ref[d, 0:size, half * LANES : (half + 1) * LANES] = buf_ref[
                    half, offset : offset + size, :
                ].astype(BF)
            offset += size
    fill = ((0, 0), (0, LANES - cap))
    codes = jnp.concatenate([jnp.pad(high, fill), jnp.pad(low, fill)], axis=1)
    for d in range(devices):
        send1_ref[d, parts[0] : parts[0] + EXTRA, :] = jnp.broadcast_to(
            codes[d : d + 1], (EXTRA, 2 * LANES)
        ).astype(BF)


def route(owner, point, count, values, r_inverse, w2, devices, parts):
    slots, channels = values.shape
    cap = sum(parts)
    sizes = (parts[0] + EXTRA,) + tuple(parts[1:])
    return staged(
        functools.partial(route_kernel, parts),
        "route",
        (count, owner, point, r_inverse, w2, values),
        tuple(jax.ShapeDtypeStruct((devices, n, channels), BF) for n in sizes)
        + (jax.ShapeDtypeStruct(w2.shape, BF),),
        [
            pltpu.VMEM((2, slots, LANES), F32),
            pltpu.VMEM((2, devices * cap + EXTRA, LANES), F32),
            pltpu.VMEM((slots // LANES, LANES), jnp.int32),
            pltpu.SMEM((slots // LANES, LANES), jnp.int32),
            pltpu.SemaphoreType.DMA,
        ],
        1e9,
        smem=(0,),
    )


def first_kernel(
    stage, scale_ref, order_ref, state_hbm, we_ref, gain_ref, wqkv_ref, wproj_ref, wup_ref, wdown_ref,
    top_ref, left_ref, corner_ref, z1_ref, h1_ref, h0_ref, hm_ref, qkv_ref, gp_ref,
    state_ref, ones_ref, mask_ref, e_ref, o_ref, sems,
):
    rows, _, cols, _, _ = state_ref.shape
    width = we_ref.shape[1]
    tokens = WIN * WIN
    chunk = cols * tokens

    def load(i):
        return pltpu.make_async_copy(state_hbm.at[i], state_ref.at[i], sems.at[i])

    for i in range(rows):
        load(i).start()
    ones_ref[...] = head_ones(width, width // HEADS)
    mask_ref[...] = head_stack(tokens, width // HEADS)
    scale = scale_lanes(scale_ref, 0, width)
    stage.need(we_ref, gain_ref)

    def body(i, _):
        load(i).wait()
        x = jnp.concatenate([window(state_ref, i, w).astype(BF) for w in range(cols)], axis=0)
        h0 = nn(x, we_ref[...])
        here = pl.ds(pl.multiple_of(i * chunk, chunk), chunk)
        h0_ref[here, :] = h0
        stage.emit_part(here, h0_ref)
        stage.need_at(i == 0, wqkv_ref)
        qkv = nn(norm(h0, gain_ref[0, 0:1]), wqkv_ref[...]).astype(BF)
        qkv_ref[here, :] = qkv
        stage.emit_part(here, qkv_ref)
        mixed = attention_chunk(qkv, scale, ones_ref, mask_ref, None, e_ref, o_ref, cols, tokens)
        stage.need_at(i == 0, wproj_ref, wup_ref, wdown_ref)
        hm = h0 + nn(mixed, wproj_ref[...]).astype(BF).astype(F32)
        hm_ref[here, :] = hm
        stage.emit_part(here, hm_ref)
        inner, slope = gelu_parts(nn(norm(hm, gain_ref[0, 1:2]), wup_ref[...]))
        gp_ref[here, :] = slope.astype(BF)
        stage.emit_part(here, gp_ref)
        h1 = hm + nn(inner.astype(BF), wdown_ref[...])
        z1 = norm(h1, gain_ref[1, 0:1]).astype(F32)
        for w in range(cols):
            part = slice(w * tokens, (w + 1) * tokens)
            h1_ref[i, :, w, :, :] = h1[part].reshape(WIN, WIN, width)
            z1_ref[i, :, w, :, :] = z1[part].reshape(WIN, WIN, width)
        stage.emit_part(i, z1_ref, h1_ref)
        return 0

    lax.fori_loop(0, rows, body, 0)
    top_ref[...] = z1_ref[0, 0:SHIFT, :, :, :].astype(BF)
    left_ref[...] = z1_ref[:, :, 0, 0:SHIFT, :].astype(BF)
    corner_ref[...] = z1_ref[0, 0:SHIFT, 0, 0:SHIFT, :].astype(BF)


def first_block(order, state5, we, gains, wqkv, wproj, scale, wup, wdown):
    wr, _, wc, _, _ = state5.shape
    width = we.shape[1]
    tokens = wr * wc * WIN * WIN
    chunk = wc * WIN * WIN
    sh = jax.ShapeDtypeStruct
    outs = (
        sh((SHIFT, wc, WIN, width), BF),
        sh((wr, WIN, SHIFT, width), BF),
        sh((SHIFT, SHIFT, width), BF),
        sh((wr, WIN, wc, WIN, width), F32),
        sh((wr, WIN, wc, WIN, width), F32),
        sh((tokens, width), F32),
        sh((tokens, width), F32),
        sh((tokens, 3 * width), BF),
        sh((tokens, wup.shape[2]), BF),
    )
    return staged(
        first_kernel,
        "first_block",
        (scale, order, state5, we, gains, wqkv, wproj, wup, wdown),
        outs,
        [
            pltpu.VMEM(state5.shape, F32),
            pltpu.VMEM((width, width), BF),
            pltpu.VMEM((LANES * HEADS // width * WIN * WIN, LANES), BF),
            pltpu.VMEM((chunk, HEADS * WIN * WIN), BF),
            pltpu.VMEM((chunk, width), F32),
            pltpu.SemaphoreType.DMA((wr,)),
        ],
        2e9,
        smem=(0,),
        raw=(1, 2),
        layer={5: 0, 6: 0, 7: 0, 8: 0},
    )


def fill_ahead(pad_ref, own, right_ref, below_ref, corner_ref):
    rows, cols, _ = own.shape
    pad_ref[0:rows, 0:cols, :] = own
    pad_ref[0:rows, cols : cols + SHIFT, :] = right_ref[...].astype(F32)
    pad_ref[rows : rows + SHIFT, 0:cols, :] = below_ref[...].astype(F32)
    pad_ref[rows : rows + SHIFT, cols : cols + SHIFT, :] = corner_ref[...].astype(F32)


def rolled_window(pad_ref, i, w):
    block = pad_ref[
        pl.ds(i * WIN + SHIFT, WIN), SHIFT + w * WIN : SHIFT + (w + 1) * WIN, :
    ]
    return block.reshape(WIN * WIN, block.shape[2])


def emit_behind(out_ref, low_ref, east_ref, corner_ref):
    rows, cols, _ = out_ref.shape
    low_ref[...] = out_ref[rows - SHIFT : rows, :, :].astype(BF)
    east_ref[...] = out_ref[:, cols - SHIFT : cols, :].astype(BF)
    corner_ref[...] = out_ref[rows - SHIFT : rows, cols - SHIFT : cols, :].astype(BF)


def shifted_kernel(
    total_rows, stage, start_ref, scale_ref, z1_ref, right_ref, below_ref, corner_ref, wqkv_ref,
    wproj_ref, ans_ref, low_ref, east_ref, last_ref, qkv_ref,
    pad_ref, ones_ref, mask_ref, e_ref, o_ref,
):
    rows, cols, width = z1_ref.shape
    wr, wc = rows // WIN, cols // WIN
    tokens = WIN * WIN
    chunk = wc * tokens
    ones_ref[...] = head_ones(width, width // HEADS)
    mask_ref[...] = head_stack(tokens, width // HEADS)
    scale = scale_lanes(scale_ref, 1, width)
    stage.need(z1_ref, right_ref, below_ref, corner_ref)
    fill_ahead(pad_ref, z1_ref[...], right_ref, below_ref, corner_ref)
    threshold = total_rows - SHIFT - start_ref[0]

    def body(i, _):
        z = jnp.concatenate([rolled_window(pad_ref, i, w).astype(BF) for w in range(wc)], axis=0)
        stage.need_at(i == 0, wqkv_ref, wproj_ref)
        qkv = nn(z, wqkv_ref[...]).astype(BF)
        here = pl.ds(pl.multiple_of(i * chunk, chunk), chunk)
        qkv_ref[here, :] = qkv
        stage.emit_part(here, qkv_ref)
        allowed = side_mask(i, threshold, tokens)
        mixed = attention_chunk(qkv, scale, ones_ref, mask_ref, allowed, e_ref, o_ref, wc, tokens)
        answer = nn(mixed, wproj_ref[...]).astype(BF).astype(F32)
        for w in range(wc):
            ans_ref[pl.ds(i * WIN, WIN), w * WIN : (w + 1) * WIN, :] = answer[
                w * tokens : (w + 1) * tokens
            ].reshape(WIN, WIN, width)
        stage.emit_part(pl.ds(i * WIN, WIN), ans_ref)
        return 0

    lax.fori_loop(0, wr, body, 0)
    emit_behind(ans_ref, low_ref, east_ref, last_ref)


def behind_shapes(rows, cols, width):
    sh = jax.ShapeDtypeStruct
    return (
        sh((rows, cols, width), F32),
        sh((SHIFT, cols, width), BF),
        sh((rows, SHIFT, width), BF),
        sh((SHIFT, SHIFT, width), BF),
    )


def shifted_forward(start, z1, right, below, corner, wqkv, wproj, scale, total_rows):
    rows, cols, width = z1.shape
    tokens = rows * cols
    chunk = cols * WIN
    outs = behind_shapes(rows, cols, width) + (jax.ShapeDtypeStruct((tokens, 3 * width), BF),)
    return staged(
        functools.partial(shifted_kernel, total_rows),
        "shifted_forward",
        (start, scale, z1, right, below, corner, wqkv, wproj),
        outs,
        [
            pltpu.VMEM((rows + SHIFT, cols + WIN, width), F32),
            pltpu.VMEM((width, width), BF),
            pltpu.VMEM((LANES * HEADS // width * WIN * WIN, LANES), BF),
            pltpu.VMEM((chunk, HEADS * WIN * WIN), BF),
            pltpu.VMEM((chunk, width), F32),
        ],
        1e9,
        smem=(0, 1),
        layer={6: 1, 7: 1},
    )


def fill_behind(pad_ref, own, above_ref, west_ref, corner_ref):
    rows, cols, _ = own.shape
    pad_ref[SHIFT : SHIFT + rows, SHIFT : SHIFT + cols, :] = own
    pad_ref[0:SHIFT, SHIFT : SHIFT + cols, :] = above_ref[...].astype(F32)
    pad_ref[SHIFT : SHIFT + rows, 0:SHIFT, :] = west_ref[...].astype(F32)
    pad_ref[0:SHIFT, 0:SHIFT, :] = corner_ref[...].astype(F32)


def group_jobs(cnt_smem, offset, size, group, body):
    devices = cnt_smem.shape[0]

    def each(d, _):
        valid = cnt_smem[d, 0] - offset
        for g in range(0, size, group):

            @pl.when(valid > g)
            def _():
                body(d, offset + g, pl.multiple_of(d * size + g, group))

        return 0

    lax.fori_loop(0, devices, each, 0)


def gather_part(table_ref, found_ref, idx_smem, cnt_smem, offset, size, group):
    def body(d, slot, row):
        for u in range(group):
            found_ref[pl.ds(row + u, 1), :] = table_ref[pl.ds(idx_smem[d, slot + u], 1), :]

    group_jobs(cnt_smem, offset, size, group, body)


def scatter_part(table_ref, found_ref, idx_smem, cnt_smem, dup_smem, offset, size, group):
    def body(d, slot, row):
        @pl.when(dup_smem[d, slot] == 0)
        def _():
            spots = [idx_smem[d, slot + u] for u in range(group)]
            sums = [
                table_ref[pl.ds(spots[u], 1), :] + found_ref[pl.ds(row + u, 1), :]
                for u in range(group)
            ]
            for u in range(group):
                table_ref[pl.ds(spots[u], 1), :] = sums[u]

        @pl.when(dup_smem[d, slot] != 0)
        def _():
            def one(u, _):
                spot = pl.ds(idx_smem[d, slot + u], 1)
                table_ref[spot, :] = table_ref[spot, :] + found_ref[pl.ds(row + u, 1), :]
                return 0

            lax.fori_loop(0, group, one, 0)

    group_jobs(cnt_smem, offset, size, group, body)


def radiance_part(found_ref, obs_ref, mixed_ref, w1_ref, size):
    devices, _, channels = obs_ref.shape
    batch = min(devices, max(1, 512 // size))

    def body(i, _):
        here = pl.ds(pl.multiple_of(i * batch * size, batch * size), batch * size)
        y = obs_ref[pl.ds(i * batch, batch), 0:size, :].astype(F32)
        y = y.reshape(batch * size, channels)
        t = jnp.tanh(nn(found_ref[here, :].astype(BF), w1_ref[...].astype(BF)))
        pulled = (nn(t.astype(BF), mixed_ref[...]) - y) * (1.0 - t * t)
        found_ref[here, :] = nt(pulled.astype(BF), w1_ref[...].astype(BF))
        return 0

    lax.fori_loop(0, devices // batch, body, 0)


def spread(table_ref, moved_ref, i, step, tokens):
    for s in range(PIX):
        there = pl.ds(pl.multiple_of(s * tokens + i * step, WIN), step)
        moved_ref[:, s * VARS : (s + 1) * VARS] = table_ref[there, 0:VARS]


def forecast_kernel(
    parts, group, stage, obs1_ref, h1_ref, ans_ref, above_ref, west_ref, corner_ref, gain_ref,
    wup_ref, wdown_ref, whead_ref, state_ref, w1_in_ref, mixed_ref, obs2_ref, back_ref, inv_ref,
    h2_ref, gp_ref, prior_ref, found3_ref, idx_ref, cnt_ref, dup_ref, pulled_ref, w1_ref,
    pad_ref, table_ref, moved_ref, found1_ref, found2_ref, idx_smem, cnt_smem, dup_smem, sems,
):
    rows, cols, width = h1_ref.shape
    devices = obs1_ref.shape[0]
    tokens = rows * cols
    step = tokens // 2

    stage.need(obs1_ref)
    codes = obs1_ref[:, parts[0] : parts[0] + EXTRA, :].astype(F32)[:, 0, :]
    high = codes[:, :LANES].astype(jnp.int32)
    low = codes[:, LANES : 2 * LANES].astype(jnp.int32)
    point = jnp.where(high > 0, (high - 1) * LANES + low, 0)
    lane = lax.broadcasted_iota(jnp.int32, (devices, LANES), 1)
    idx = jnp.where(
        high > 0, (point % PIX) * tokens + point // PIX, PIX * tokens + lane % group
    )
    idx_ref[...] = idx
    cnt_ref[...] = jnp.broadcast_to(
        jnp.sum(jnp.where(high > 0, 1.0, 0.0), 1, keepdims=True), (devices, LANES)
    ).astype(jnp.int32)
    same = jnp.zeros((devices, LANES), jnp.int32)
    for s in range(1, group):
        hit = (pltpu.roll(idx, s, 1) == idx) & (lane % group >= s)
        same = jnp.maximum(same, jnp.where(hit, 1, 0))
    s = group // 2
    while s:
        same = jnp.maximum(same, pltpu.roll(same, LANES - s, 1))
        s //= 2
    dup_ref[...] = same
    copies = [
        pltpu.make_async_copy(a, b, sems.at[n])
        for n, (a, b) in enumerate(
            ((idx_ref, idx_smem), (cnt_ref, cnt_smem), (dup_ref, dup_smem))
        )
    ]
    for copy in copies:
        copy.start()
    stage.need(h1_ref, ans_ref, above_ref, west_ref, corner_ref)
    fill_behind(pad_ref, ans_ref[...], above_ref, west_ref, corner_ref)
    h2_ref[...] = (h1_ref[...] + pad_ref[0:rows, 0:cols, :]).reshape(tokens, width)
    table_ref[PIX * tokens :, :] = jnp.zeros((group, LANES), F32)
    blank = jnp.zeros((step, LANES - VARS), F32)
    stage.need(gain_ref, wup_ref, wdown_ref)

    def forward(i, _):
        here = pl.ds(pl.multiple_of(i * step, step), step)
        h2 = h2_ref[here, :]
        inner, slope = gelu_parts(nn(norm(h2, gain_ref[1, 1:2]), wup_ref[...]))
        gp_ref[here, :] = slope.astype(BF)
        h3 = (h2 + nn(inner.astype(BF), wdown_ref[...])).astype(BF)
        stage.need_at(i == 0, whead_ref, state_ref)
        moved = state_ref[here, :] + nt(h3, whead_ref[...])
        for s in range(PIX):
            there = pl.ds(pl.multiple_of(s * tokens + i * step, WIN), step)
            table_ref[there, :] = jnp.concatenate(
                [moved[:, s * VARS : (s + 1) * VARS], blank], axis=1
            )
        return 0

    lax.fori_loop(0, 2, forward, 0)
    stage.emit(h2_ref, gp_ref, idx_ref, cnt_ref, dup_ref)
    stage.need(back_ref, inv_ref, w1_in_ref, mixed_ref, obs2_ref)
    w1_ref[...] = jnp.zeros_like(w1_ref)
    w1_ref[0:VARS, :] = w1_in_ref[...]
    w1_ref[...] = w1_ref[...].astype(BF).astype(F32)
    for copy in copies:
        copy.wait()
    offsets = (0, parts[0], parts[0] + parts[1])
    founds = (found1_ref, found2_ref, found3_ref)
    for offset, size, found in zip(offsets, parts, founds):
        gather_part(table_ref, found, idx_smem, cnt_smem, offset, size, group)
    stage.emit(found3_ref)
    table_ref[...] = jnp.zeros_like(table_ref)
    radiance_part(found1_ref, obs1_ref, mixed_ref, w1_ref, parts[0])
    scatter_part(table_ref, found1_ref, idx_smem, cnt_smem, dup_smem, 0, parts[0], group)
    radiance_part(found2_ref, obs2_ref, mixed_ref, w1_ref, parts[1])
    scatter_part(table_ref, found2_ref, idx_smem, cnt_smem, dup_smem, parts[0], parts[1], group)

    def collect(i, _):
        here = pl.ds(pl.multiple_of(i * step, step), step)
        spread(table_ref, moved_ref, i, step, tokens)
        moved = moved_ref[...]
        prior_ref[here, :] = moved + inv_ref[...] * (state_ref[here, :] - back_ref[here, :])
        stage.emit_part(here, prior_ref)
        pulled_ref[here, :] = nn(moved.astype(BF), whead_ref[...])
        stage.emit_part(here, pulled_ref)
        return 0

    lax.fori_loop(0, 2, collect, 0)


def forecast(
    h1, ans, above, west, corner, state, background, inv, obs1, obs2, mixed, gains, wup, wdown,
    whead, w1, parts, group,
):
    rows, cols, width = h1.shape
    tokens = rows * cols
    devices = obs1.shape[0]
    sh = jax.ShapeDtypeStruct
    outs = (
        sh((tokens, width), F32),
        sh((tokens, wup.shape[2]), BF),
        sh(state.shape, F32),
        sh((devices * parts[2], LANES), F32),
        sh((devices, LANES), jnp.int32),
        sh((devices, LANES), jnp.int32),
        sh((devices, LANES), jnp.int32),
        sh((tokens, width), F32),
        sh((LANES, w1.shape[1]), F32),
    )
    return staged(
        functools.partial(forecast_kernel, parts, group),
        "forecast",
        (
            obs1, h1, ans, above, west, corner, gains, wup, wdown, whead, state, w1, mixed, obs2,
            background, inv,
        ),
        outs,
        [
            pltpu.VMEM((rows + SHIFT, cols + WIN, width), F32),
            pltpu.VMEM((PIX * tokens + group, LANES), F32),
            pltpu.VMEM((tokens // 2, state.shape[1]), F32),
            pltpu.VMEM((devices * parts[0], LANES), F32),
            pltpu.VMEM((devices * parts[1], LANES), F32),
        ]
        + [pltpu.SMEM((devices, LANES), jnp.int32)] * 3
        + [pltpu.SemaphoreType.DMA((3,))],
        3e9,
        layer={7: 1, 8: 1},
    )


def adjoint_kernel(
    parts, group, stage, idx_smem, cnt_smem, dup_smem, w1_ref, mixed_ref, work_ref, obs3_ref,
    whead_ref, pulled_ref, prior_ref, wdown_ref, gp_ref, wup_ref, h2_ref, gain_ref,
    top_ref, left_ref, edge_ref, third_ref, out_ref, table_ref, moved_ref,
):
    rows, cols, width = third_ref.shape
    tokens = rows * cols
    step = tokens // 2
    table_ref[...] = jnp.zeros_like(table_ref)
    stage.need(w1_ref, mixed_ref, work_ref, obs3_ref)
    radiance_part(work_ref, obs3_ref, mixed_ref, w1_ref, parts[2])
    scatter_part(
        table_ref, work_ref, idx_smem, cnt_smem, dup_smem, parts[0] + parts[1], parts[2], group
    )
    stage.need(whead_ref, pulled_ref, prior_ref, wdown_ref, gp_ref, wup_ref, h2_ref, gain_ref)
    half = rows // 2

    def backward(i, _):
        here = pl.ds(pl.multiple_of(i * step, step), step)
        spread(table_ref, moved_ref, i, step, tokens)
        moved = moved_ref[...]
        out_ref[here, :] = moved + prior_ref[here, :]
        stage.emit_part(here, out_ref)
        grad = (pulled_ref[here, :] + nn(moved.astype(BF), whead_ref[...])).astype(BF)
        d_inner = nt(grad, wdown_ref[...]) * gp_ref[here, :].astype(F32)
        d_normed = nt(d_inner.astype(BF), wup_ref[...])
        third = grad.astype(F32) + norm_back(h2_ref[here, :], gain_ref[1, 1:2], d_normed)
        third_ref[pl.ds(i * half, half), :, :] = third.reshape(half, cols, width)
        stage.emit_part(pl.ds(i * half, half), third_ref)
        return 0

    lax.fori_loop(0, 2, backward, 0)
    top_ref[...] = third_ref[0:SHIFT, :, :].astype(BF)
    left_ref[...] = third_ref[:, 0:SHIFT, :].astype(BF)
    edge_ref[...] = third_ref[0:SHIFT, 0:SHIFT, :].astype(BF)


def adjoint(
    idx, cnt, dup, found, obs3, mixed, w1, h2, gp, gains, wup, wdown, whead, prior, pulled, parts,
    group, rows, cols,
):
    width = h2.shape[1]
    third, top, left, edge = behind_shapes(rows, cols, width)
    outs = (top, left, edge, third, jax.ShapeDtypeStruct(prior.shape, F32))
    return staged(
        functools.partial(adjoint_kernel, parts, group),
        "adjoint",
        (idx, cnt, dup, w1, mixed, found, obs3, whead, pulled, prior, wdown, gp, wup, h2, gains),
        outs,
        [
            pltpu.VMEM((PIX * rows * cols + group, LANES), F32),
            pltpu.VMEM((prior.shape[0] // 2, prior.shape[1]), F32),
        ],
        2e9,
        smem=(0, 1, 2),
        layer={10: 1, 12: 1},
    )


def shifted_back_kernel(
    total_rows, stage, start_ref, scale_ref, third_ref, right_ref, below_ref, corner_ref,
    wproj_ref, qkv_ref, wqkv_ref, dz_ref, low_ref, east_ref, last_ref,
    pad_ref, ones_ref, mask_ref, dq_ref, dk_ref, dv_ref,
):
    rows, cols, width = third_ref.shape
    wr, wc = rows // WIN, cols // WIN
    tokens = WIN * WIN
    chunk = wc * tokens
    ones_ref[...] = head_ones(width, width // HEADS)
    mask_ref[...] = head_stack(tokens, width // HEADS)
    scale = scale_lanes(scale_ref, 1, width)
    stage.need(third_ref, right_ref, below_ref, corner_ref)
    fill_ahead(pad_ref, third_ref[...], right_ref, below_ref, corner_ref)
    threshold = total_rows - SHIFT - start_ref[0]

    def body(i, _):
        d_answer = jnp.concatenate(
            [rolled_window(pad_ref, i, w).astype(BF) for w in range(wc)], axis=0
        )
        stage.need_at(i == 0, wproj_ref, qkv_ref, wqkv_ref)
        d_out = nt(d_answer, wproj_ref[...]).astype(BF)
        allowed = side_mask(i, threshold, tokens)
        qkv = qkv_ref[pl.ds(pl.multiple_of(i * chunk, chunk), chunk), :]
        d_qkv = attention_chunk_back(
            qkv, d_out, scale, ones_ref, mask_ref, allowed,
            dq_ref, dk_ref, dv_ref, wc, tokens,
        )
        dz = nt(d_qkv, wqkv_ref[...]).astype(BF).astype(F32)
        for w in range(wc):
            dz_ref[pl.ds(i * WIN, WIN), w * WIN : (w + 1) * WIN, :] = dz[
                w * tokens : (w + 1) * tokens
            ].reshape(WIN, WIN, width)
        stage.emit_part(pl.ds(i * WIN, WIN), dz_ref)
        return 0

    lax.fori_loop(0, wr, body, 0)
    emit_behind(dz_ref, low_ref, east_ref, last_ref)


def shifted_backward(start, third, right, below, corner, qkv, wqkv, wproj, scale, total_rows):
    rows, cols, width = third.shape
    chunk = cols * WIN
    outs = behind_shapes(rows, cols, width)
    return staged(
        functools.partial(shifted_back_kernel, total_rows),
        "shifted_backward",
        (start, scale, third, right, below, corner, wproj, qkv, wqkv),
        outs,
        [
            pltpu.VMEM((rows + SHIFT, cols + WIN, width), F32),
            pltpu.VMEM((width, width), BF),
            pltpu.VMEM((LANES * HEADS // width * WIN * WIN, LANES), BF),
        ]
        + [pltpu.VMEM((chunk, width), F32)] * 3,
        1e9,
        smem=(0, 1),
        layer={6: 1, 8: 1},
    )


def last_kernel(
    stage, scale_ref, partial_hbm, dz_ref, above_ref, west_ref, corner_ref, third_ref, h1_ref,
    gain_ref, wdown_ref, gp_ref, wup_ref, hm_ref, wproj_ref, qkv_ref, wqkv_ref, h0_ref, we_ref,
    out_hbm,
    pad_ref, ones_ref, mask_ref, dq_ref, dk_ref, dv_ref, out_ref, in_sems, out_sems,
):
    rows, cols, width = dz_ref.shape
    wr, wc = rows // WIN, cols // WIN
    tokens = WIN * WIN
    chunk = wc * tokens

    def rows_of(ref, i):
        return ref.at[pl.ds(i * WIN, WIN)]

    ones_ref[...] = head_ones(width, width // HEADS)
    mask_ref[...] = head_stack(tokens, width // HEADS)
    scale = scale_lanes(scale_ref, 0, width)
    for i in range(wr):
        pltpu.make_async_copy(rows_of(partial_hbm, i), rows_of(out_ref, i), in_sems.at[i]).start()
    stage.need(dz_ref, above_ref, west_ref, corner_ref)
    fill_behind(pad_ref, dz_ref[...], above_ref, west_ref, corner_ref)

    def body(i, _):
        here = pl.ds(pl.multiple_of(i * chunk, chunk), chunk)
        band = pl.ds(i * WIN, WIN)

        def take(ref):
            return jnp.concatenate(
                [
                    ref[band, w * WIN : (w + 1) * WIN, :].reshape(tokens, width)
                    for w in range(wc)
                ],
                axis=0,
            )

        stage.need_at(i == 0, third_ref, h1_ref, gain_ref, wdown_ref, gp_ref, wup_ref)
        second = take(third_ref) + norm_back(take(h1_ref), gain_ref[1, 0:1], take(pad_ref))
        d_inner = nt(second.astype(BF), wdown_ref[...]) * gp_ref[here, :].astype(F32)
        d_normed = nt(d_inner.astype(BF), wup_ref[...])
        stage.need_at(i == 0, hm_ref, wproj_ref, qkv_ref, wqkv_ref, h0_ref, we_ref)
        d_hm = second + norm_back(hm_ref[here, :], gain_ref[0, 1:2], d_normed)
        d_out = nt(d_hm.astype(BF), wproj_ref[...]).astype(BF)
        d_qkv = attention_chunk_back(
            qkv_ref[here, :], d_out, scale, ones_ref, mask_ref, None,
            dq_ref, dk_ref, dv_ref, wc, tokens,
        )
        dz = nt(d_qkv, wqkv_ref[...])
        d_h0 = (d_hm + norm_back(h0_ref[here, :], gain_ref[0, 0:1], dz)).astype(BF)
        pltpu.make_async_copy(rows_of(partial_hbm, i), rows_of(out_ref, i), in_sems.at[i]).wait()
        for w in range(wc):
            grad = nt(d_h0[w * tokens : (w + 1) * tokens], we_ref[...])
            grad = grad.reshape(WIN, WIN, grad.shape[1])
            spot = (band, slice(w * WIN, (w + 1) * WIN), slice(None))
            out_ref[spot] = grad + out_ref[spot]
        pltpu.make_async_copy(rows_of(out_ref, i), rows_of(out_hbm, i), out_sems.at[i]).start()
        return 0

    lax.fori_loop(0, wr, body, 0)
    for i in range(wr):
        pltpu.make_async_copy(rows_of(out_ref, i), rows_of(out_hbm, i), out_sems.at[i]).wait()


def last_block(
    third, dz, above, west, corner, h1, h0, hm, qkv, gp, we, gains, wqkv, wproj, scale,
    wup, wdown, partial,
):
    rows, cols, width = dz.shape
    chunk = cols * WIN
    (result,) = staged(
        last_kernel,
        "last_block",
        (
            scale, partial, dz, above, west, corner, third, h1, gains, wdown, gp, wup, hm, wproj,
            qkv, wqkv, h0, we,
        ),
        (jax.ShapeDtypeStruct(partial.shape, F32),),
        [
            pltpu.VMEM((rows + SHIFT, cols + WIN, width), F32),
            pltpu.VMEM((width, width), BF),
            pltpu.VMEM((LANES * HEADS // width * WIN * WIN, LANES), BF),
        ]
        + [pltpu.VMEM((chunk, width), F32)] * 3
        + [
            pltpu.VMEM(partial.shape, F32),
            pltpu.SemaphoreType.DMA((rows // WIN,)),
            pltpu.SemaphoreType.DMA((rows // WIN,)),
        ],
        2e9,
        smem=(0,),
        raw=(1,),
        raw_outs=(0,),
        layer={9: 0, 11: 0, 13: 0, 15: 0},
    )
    return result


def neighbour(x, by_lat, by_lon):
    lat, lon = lax.axis_size("lat"), lax.axis_size("lon")
    pairs = [
        (a * lon + b, ((a + by_lat) % lat) * lon + (b + by_lon) % lon)
        for a in range(lat)
        for b in range(lon)
    ]
    return lax.ppermute(x, ("lat", "lon"), pairs)


def exchange(x):
    return lax.all_to_all(x, ("lat", "lon"), split_axis=0, concat_axis=0, tiled=True)


def local(
    state,
    background,
    inv_background,
    w_embed,
    norm_gain,
    w_qkv,
    w_proj,
    head_scale,
    w_up,
    w_down,
    w_head,
    w_obs1,
    w_obs2,
    r_inverse,
    obs_values,
    obs_owner,
    obs_point,
    obs_count,
):
    rows, cols, patch_values = state.shape
    width = w_embed.shape[1]
    total_rows = rows * lax.axis_size("lat")
    row_start = (lax.axis_index("lat") * rows).astype(jnp.int32).reshape(1)
    devices = lax.axis_size("lat") * lax.axis_size("lon")
    slots = obs_values.shape[0]
    cap = 2 * slots // devices

    parts, group = split(cap)

    send1, send2, send3, mixed = route(
        obs_owner.reshape(1, slots), obs_point.reshape(1, slots), obs_count, obs_values,
        r_inverse, w_obs2, devices, parts,
    )
    obs1 = exchange(send1)
    state5 = state.reshape(rows // WIN, WIN, cols // WIN, WIN, patch_values)
    top, left, corner, z1, h1, h0, hm, qkv0, gp0 = first_block(
        mixed, state5, w_embed, norm_gain, w_qkv, w_proj, head_scale, w_up, w_down
    )
    z1 = z1.reshape(rows, cols, width)
    h1 = h1.reshape(rows, cols, width)
    below = neighbour(top.reshape(SHIFT, cols, width), -1, 0)
    right = neighbour(left.reshape(rows, SHIFT, width), 0, -1)
    corner = neighbour(corner, -1, -1)
    below, right, corner, obs1, send2 = lax.optimization_barrier(
        (below, right, corner, obs1, send2)
    )
    obs2 = exchange(send2)
    answer, low, east, last, qkv1 = shifted_forward(
        row_start, z1, right, below, corner, w_qkv, w_proj, head_scale, total_rows
    )
    above = neighbour(low, 1, 0)
    west = neighbour(east, 0, 1)
    last = neighbour(last, 1, 1)
    above, west, last, obs2, send3 = lax.optimization_barrier((above, west, last, obs2, send3))
    obs3 = exchange(send3)
    flat = (rows * cols, patch_values)
    h2, gp1, prior, found, idx, cnt, dup, pulled, w1 = forecast(
        h1, answer, above, west, last, state.reshape(flat), background.reshape(flat),
        inv_background.reshape(1, -1), obs1, obs2, mixed, norm_gain, w_up, w_down, w_head.T,
        w_obs1, parts, group,
    )
    top, left, corner, third, partial = adjoint(
        idx, cnt, dup, found, obs3, mixed, w1, h2, gp1, norm_gain, w_up, w_down, w_head.T, prior,
        pulled,
        parts, group, rows, cols,
    )
    below = neighbour(top, -1, 0)
    right = neighbour(left, 0, -1)
    corner = neighbour(corner, -1, -1)
    dz, low, east, last = shifted_backward(
        row_start, third, right, below, corner, qkv1, w_qkv, w_proj, head_scale, total_rows
    )
    above = neighbour(low, 1, 0)
    west = neighbour(east, 0, 1)
    last = neighbour(last, 1, 1)
    return last_block(
        third, dz, above, west, last, h1, h0, hm, qkv0, gp0, w_embed, norm_gain, w_qkv, w_proj,
        head_scale, w_up, w_down, partial.reshape(state.shape),
    )


def solution(mesh):
    placed = (
        P("lat", "lon", None),
        P("lat", "lon", None),
        P(),
        P(),
        P(),
        P(),
        P(),
        P(),
        P(),
        P(),
        P(),
        P(),
        P(),
        P(),
        P(("lat", "lon"), None),
        P(("lat", "lon"), None),
        P(("lat", "lon")),
        P(("lat", "lon")),
    )
    return jax.shard_map(
        local, mesh=mesh, in_specs=placed, out_specs=P("lat", "lon", None), check_vma=False
    )
```

```python
import functools

import jax
import jax.numpy as jnp
from jax import lax
from jax.experimental import pallas as pl
from jax.experimental.pallas import tpu as pltpu
from jax.sharding import PartitionSpec as P

HEADS = 8
VARS = 69
PIX = 16
WIN = 8
SHIFT = 4
LANES = 128
EXTRA = 8
EPS = 1e-05
BF = jnp.bfloat16
F32 = jnp.float32
SQRT_2_OVER_PI = 0.7978845608028654
CUBIC = 0.044715

SMEM = pl.BlockSpec(memory_space=pltpu.SMEM)
VMEM = pl.BlockSpec(memory_space=pltpu.VMEM)
HBM = pl.BlockSpec(memory_space=pltpu.HBM)
MIB = 1024 * 1024
ROOM = 44


class Stage:
    def __init__(self):
        self.inputs = {}
        self.outputs = {}
        self.waited = set()
        self.sent = set()

    def need(self, *refs):
        for ref in refs:
            if id(ref) not in self.waited:
                self.waited.add(id(ref))
                self.inputs[id(ref)].wait()

    def need_at(self, first, *refs):
        pending = [ref for ref in refs if id(ref) not in self.waited]
        self.waited.update(id(ref) for ref in pending)

        @pl.when(first)
        def _():
            for ref in pending:
                self.inputs[id(ref)].wait()

    def emit_part(self, part, *refs):
        for ref in refs:
            self.sent.add(id(ref))
            self.outputs[id(ref)].part(part).start()

    def emit(self, *refs):
        for ref in refs:
            if id(ref) not in self.sent:
                self.sent.add(id(ref))
                self.outputs[id(ref)].start()

    def close(self):
        for key, copy in self.inputs.items():
            if key not in self.waited:
                copy.wait()
        for key, copy in self.outputs.items():
            if key not in self.sent:
                copy.start()
        for copy in self.outputs.values():
            copy.wait()


class Outgoing:
    def __init__(self, source, target, sem):
        self.refs = (source, target, sem)

    def part(self, part):
        source, target, sem = self.refs
        return pltpu.make_async_copy(source.at[part], target.at[part], sem)

    def start(self):
        pltpu.make_async_copy(*self.refs).start()

    def wait(self):
        pltpu.make_async_copy(*self.refs).wait()


def staged(
    body, name, args, outs, scratch, flops, smem=(), raw=(), raw_outs=(), layer=None, vmem=(),
    early=lambda ins, extra: None,
    scalars=(),
):
    layer = layer or {}
    count = len(args)
    placed = [
        x if i in smem or i in vmem else pltpu.with_memory_space_constraint(x, pltpu.HBM)
        for i, x in enumerate(args)
    ]
    in_buffers = []
    for i, x in enumerate(args):
        if i not in smem and i not in raw and i not in vmem:
            shape = x.shape[1:] if i in layer else x.shape
            space = pltpu.SMEM if i in scalars else pltpu.VMEM
            in_buffers.append((i, space(shape, x.dtype)))
    out_buffers = [
        (j, pltpu.VMEM(o.shape, o.dtype)) for j, o in enumerate(outs) if j not in raw_outs
    ]

    def kernel(*refs):
        ins = [
            ref.at[layer[i]] if i in vmem and i in layer else ref
            for i, ref in enumerate(refs[:count])
        ]
        results = list(refs[count : count + len(outs)])
        rest = list(refs[count + len(outs) :])
        ins_vmem = rest[: len(in_buffers)]
        outs_vmem = rest[len(in_buffers) : len(in_buffers) + len(out_buffers)]
        in_sems, out_sems = rest[-2:]
        extra = rest[len(in_buffers) + len(out_buffers) : -2]
        stage = Stage()
        early(ins, extra)
        stage.waited.update(id(ins[i]) for i in vmem)
        for n, ((i, _), buffer) in enumerate(zip(in_buffers, ins_vmem)):
            source = ins[i].at[layer[i]] if i in layer else ins[i]
            copy = pltpu.make_async_copy(source, buffer, in_sems.at[n])
            copy.start()
            stage.inputs[id(buffer)] = copy
            ins[i] = buffer
        for n, ((j, _), buffer) in enumerate(zip(out_buffers, outs_vmem)):
            stage.outputs[id(buffer)] = Outgoing(buffer, results[j], out_sems.at[n])
            results[j] = buffer
        body(stage, *ins, *results, *extra)
        stage.close()

    return pl.pallas_call(
        kernel,
        out_shape=tuple(pltpu.HBM(o.shape, o.dtype) for o in outs),
        in_specs=[
            SMEM if i in smem else VMEM if i in vmem else HBM for i in range(count)
        ],
        out_specs=(HBM,) * len(outs),
        scratch_shapes=[b for _, b in in_buffers]
        + [b for _, b in out_buffers]
        + list(scratch)
        + [
            pltpu.SemaphoreType.DMA((max(1, len(in_buffers)),)),
            pltpu.SemaphoreType.DMA((max(1, len(out_buffers)),)),
        ],
        compiler_params=pltpu.CompilerParams(vmem_limit_bytes=ROOM * MIB),
        cost_estimate=pl.CostEstimate(
            flops=int(flops), bytes_accessed=8 * MIB, transcendentals=0
        ),
        name=name,
    )(*placed)


def scale_lanes(scale_ref, block, width):
    head = lax.broadcasted_iota(jnp.int32, (1, width), 1) // (width // HEADS)
    row = jnp.zeros((1, width), F32)
    for h in range(HEADS):
        row = jnp.where(head == h, scale_ref[block, h], row)
    return row


def nn(a, b):
    return lax.dot_general(a, b, (((1,), (0,)), ((), ())), preferred_element_type=F32)


def nt(a, b):
    return lax.dot_general(a, b, (((1,), (1,)), ((), ())), preferred_element_type=F32)


def tn(a, b):
    return lax.dot_general(a, b, (((0,), (0,)), ((), ())), preferred_element_type=F32)


def norm_parts(h):
    mean = jnp.mean(h, -1, keepdims=True)
    centred = h - mean
    spread = jnp.mean(centred * centred, -1, keepdims=True)
    rstd = lax.rsqrt(spread + EPS)
    return centred * rstd, rstd


def norm(h, gain):
    return (norm_parts(h)[0] * gain).astype(BF)


def norm_back(h, gain, cotangent):
    xhat, rstd = norm_parts(h)
    scaled = cotangent * gain
    m1 = jnp.mean(scaled, -1, keepdims=True)
    m2 = jnp.mean(scaled * xhat, -1, keepdims=True)
    return rstd * (scaled - m1 - xhat * m2)


def gelu_parts(u):
    square = u * u
    t = jnp.tanh(u * (SQRT_2_OVER_PI + SQRT_2_OVER_PI * CUBIC * square))
    half = 0.5 + 0.5 * t
    value = u * half
    rate = 2.0 * SQRT_2_OVER_PI + 6.0 * SQRT_2_OVER_PI * CUBIC * square
    return value, half + value * (1.0 - half) * rate


def head_ones(width, size):
    a = lax.broadcasted_iota(jnp.int32, (width, width), 0) // size
    b = lax.broadcasted_iota(jnp.int32, (width, width), 1) // size
    return (a == b).astype(F32).astype(BF)


def head_stack(tokens, size):
    heads = LANES // size
    a = lax.broadcasted_iota(jnp.int32, (heads * tokens, LANES), 0) // tokens
    b = lax.broadcasted_iota(jnp.int32, (heads * tokens, LANES), 1) // size
    return (a == b).astype(F32).astype(BF)


def stacked(x, mask):
    copies = mask.shape[0] // x.shape[0]
    return [
        jnp.concatenate([x[:, t : t + LANES]] * copies, axis=0) * mask
        for t in range(0, x.shape[1], LANES)
    ]


def scores_of(x, blocks):
    return jnp.concatenate(
        [nt(x[:, t * LANES : (t + 1) * LANES], b) for t, b in enumerate(blocks)], axis=1
    )


def mix_of(p, blocks):
    rows = blocks[0].shape[0]
    return jnp.concatenate(
        [nn(p[:, t * rows : (t + 1) * rows], b) for t, b in enumerate(blocks)], axis=1
    )


def side_mask(window_row, threshold, tokens):
    shape = (tokens, HEADS * tokens)
    a = lax.broadcasted_iota(jnp.int32, shape, 0) // WIN
    b = (lax.broadcasted_iota(jnp.int32, shape, 1) % tokens) // WIN
    first = (window_row * WIN + a) >= threshold
    second = (window_row * WIN + b) >= threshold
    return jnp.where(first == second, 1.0, 0.0).astype(F32)


def window(ref, i, w):
    block = ref[i, :, w, :, :]
    return block.reshape(block.shape[0] * block.shape[1], block.shape[2])


def attention_chunk(qkv, scale, ones_ref, mask_ref, allowed, e_ref, o_ref, count, tokens):
    width = qkv.shape[1] // 3
    q = qkv[:, :width].astype(F32)
    k = qkv[:, width : 2 * width].astype(F32)
    v = qkv[:, 2 * width :]
    ones = ones_ref[...]
    qs = (q * lax.rsqrt(nn((q * q).astype(BF), ones) + 1.0) * scale).astype(BF)
    kn = (k * lax.rsqrt(nn((k * k).astype(BF), ones) + 1.0)).astype(BF)
    mask = mask_ref[...]
    for w in range(count):
        part = slice(w * tokens, (w + 1) * tokens)
        expo = jnp.exp(scores_of(qs[part], stacked(kn[part], mask)))
        if allowed is not None:
            expo = expo * allowed
        expo = expo.astype(BF)
        e_ref[part] = expo
        o_ref[part] = mix_of(expo, stacked(v[part], mask))
    total = mix_of(e_ref[...], [mask] * (width // LANES))
    return (o_ref[...] / total).astype(BF)


def attention_chunk_back(
    qkv, d_out, scale, ones_ref, mask_ref, allowed, dq_ref, dk_ref, dv_ref, count, tokens
):
    width = qkv.shape[1] // 3
    size = width // HEADS
    q = qkv[:, :width].astype(F32)
    k = qkv[:, width : 2 * width].astype(F32)
    v = qkv[:, 2 * width :]
    ones = ones_ref[...]
    rq = lax.rsqrt(nn((q * q).astype(BF), ones) + 1.0)
    rk = lax.rsqrt(nn((k * k).astype(BF), ones) + 1.0)
    qs = (q * rq * scale).astype(BF)
    kn = (k * rk).astype(BF)
    mask = mask_ref[...]
    lane_head = lax.broadcasted_iota(jnp.int32, (1, LANES), 1) // size
    per_tile = LANES // size
    for w in range(count):
        part = slice(w * tokens, (w + 1) * tokens)
        kw = kn[part]
        qm = stacked(qs[part], mask)
        dm = stacked(d_out[part], mask)
        expo = jnp.exp(scores_of(kw, qm))
        if allowed is not None:
            expo = expo * allowed
        p = expo * (1.0 / jnp.sum(expo, 0, keepdims=True))
        dp = scores_of(v[part], dm)
        ds = (p * (dp - jnp.sum(p * dp, 0, keepdims=True))).astype(BF)
        dv_ref[part] = mix_of(p.astype(BF), dm)
        dk_ref[part] = mix_of(ds, qm)
        tiles = []
        for tile in range(width // LANES):
            span = per_tile * tokens
            full = tn(
                ds[:, tile * span : (tile + 1) * span], kw[:, tile * LANES : (tile + 1) * LANES]
            )
            total = None
            for s in range(per_tile):
                block = full[s * tokens : (s + 1) * tokens]
                block = jnp.where(lane_head == s, block, 0.0)
                total = block if total is None else total + block
            tiles.append(total)
        dq_ref[part] = jnp.concatenate(tiles, axis=1)
    dqs = dq_ref[...]
    dkn = dk_ref[...]
    dq = scale * rq * (dqs - q * (rq * rq) * nn((q * dqs).astype(BF), ones))
    dk = rk * (dkn - k * (rk * rk) * nn((k * dkn).astype(BF), ones))
    return jnp.concatenate([dq.astype(BF), dk.astype(BF), dv_ref[...].astype(BF)], axis=1)


def split(cap):
    first = max(8, cap // 4)
    return (first, first, cap - 2 * first), min(16, first)


def route_kernel(
    parts, stage, count_ref, owner_ref, point_ref, r_ref, w2_ref, values_ref,
    send1_ref, send2_ref, send3_ref, mixed_ref, y_ref, buf_ref, tgt_ref, tgt_smem, sem,
):
    cap = sum(parts)
    slots = owner_ref.shape[1]
    devices = send1_ref.shape[0]
    stage.need(owner_ref, point_ref)
    owner = owner_ref[...]
    live = lax.broadcasted_iota(jnp.int32, (1, slots), 1) < count_ref[0]
    match = lax.broadcasted_iota(jnp.int32, (devices, slots), 0) == owner
    match = jnp.where(match, 1.0, 0.0).astype(F32)
    a = lax.broadcasted_iota(jnp.int32, (LANES, LANES), 0)
    b = lax.broadcasted_iota(jnp.int32, (LANES, LANES), 1)
    upper = jnp.where(a < b, 1.0, 0.0).astype(BF)
    chunks = slots // LANES
    flat = jnp.concatenate(
        [match[:, c * LANES : (c + 1) * LANES] for c in range(chunks)], axis=0
    )
    before = nn(flat.astype(BF), upper)
    carry = jnp.zeros((devices, 1), F32)
    ranks = []
    dump = devices * cap
    for c in range(chunks):
        here = match[:, c * LANES : (c + 1) * LANES]
        seen = before[c * devices : (c + 1) * devices] + carry
        ranks.append(jnp.sum(here * seen, 0, keepdims=True))
        span = slice(c * LANES, (c + 1) * LANES)
        spot = owner[:, span] * cap + ranks[-1].astype(jnp.int32)
        tgt_ref[c : c + 1, :] = jnp.where(live[:, span], spot, dump)
        carry = carry + jnp.sum(here, 1, keepdims=True)
    rank = jnp.concatenate(ranks, axis=1).astype(jnp.int32)
    copy = pltpu.make_async_copy(tgt_ref, tgt_smem, sem)
    copy.start()
    place = lax.broadcasted_iota(jnp.int32, (cap, slots), 0) == rank
    place = jnp.where(place & live, 1.0, 0.0).astype(BF)
    point = point_ref[...]
    high = (match * (point // LANES + 1).astype(F32)).astype(BF)
    low = (match * (point % LANES).astype(F32)).astype(BF)
    high = nt(high, place)
    low = nt(low, place)
    stage.need(r_ref, w2_ref, values_ref)
    best = lax.Precision.HIGHEST
    dims = (((1,), (1,)), ((), ()))
    m2 = lax.dot_general(
        r_ref[...], w2_ref[...], dims, precision=best, preferred_element_type=F32
    )
    mixed_ref[...] = jnp.dot(
        w2_ref[...], m2, precision=best, preferred_element_type=F32
    ).astype(BF)
    y = nn(values_ref[...].astype(BF), m2.astype(BF))
    y_ref[0, :, :] = y[:, :LANES]
    y_ref[1, :, :] = y[:, LANES:]
    buf_ref[...] = jnp.zeros_like(buf_ref)
    copy.wait()
    unroll = 16

    def move(c, _):
        base = pl.multiple_of(c * LANES, LANES)
        for start in range(0, LANES, unroll):
            spots = [tgt_smem[c, start + u] for u in range(unroll)]
            for half in range(2):
                for u in range(unroll):
                    buf_ref[half, pl.ds(spots[u], 1), :] = y_ref[
                        half, pl.ds(base + start + u, 1), :
                    ]
        return 0

    lax.fori_loop(0, chunks, move, 0)
    for d in range(devices):
        offset = d * cap
        for ref, size in zip((send1_ref, send2_ref, send3_ref), parts):
            for half in range(2):
                ref[d, 0:size, half * LANES : (half + 1) * LANES] = buf_ref[
                    half, offset : offset + size, :
                ].astype(BF)
            offset += size
    fill = ((0, 0), (0, LANES - cap))
    codes = jnp.concatenate([jnp.pad(high, fill), jnp.pad(low, fill)], axis=1)
    for d in range(devices):
        send1_ref[d, parts[0] : parts[0] + EXTRA, :] = jnp.broadcast_to(
            codes[d : d + 1], (EXTRA, 2 * LANES)
        ).astype(BF)


def route(owner, point, count, values, r_inverse, w2, devices, parts):
    slots, channels = values.shape
    cap = sum(parts)
    sizes = (parts[0] + EXTRA,) + tuple(parts[1:])
    return staged(
        functools.partial(route_kernel, parts),
        "route",
        (count, owner, point, r_inverse, w2, values),
        tuple(jax.ShapeDtypeStruct((devices, n, channels), BF) for n in sizes)
        + (jax.ShapeDtypeStruct(w2.shape, BF),),
        [
            pltpu.VMEM((2, slots, LANES), F32),
            pltpu.VMEM((2, devices * cap + EXTRA, LANES), F32),
            pltpu.VMEM((slots // LANES, LANES), jnp.int32),
            pltpu.SMEM((slots // LANES, LANES), jnp.int32),
            pltpu.SemaphoreType.DMA,
        ],
        1e9,
        smem=(0,),
    )


def load_state(ins, extra):
    source, target, sems = ins[2], extra[0], extra[-1]
    for i in range(source.shape[0]):
        pltpu.make_async_copy(source.at[i], target.at[i], sems.at[i]).start()


def first_kernel(
    stage, scale_ref, order_ref, state_hbm, we_ref, gain_ref, wqkv_ref, wproj_ref, wup_ref, wdown_ref,
    top_ref, left_ref, corner_ref, z1_ref, h1_ref, h0_ref, hm_ref, qkv_ref, gp_ref,
    state_ref, ones_ref, mask_ref, e_ref, o_ref, sems,
):
    rows, _, cols, _, _ = state_ref.shape
    width = we_ref.shape[1]
    tokens = WIN * WIN
    chunk = cols * tokens

    def load(i):
        return pltpu.make_async_copy(state_hbm.at[i], state_ref.at[i], sems.at[i])

    ones_ref[...] = head_ones(width, width // HEADS)
    mask_ref[...] = head_stack(tokens, width // HEADS)
    scale = scale_lanes(scale_ref, 0, width)
    stage.need(we_ref, gain_ref)

    def body(i, _):
        load(i).wait()
        x = jnp.concatenate([window(state_ref, i, w).astype(BF) for w in range(cols)], axis=0)
        h0 = nn(x, we_ref[...])
        here = pl.ds(pl.multiple_of(i * chunk, chunk), chunk)
        h0_ref[here, :] = h0
        stage.emit_part(here, h0_ref)
        stage.need_at(i == 0, wqkv_ref)
        qkv = nn(norm(h0, gain_ref[0, 0:1]), wqkv_ref[...]).astype(BF)
        qkv_ref[here, :] = qkv
        stage.emit_part(here, qkv_ref)
        mixed = attention_chunk(qkv, scale, ones_ref, mask_ref, None, e_ref, o_ref, cols, tokens)
        stage.need_at(i == 0, wproj_ref, wup_ref, wdown_ref)
        hm = h0 + nn(mixed, wproj_ref[...]).astype(BF).astype(F32)
        hm_ref[here, :] = hm
        stage.emit_part(here, hm_ref)
        inner, slope = gelu_parts(nn(norm(hm, gain_ref[0, 1:2]), wup_ref[...]))
        gp_ref[here, :] = slope.astype(BF)
        stage.emit_part(here, gp_ref)
        h1 = hm + nn(inner.astype(BF), wdown_ref[...])
        z1 = norm(h1, gain_ref[1, 0:1]).astype(F32)
        for w in range(cols):
            part = slice(w * tokens, (w + 1) * tokens)
            h1_ref[i, :, w, :, :] = h1[part].reshape(WIN, WIN, width)
            z1_ref[i, :, w, :, :] = z1[part].reshape(WIN, WIN, width)
        stage.emit_part(i, z1_ref, h1_ref)
        return 0

    lax.fori_loop(0, rows, body, 0)
    top_ref[...] = z1_ref[0, 0:SHIFT, :, :, :].astype(BF)
    left_ref[...] = z1_ref[:, :, 0, 0:SHIFT, :].astype(BF)
    corner_ref[...] = z1_ref[0, 0:SHIFT, 0, 0:SHIFT, :].astype(BF)


def first_block(order, state5, we, gains, wqkv, wproj, scale, wup, wdown):
    wr, _, wc, _, _ = state5.shape
    width = we.shape[1]
    tokens = wr * wc * WIN * WIN
    chunk = wc * WIN * WIN
    sh = jax.ShapeDtypeStruct
    outs = (
        sh((SHIFT, wc, WIN, width), BF),
        sh((wr, WIN, SHIFT, width), BF),
        sh((SHIFT, SHIFT, width), BF),
        sh((wr, WIN, wc, WIN, width), F32),
        sh((wr, WIN, wc, WIN, width), F32),
        sh((tokens, width), F32),
        sh((tokens, width), F32),
        sh((tokens, 3 * width), BF),
        sh((tokens, wup.shape[2]), BF),
    )
    return staged(
        first_kernel,
        "first_block",
        (scale, order, state5, we, gains, wqkv, wproj, wup, wdown),
        outs,
        [
            pltpu.VMEM(state5.shape, F32),
            pltpu.VMEM((width, width), BF),
            pltpu.VMEM((LANES * HEADS // width * WIN * WIN, LANES), BF),
            pltpu.VMEM((chunk, HEADS * WIN * WIN), BF),
            pltpu.VMEM((chunk, width), F32),
            pltpu.SemaphoreType.DMA((wr,)),
        ],
        2e9,
        smem=(0,),
        raw=(1, 2),
        early=load_state,
        layer={5: 0, 6: 0, 7: 0, 8: 0},
    )


def fill_ahead(pad_ref, own, right_ref, below_ref, corner_ref):
    rows, cols, _ = own.shape
    pad_ref[0:rows, 0:cols, :] = own
    pad_ref[0:rows, cols : cols + SHIFT, :] = right_ref[...].astype(F32)
    pad_ref[rows : rows + SHIFT, 0:cols, :] = below_ref[...].astype(F32)
    pad_ref[rows : rows + SHIFT, cols : cols + SHIFT, :] = corner_ref[...].astype(F32)


def rolled_window(pad_ref, i, w):
    block = pad_ref[
        pl.ds(i * WIN + SHIFT, WIN), SHIFT + w * WIN : SHIFT + (w + 1) * WIN, :
    ]
    return block.reshape(WIN * WIN, block.shape[2])


def emit_behind(out_ref, low_ref, east_ref, corner_ref):
    rows, cols, _ = out_ref.shape
    low_ref[...] = out_ref[rows - SHIFT : rows, :, :].astype(BF)
    east_ref[...] = out_ref[:, cols - SHIFT : cols, :].astype(BF)
    corner_ref[...] = out_ref[rows - SHIFT : rows, cols - SHIFT : cols, :].astype(BF)


def shifted_kernel(
    total_rows, stage, start_ref, scale_ref, z1_ref, right_ref, below_ref, corner_ref, wqkv_ref,
    wproj_ref, ans_ref, low_ref, east_ref, last_ref, qkv_ref,
    pad_ref, ones_ref, mask_ref, e_ref, o_ref,
):
    rows, cols, width = z1_ref.shape
    wr, wc = rows // WIN, cols // WIN
    tokens = WIN * WIN
    chunk = wc * tokens
    ones_ref[...] = head_ones(width, width // HEADS)
    mask_ref[...] = head_stack(tokens, width // HEADS)
    scale = scale_lanes(scale_ref, 1, width)
    stage.need(z1_ref, right_ref, below_ref, corner_ref)
    fill_ahead(pad_ref, z1_ref[...], right_ref, below_ref, corner_ref)
    threshold = total_rows - SHIFT - start_ref[0]

    def body(i, _):
        z = jnp.concatenate([rolled_window(pad_ref, i, w).astype(BF) for w in range(wc)], axis=0)
        stage.need_at(i == 0, wqkv_ref, wproj_ref)
        qkv = nn(z, wqkv_ref[...]).astype(BF)
        here = pl.ds(pl.multiple_of(i * chunk, chunk), chunk)
        qkv_ref[here, :] = qkv
        stage.emit_part(here, qkv_ref)
        allowed = side_mask(i, threshold, tokens)
        mixed = attention_chunk(qkv, scale, ones_ref, mask_ref, allowed, e_ref, o_ref, wc, tokens)
        answer = nn(mixed, wproj_ref[...]).astype(BF).astype(F32)
        for w in range(wc):
            ans_ref[pl.ds(i * WIN, WIN), w * WIN : (w + 1) * WIN, :] = answer[
                w * tokens : (w + 1) * tokens
            ].reshape(WIN, WIN, width)
        stage.emit_part(pl.ds(i * WIN, WIN), ans_ref)
        return 0

    lax.fori_loop(0, wr, body, 0)
    emit_behind(ans_ref, low_ref, east_ref, last_ref)


def behind_shapes(rows, cols, width):
    sh = jax.ShapeDtypeStruct
    return (
        sh((rows, cols, width), F32),
        sh((SHIFT, cols, width), BF),
        sh((rows, SHIFT, width), BF),
        sh((SHIFT, SHIFT, width), BF),
    )


def shifted_forward(start, z1, right, below, corner, wqkv, wproj, scale, total_rows):
    rows, cols, width = z1.shape
    tokens = rows * cols
    chunk = cols * WIN
    outs = behind_shapes(rows, cols, width) + (jax.ShapeDtypeStruct((tokens, 3 * width), BF),)
    return staged(
        functools.partial(shifted_kernel, total_rows),
        "shifted_forward",
        (start, scale, z1, right, below, corner, wqkv, wproj),
        outs,
        [
            pltpu.VMEM((rows + SHIFT, cols + WIN, width), F32),
            pltpu.VMEM((width, width), BF),
            pltpu.VMEM((LANES * HEADS // width * WIN * WIN, LANES), BF),
            pltpu.VMEM((chunk, HEADS * WIN * WIN), BF),
            pltpu.VMEM((chunk, width), F32),
        ],
        1e9,
        smem=(0, 1),
        vmem=(3, 4, 5),
        layer={6: 1, 7: 1},
    )


def fill_behind(pad_ref, own, above_ref, west_ref, corner_ref):
    rows, cols, _ = own.shape
    pad_ref[SHIFT : SHIFT + rows, SHIFT : SHIFT + cols, :] = own
    pad_ref[0:SHIFT, SHIFT : SHIFT + cols, :] = above_ref[...].astype(F32)
    pad_ref[SHIFT : SHIFT + rows, 0:SHIFT, :] = west_ref[...].astype(F32)
    pad_ref[0:SHIFT, 0:SHIFT, :] = corner_ref[...].astype(F32)


def group_jobs(cnt_smem, offset, size, group, body):
    devices = cnt_smem.shape[0]

    def each(d, _):
        valid = cnt_smem[d, 0] - offset
        for g in range(0, size, group):

            @pl.when(valid > g)
            def _():
                body(d, offset + g, pl.multiple_of(d * size + g, group))

        return 0

    lax.fori_loop(0, devices, each, 0)


def gather_part(table_ref, found_ref, idx_smem, cnt_smem, offset, size, group):
    def body(d, slot, row):
        for u in range(group):
            found_ref[pl.ds(row + u, 1), :] = table_ref[pl.ds(idx_smem[d, slot + u], 1), :]

    group_jobs(cnt_smem, offset, size, group, body)


def scatter_part(table_ref, found_ref, idx_smem, cnt_smem, dup_smem, offset, size, group):
    def body(d, slot, row):
        @pl.when(dup_smem[d, slot] == 0)
        def _():
            spots = [idx_smem[d, slot + u] for u in range(group)]
            sums = [
                table_ref[pl.ds(spots[u], 1), :] + found_ref[pl.ds(row + u, 1), :]
                for u in range(group)
            ]
            for u in range(group):
                table_ref[pl.ds(spots[u], 1), :] = sums[u]

        @pl.when(dup_smem[d, slot] != 0)
        def _():
            def one(u, _):
                spot = pl.ds(idx_smem[d, slot + u], 1)
                table_ref[spot, :] = table_ref[spot, :] + found_ref[pl.ds(row + u, 1), :]
                return 0

            lax.fori_loop(0, group, one, 0)

    group_jobs(cnt_smem, offset, size, group, body)


def radiance_part(found_ref, obs_ref, mixed_ref, w1_ref, size):
    devices, _, channels = obs_ref.shape
    batch = min(devices, max(1, 512 // size))

    def body(i, _):
        here = pl.ds(pl.multiple_of(i * batch * size, batch * size), batch * size)
        y = obs_ref[pl.ds(i * batch, batch), 0:size, :].astype(F32)
        y = y.reshape(batch * size, channels)
        t = jnp.tanh(nn(found_ref[here, :].astype(BF), w1_ref[...].astype(BF)))
        pulled = (nn(t.astype(BF), mixed_ref[...]) - y) * (1.0 - t * t)
        found_ref[here, :] = nt(pulled.astype(BF), w1_ref[...].astype(BF))
        return 0

    lax.fori_loop(0, devices // batch, body, 0)


def spread(table_ref, moved_ref, i, step, tokens):
    for s in range(PIX):
        there = pl.ds(pl.multiple_of(s * tokens + i * step, WIN), step)
        moved_ref[:, s * VARS : (s + 1) * VARS] = table_ref[there, 0:VARS]


def forecast_kernel(
    parts, group, stage, obs1_ref, h1_ref, ans_ref, above_ref, west_ref, corner_ref, gain_ref,
    wup_ref, wdown_ref, whead_ref, state_ref, w1_in_ref, mixed_ref, obs2_ref, back_ref, inv_ref,
    h2_ref, gp_ref, prior_ref, found3_ref, idx_ref, cnt_ref, dup_ref, pulled_ref, w1_ref,
    pad_ref, table_ref, moved_ref, found1_ref, found2_ref, idx_smem, cnt_smem, dup_smem, sems,
):
    rows, cols, width = h1_ref.shape
    devices = obs1_ref.shape[0]
    tokens = rows * cols
    step = tokens // 2

    stage.need(obs1_ref)
    codes = obs1_ref[:, parts[0] : parts[0] + EXTRA, :].astype(F32)[:, 0, :]
    high = codes[:, :LANES].astype(jnp.int32)
    low = codes[:, LANES : 2 * LANES].astype(jnp.int32)
    point = jnp.where(high > 0, (high - 1) * LANES + low, 0)
    lane = lax.broadcasted_iota(jnp.int32, (devices, LANES), 1)
    idx = jnp.where(
        high > 0, (point % PIX) * tokens + point // PIX, PIX * tokens + lane % group
    )
    idx_ref[...] = idx
    cnt_ref[...] = jnp.broadcast_to(
        jnp.sum(jnp.where(high > 0, 1.0, 0.0), 1, keepdims=True), (devices, LANES)
    ).astype(jnp.int32)
    same = jnp.zeros((devices, LANES), jnp.int32)
    for s in range(1, group):
        hit = (pltpu.roll(idx, s, 1) == idx) & (lane % group >= s)
        same = jnp.maximum(same, jnp.where(hit, 1, 0))
    s = group // 2
    while s:
        same = jnp.maximum(same, pltpu.roll(same, LANES - s, 1))
        s //= 2
    dup_ref[...] = same
    copies = [
        pltpu.make_async_copy(a, b, sems.at[n])
        for n, (a, b) in enumerate(
            ((idx_ref, idx_smem), (cnt_ref, cnt_smem), (dup_ref, dup_smem))
        )
    ]
    for copy in copies:
        copy.start()
    stage.need(h1_ref, ans_ref, above_ref, west_ref, corner_ref)
    fill_behind(pad_ref, ans_ref[...], above_ref, west_ref, corner_ref)
    h2_ref[...] = (h1_ref[...] + pad_ref[0:rows, 0:cols, :]).reshape(tokens, width)
    table_ref[PIX * tokens :, :] = jnp.zeros((group, LANES), F32)
    blank = jnp.zeros((step, LANES - VARS), F32)
    stage.need(gain_ref, wup_ref, wdown_ref)

    def forward(i, _):
        here = pl.ds(pl.multiple_of(i * step, step), step)
        h2 = h2_ref[here, :]
        inner, slope = gelu_parts(nn(norm(h2, gain_ref[1, 1:2]), wup_ref[...]))
        gp_ref[here, :] = slope.astype(BF)
        h3 = (h2 + nn(inner.astype(BF), wdown_ref[...])).astype(BF)
        stage.need_at(i == 0, whead_ref, state_ref)
        moved = state_ref[here, :] + nt(h3, whead_ref[...])
        for s in range(PIX):
            there = pl.ds(pl.multiple_of(s * tokens + i * step, WIN), step)
            table_ref[there, :] = jnp.concatenate(
                [moved[:, s * VARS : (s + 1) * VARS], blank], axis=1
            )
        return 0

    lax.fori_loop(0, 2, forward, 0)
    stage.emit(h2_ref, gp_ref, idx_ref, cnt_ref, dup_ref)
    stage.need(back_ref, inv_ref, w1_in_ref, mixed_ref, obs2_ref)
    w1_ref[...] = jnp.zeros_like(w1_ref)
    w1_ref[0:VARS, :] = w1_in_ref[...]
    w1_ref[...] = w1_ref[...].astype(BF).astype(F32)
    for copy in copies:
        copy.wait()
    offsets = (0, parts[0], parts[0] + parts[1])
    founds = (found1_ref, found2_ref, found3_ref)
    for offset, size, found in zip(offsets, parts, founds):
        gather_part(table_ref, found, idx_smem, cnt_smem, offset, size, group)
    stage.emit(found3_ref)
    table_ref[...] = jnp.zeros_like(table_ref)
    radiance_part(found1_ref, obs1_ref, mixed_ref, w1_ref, parts[0])
    scatter_part(table_ref, found1_ref, idx_smem, cnt_smem, dup_smem, 0, parts[0], group)
    radiance_part(found2_ref, obs2_ref, mixed_ref, w1_ref, parts[1])
    scatter_part(table_ref, found2_ref, idx_smem, cnt_smem, dup_smem, parts[0], parts[1], group)

    def collect(i, _):
        here = pl.ds(pl.multiple_of(i * step, step), step)
        spread(table_ref, moved_ref, i, step, tokens)
        moved = moved_ref[...]
        prior_ref[here, :] = moved + inv_ref[...].reshape(1, -1) * (state_ref[here, :] - back_ref[here, :])
        stage.emit_part(here, prior_ref)
        pulled_ref[here, :] = nn(moved.astype(BF), whead_ref[...])
        stage.emit_part(here, pulled_ref)
        return 0

    lax.fori_loop(0, 2, collect, 0)


def forecast(
    h1, ans, above, west, corner, state, background, inv, obs1, obs2, mixed, gains, wup, wdown,
    whead, w1, parts, group,
):
    rows, cols, width = h1.shape
    tokens = rows * cols
    devices = obs1.shape[0]
    sh = jax.ShapeDtypeStruct
    outs = (
        sh((tokens, width), F32),
        sh((tokens, wup.shape[2]), BF),
        sh(state.shape, F32),
        sh((devices * parts[2], LANES), F32),
        sh((devices, LANES), jnp.int32),
        sh((devices, LANES), jnp.int32),
        sh((devices, LANES), jnp.int32),
        sh((tokens, width), F32),
        sh((LANES, w1.shape[1]), F32),
    )
    return staged(
        functools.partial(forecast_kernel, parts, group),
        "forecast",
        (
            obs1, h1, ans, above, west, corner, gains, wup, wdown, whead, state, w1, mixed, obs2,
            background, inv,
        ),
        outs,
        [
            pltpu.VMEM((rows + SHIFT, cols + WIN, width), F32),
            pltpu.VMEM((PIX * tokens + group, LANES), F32),
            pltpu.VMEM((tokens // 2, state.shape[1]), F32),
            pltpu.VMEM((devices * parts[0], LANES), F32),
            pltpu.VMEM((devices * parts[1], LANES), F32),
        ]
        + [pltpu.SMEM((devices, LANES), jnp.int32)] * 3
        + [pltpu.SemaphoreType.DMA((3,))],
        3e9,
        vmem=(0, 3, 4, 5, 13),
        layer={7: 1, 8: 1},
    )


def adjoint_kernel(
    parts, group, stage, idx_smem, cnt_smem, dup_smem, w1_ref, mixed_ref, work_ref, obs3_ref,
    whead_ref, pulled_ref, prior_ref, wdown_ref, gp_ref, wup_ref, h2_ref, gain_ref,
    top_ref, left_ref, edge_ref, third_ref, out_ref, table_ref, moved_ref,
):
    rows, cols, width = third_ref.shape
    tokens = rows * cols
    step = tokens // 2
    table_ref[...] = jnp.zeros_like(table_ref)
    stage.need(idx_smem, cnt_smem, dup_smem, w1_ref, mixed_ref, work_ref, obs3_ref)
    radiance_part(work_ref, obs3_ref, mixed_ref, w1_ref, parts[2])
    scatter_part(
        table_ref, work_ref, idx_smem, cnt_smem, dup_smem, parts[0] + parts[1], parts[2], group
    )
    stage.need(whead_ref, pulled_ref, prior_ref, wdown_ref, gp_ref, wup_ref, h2_ref, gain_ref)
    half = rows // 2

    def backward(i, _):
        here = pl.ds(pl.multiple_of(i * step, step), step)
        spread(table_ref, moved_ref, i, step, tokens)
        moved = moved_ref[...]
        out_ref[here, :] = moved + prior_ref[here, :]
        stage.emit_part(here, out_ref)
        grad = (pulled_ref[here, :] + nn(moved.astype(BF), whead_ref[...])).astype(BF)
        d_inner = nt(grad, wdown_ref[...]) * gp_ref[here, :].astype(F32)
        d_normed = nt(d_inner.astype(BF), wup_ref[...])
        third = grad.astype(F32) + norm_back(h2_ref[here, :], gain_ref[1, 1:2], d_normed)
        third_ref[pl.ds(i * half, half), :, :] = third.reshape(half, cols, width)
        stage.emit_part(pl.ds(i * half, half), third_ref)
        return 0

    lax.fori_loop(0, 2, backward, 0)
    top_ref[...] = third_ref[0:SHIFT, :, :].astype(BF)
    left_ref[...] = third_ref[:, 0:SHIFT, :].astype(BF)
    edge_ref[...] = third_ref[0:SHIFT, 0:SHIFT, :].astype(BF)


def adjoint(
    idx, cnt, dup, found, obs3, mixed, w1, h2, gp, gains, wup, wdown, whead, prior, pulled, parts,
    group, rows, cols,
):
    width = h2.shape[1]
    third, top, left, edge = behind_shapes(rows, cols, width)
    outs = (top, left, edge, third, jax.ShapeDtypeStruct(prior.shape, F32))
    return staged(
        functools.partial(adjoint_kernel, parts, group),
        "adjoint",
        (idx, cnt, dup, w1, mixed, found, obs3, whead, pulled, prior, wdown, gp, wup, h2, gains),
        outs,
        [
            pltpu.VMEM((PIX * rows * cols + group, LANES), F32),
            pltpu.VMEM((prior.shape[0] // 2, prior.shape[1]), F32),
        ],
        2e9,
        scalars=(0, 1, 2),
        vmem=(6,),
        layer={10: 1, 12: 1},
    )


def shifted_back_kernel(
    total_rows, stage, start_ref, scale_ref, third_ref, right_ref, below_ref, corner_ref,
    wproj_ref, qkv_ref, wqkv_ref, dz_ref, low_ref, east_ref, last_ref,
    pad_ref, ones_ref, mask_ref, dq_ref, dk_ref, dv_ref,
):
    rows, cols, width = third_ref.shape
    wr, wc = rows // WIN, cols // WIN
    tokens = WIN * WIN
    chunk = wc * tokens
    ones_ref[...] = head_ones(width, width // HEADS)
    mask_ref[...] = head_stack(tokens, width // HEADS)
    scale = scale_lanes(scale_ref, 1, width)
    stage.need(third_ref, right_ref, below_ref, corner_ref)
    fill_ahead(pad_ref, third_ref[...], right_ref, below_ref, corner_ref)
    threshold = total_rows - SHIFT - start_ref[0]

    def body(i, _):
        d_answer = jnp.concatenate(
            [rolled_window(pad_ref, i, w).astype(BF) for w in range(wc)], axis=0
        )
        stage.need_at(i == 0, wproj_ref, qkv_ref, wqkv_ref)
        d_out = nt(d_answer, wproj_ref[...]).astype(BF)
        allowed = side_mask(i, threshold, tokens)
        qkv = qkv_ref[pl.ds(pl.multiple_of(i * chunk, chunk), chunk), :]
        d_qkv = attention_chunk_back(
            qkv, d_out, scale, ones_ref, mask_ref, allowed,
            dq_ref, dk_ref, dv_ref, wc, tokens,
        )
        dz = nt(d_qkv, wqkv_ref[...]).astype(BF).astype(F32)
        for w in range(wc):
            dz_ref[pl.ds(i * WIN, WIN), w * WIN : (w + 1) * WIN, :] = dz[
                w * tokens : (w + 1) * tokens
            ].reshape(WIN, WIN, width)
        stage.emit_part(pl.ds(i * WIN, WIN), dz_ref)
        return 0

    lax.fori_loop(0, wr, body, 0)
    emit_behind(dz_ref, low_ref, east_ref, last_ref)


def shifted_backward(start, third, right, below, corner, qkv, wqkv, wproj, scale, total_rows):
    rows, cols, width = third.shape
    chunk = cols * WIN
    outs = behind_shapes(rows, cols, width)
    return staged(
        functools.partial(shifted_back_kernel, total_rows),
        "shifted_backward",
        (start, scale, third, right, below, corner, wproj, qkv, wqkv),
        outs,
        [
            pltpu.VMEM((rows + SHIFT, cols + WIN, width), F32),
            pltpu.VMEM((width, width), BF),
            pltpu.VMEM((LANES * HEADS // width * WIN * WIN, LANES), BF),
        ]
        + [pltpu.VMEM((chunk, width), F32)] * 3,
        1e9,
        smem=(0, 1),
        vmem=(3, 4, 5, 6, 7, 8),
        layer={6: 1, 8: 1},
    )


def last_kernel(
    stage, scale_ref, partial_hbm, dz_ref, above_ref, west_ref, corner_ref, third_ref, h1_ref,
    gain_ref, wdown_ref, gp_ref, wup_ref, hm_ref, wproj_ref, qkv_ref, wqkv_ref, h0_ref, we_ref,
    out_hbm,
    pad_ref, ones_ref, mask_ref, dq_ref, dk_ref, dv_ref, out_ref, in_sems, out_sems,
):
    rows, cols, width = dz_ref.shape
    wr, wc = rows // WIN, cols // WIN
    tokens = WIN * WIN
    chunk = wc * tokens

    def rows_of(ref, i):
        return ref.at[pl.ds(i * WIN, WIN)]

    ones_ref[...] = head_ones(width, width // HEADS)
    mask_ref[...] = head_stack(tokens, width // HEADS)
    scale = scale_lanes(scale_ref, 0, width)
    for i in range(wr):
        pltpu.make_async_copy(rows_of(partial_hbm, i), rows_of(out_ref, i), in_sems.at[i]).start()
    stage.need(dz_ref, above_ref, west_ref, corner_ref)
    fill_behind(pad_ref, dz_ref[...], above_ref, west_ref, corner_ref)

    def body(i, _):
        here = pl.ds(pl.multiple_of(i * chunk, chunk), chunk)
        band = pl.ds(i * WIN, WIN)

        def take(ref):
            return jnp.concatenate(
                [
                    ref[band, w * WIN : (w + 1) * WIN, :].reshape(tokens, width)
                    for w in range(wc)
                ],
                axis=0,
            )

        stage.need_at(i == 0, third_ref, h1_ref, gain_ref, wdown_ref, gp_ref, wup_ref)
        second = take(third_ref) + norm_back(take(h1_ref), gain_ref[1, 0:1], take(pad_ref))
        d_inner = nt(second.astype(BF), wdown_ref[...]) * gp_ref[here, :].astype(F32)
        d_normed = nt(d_inner.astype(BF), wup_ref[...])
        stage.need_at(i == 0, hm_ref, wproj_ref, qkv_ref, wqkv_ref, h0_ref, we_ref)
        d_hm = second + norm_back(hm_ref[here, :], gain_ref[0, 1:2], d_normed)
        d_out = nt(d_hm.astype(BF), wproj_ref[...]).astype(BF)
        d_qkv = attention_chunk_back(
            qkv_ref[here, :], d_out, scale, ones_ref, mask_ref, None,
            dq_ref, dk_ref, dv_ref, wc, tokens,
        )
        dz = nt(d_qkv, wqkv_ref[...])
        d_h0 = (d_hm + norm_back(h0_ref[here, :], gain_ref[0, 0:1], dz)).astype(BF)
        pltpu.make_async_copy(rows_of(partial_hbm, i), rows_of(out_ref, i), in_sems.at[i]).wait()
        for w in range(wc):
            grad = nt(d_h0[w * tokens : (w + 1) * tokens], we_ref[...])
            grad = grad.reshape(WIN, WIN, grad.shape[1])
            spot = (band, slice(w * WIN, (w + 1) * WIN), slice(None))
            out_ref[spot] = grad + out_ref[spot]
        pltpu.make_async_copy(rows_of(out_ref, i), rows_of(out_hbm, i), out_sems.at[i]).start()
        return 0

    lax.fori_loop(0, wr, body, 0)
    for i in range(wr):
        pltpu.make_async_copy(rows_of(out_ref, i), rows_of(out_hbm, i), out_sems.at[i]).wait()


def last_block(
    third, dz, above, west, corner, h1, h0, hm, qkv, gp, we, gains, wqkv, wproj, scale,
    wup, wdown, partial,
):
    rows, cols, width = dz.shape
    chunk = cols * WIN
    (result,) = staged(
        last_kernel,
        "last_block",
        (
            scale, partial, dz, above, west, corner, third, h1, gains, wdown, gp, wup, hm, wproj,
            qkv, wqkv, h0, we,
        ),
        (jax.ShapeDtypeStruct(partial.shape, F32),),
        [
            pltpu.VMEM((rows + SHIFT, cols + WIN, width), F32),
            pltpu.VMEM((width, width), BF),
            pltpu.VMEM((LANES * HEADS // width * WIN * WIN, LANES), BF),
        ]
        + [pltpu.VMEM((chunk, width), F32)] * 3
        + [
            pltpu.VMEM(partial.shape, F32),
            pltpu.SemaphoreType.DMA((rows // WIN,)),
            pltpu.SemaphoreType.DMA((rows // WIN,)),
        ],
        2e9,
        smem=(0,),
        raw=(1,),
        raw_outs=(0,),
        vmem=(3, 4, 5, 7, 8, 9, 10, 11, 12, 13, 14, 15, 16, 17),
        layer={9: 0, 11: 0, 13: 0, 15: 0},
    )
    return result


def neighbour(x, by_lat, by_lon):
    lat, lon = lax.axis_size("lat"), lax.axis_size("lon")
    pairs = [
        (a * lon + b, ((a + by_lat) % lat) * lon + (b + by_lon) % lon)
        for a in range(lat)
        for b in range(lon)
    ]
    return lax.ppermute(x, ("lat", "lon"), pairs)


def exchange(x):
    return lax.all_to_all(x, ("lat", "lon"), split_axis=0, concat_axis=0, tiled=True)


def local(
    state,
    background,
    inv_background,
    w_embed,
    norm_gain,
    w_qkv,
    w_proj,
    head_scale,
    w_up,
    w_down,
    w_head,
    w_obs1,
    w_obs2,
    r_inverse,
    obs_values,
    obs_owner,
    obs_point,
    obs_count,
):
    rows, cols, patch_values = state.shape
    width = w_embed.shape[1]
    total_rows = rows * lax.axis_size("lat")
    row_start = (lax.axis_index("lat") * rows).astype(jnp.int32).reshape(1)
    devices = lax.axis_size("lat") * lax.axis_size("lon")
    slots = obs_values.shape[0]
    cap = 2 * slots // devices

    parts, group = split(cap)

    send1, send2, send3, mixed = route(
        obs_owner.reshape(1, slots), obs_point.reshape(1, slots), obs_count, obs_values,
        r_inverse, w_obs2, devices, parts,
    )
    obs1 = exchange(send1)
    state5 = state.reshape(rows // WIN, WIN, cols // WIN, WIN, patch_values)
    top, left, corner, z1, h1, h0, hm, qkv0, gp0 = first_block(
        mixed, state5, w_embed, norm_gain, w_qkv, w_proj, head_scale, w_up, w_down
    )
    z1 = z1.reshape(rows, cols, width)
    h1 = h1.reshape(rows, cols, width)
    below = neighbour(top.reshape(SHIFT, cols, width), -1, 0)
    right = neighbour(left.reshape(rows, SHIFT, width), 0, -1)
    corner = neighbour(corner, -1, -1)
    below, right, corner, obs1, send2 = lax.optimization_barrier(
        (below, right, corner, obs1, send2)
    )
    obs2 = exchange(send2)
    answer, low, east, last, qkv1 = shifted_forward(
        row_start, z1, right, below, corner, w_qkv, w_proj, head_scale, total_rows
    )
    above = neighbour(low, 1, 0)
    west = neighbour(east, 0, 1)
    last = neighbour(last, 1, 1)
    above, west, last, obs2, send3 = lax.optimization_barrier((above, west, last, obs2, send3))
    obs3 = exchange(send3)
    flat = (rows * cols, patch_values)
    h2, gp1, prior, found, idx, cnt, dup, pulled, w1 = forecast(
        h1, answer, above, west, last, state.reshape(flat), background.reshape(flat),
        inv_background, obs1, obs2, mixed, norm_gain, w_up, w_down, w_head.T,
        w_obs1, parts, group,
    )
    top, left, corner, third, partial = adjoint(
        idx, cnt, dup, found, obs3, mixed, w1, h2, gp1, norm_gain, w_up, w_down, w_head.T, prior,
        pulled,
        parts, group, rows, cols,
    )
    below = neighbour(top, -1, 0)
    right = neighbour(left, 0, -1)
    corner = neighbour(corner, -1, -1)
    dz, low, east, last = shifted_backward(
        row_start, third, right, below, corner, qkv1, w_qkv, w_proj, head_scale, total_rows
    )
    above = neighbour(low, 1, 0)
    west = neighbour(east, 0, 1)
    last = neighbour(last, 1, 1)
    return last_block(
        third, dz, above, west, last, h1, h0, hm, qkv0, gp0, w_embed, norm_gain, w_qkv, w_proj,
        head_scale, w_up, w_down, partial.reshape(state.shape),
    )


def solution(mesh):
    placed = (
        P("lat", "lon", None),
        P("lat", "lon", None),
        P(),
        P(),
        P(),
        P(),
        P(),
        P(),
        P(),
        P(),
        P(),
        P(),
        P(),
        P(),
        P(("lat", "lon"), None),
        P(("lat", "lon"), None),
        P(("lat", "lon")),
        P(("lat", "lon")),
    )
    return jax.shard_map(
        local, mesh=mesh, in_specs=placed, out_specs=P("lat", "lon", None), check_vma=False
    )
```

```python
import functools

import jax
import jax.numpy as jnp
from jax import lax
from jax.experimental import pallas as pl
from jax.experimental.pallas import tpu as pltpu
from jax.sharding import PartitionSpec as P


HEADS = 8
VARS = 69
PIX = 16
WIN = 8
SHIFT = 4
LANES = 128
EXTRA = 8
EPS = 1e-05
BF = jnp.bfloat16
F32 = jnp.float32
SQRT_2_OVER_PI = 0.7978845608028654
CUBIC = 0.044715

SMEM = pl.BlockSpec(memory_space=pltpu.SMEM)
VMEM = pl.BlockSpec(memory_space=pltpu.VMEM)
HBM = pl.BlockSpec(memory_space=pltpu.HBM)
MIB = 1024 * 1024
ROOM = 44


class Stage:
    def __init__(self):
        self.inputs = {}
        self.outputs = {}
        self.waited = set()
        self.sent = set()

    def need(self, *refs):
        for ref in refs:
            if id(ref) not in self.waited:
                self.waited.add(id(ref))
                self.inputs[id(ref)].wait()

    def need_at(self, first, *refs):
        pending = [ref for ref in refs if id(ref) not in self.waited]
        self.waited.update(id(ref) for ref in pending)

        @pl.when(first)
        def _():
            for ref in pending:
                self.inputs[id(ref)].wait()

    def emit_part(self, part, *refs):
        for ref in refs:
            self.sent.add(id(ref))
            self.outputs[id(ref)].part(part).start()

    def emit(self, *refs):
        for ref in refs:
            if id(ref) not in self.sent:
                self.sent.add(id(ref))
                self.outputs[id(ref)].start()

    def close(self):
        for key, copy in self.inputs.items():
            if key not in self.waited:
                copy.wait()
        for key, copy in self.outputs.items():
            if key not in self.sent:
                copy.start()
        for copy in self.outputs.values():
            copy.wait()


class Outgoing:
    def __init__(self, source, target, sem):
        self.refs = (source, target, sem)

    def part(self, part):
        source, target, sem = self.refs
        return pltpu.make_async_copy(source.at[part], target.at[part], sem)

    def start(self):
        pltpu.make_async_copy(*self.refs).start()

    def wait(self):
        pltpu.make_async_copy(*self.refs).wait()


def staged(
    body, args, outs, scratch, flops, smem=(), raw=(), raw_outs=(), layer=None, vmem=(),
    early=lambda ins, extra: None,
    scalars=(),
):
    layer = layer or {}
    count = len(args)
    placed = [
        x if i in smem or i in vmem else pltpu.with_memory_space_constraint(x, pltpu.HBM)
        for i, x in enumerate(args)
    ]
    in_buffers = []
    for i, x in enumerate(args):
        if i not in smem and i not in raw and i not in vmem:
            shape = x.shape[1:] if i in layer else x.shape
            space = pltpu.SMEM if i in scalars else pltpu.VMEM
            in_buffers.append((i, space(shape, x.dtype)))
    out_buffers = [
        (j, pltpu.VMEM(o.shape, o.dtype)) for j, o in enumerate(outs) if j not in raw_outs
    ]

    def kernel(*refs):
        ins = [
            ref.at[layer[i]] if i in vmem and i in layer else ref
            for i, ref in enumerate(refs[:count])
        ]
        results = list(refs[count : count + len(outs)])
        rest = list(refs[count + len(outs) :])
        ins_vmem = rest[: len(in_buffers)]
        outs_vmem = rest[len(in_buffers) : len(in_buffers) + len(out_buffers)]
        in_sems, out_sems = rest[-2:]
        extra = rest[len(in_buffers) + len(out_buffers) : -2]
        stage = Stage()
        early(ins, extra)
        stage.waited.update(id(ins[i]) for i in vmem)
        for n, ((i, _), buffer) in enumerate(zip(in_buffers, ins_vmem)):
            source = ins[i].at[layer[i]] if i in layer else ins[i]
            copy = pltpu.make_async_copy(source, buffer, in_sems.at[n])
            copy.start()
            stage.inputs[id(buffer)] = copy
            ins[i] = buffer
        for n, ((j, _), buffer) in enumerate(zip(out_buffers, outs_vmem)):
            stage.outputs[id(buffer)] = Outgoing(buffer, results[j], out_sems.at[n])
            results[j] = buffer
        body(stage, *ins, *results, *extra)
        stage.close()

    return pl.pallas_call(
        kernel,
        out_shape=tuple(pltpu.HBM(o.shape, o.dtype) for o in outs),
        in_specs=[
            SMEM if i in smem else VMEM if i in vmem else HBM for i in range(count)
        ],
        out_specs=(HBM,) * len(outs),
        scratch_shapes=[b for _, b in in_buffers]
        + [b for _, b in out_buffers]
        + list(scratch)
        + [
            pltpu.SemaphoreType.DMA((max(1, len(in_buffers)),)),
            pltpu.SemaphoreType.DMA((max(1, len(out_buffers)),)),
        ],
        compiler_params=pltpu.CompilerParams(vmem_limit_bytes=ROOM * MIB),
        cost_estimate=pl.CostEstimate(
            flops=int(flops), bytes_accessed=8 * MIB, transcendentals=0
        ),
    )(*placed)


def scale_lanes(scale_ref, block, width):
    head = lax.broadcasted_iota(jnp.int32, (1, width), 1) // (width // HEADS)
    row = jnp.zeros((1, width), F32)
    for h in range(HEADS):
        row = jnp.where(head == h, scale_ref[block, h], row)
    return row


def nn(a, b):
    return lax.dot_general(a, b, (((1,), (0,)), ((), ())), preferred_element_type=F32)


def nt(a, b):
    return lax.dot_general(a, b, (((1,), (1,)), ((), ())), preferred_element_type=F32)


def tn(a, b):
    return lax.dot_general(a, b, (((0,), (0,)), ((), ())), preferred_element_type=F32)


def norm_parts(h):
    mean = jnp.mean(h, -1, keepdims=True)
    centred = h - mean
    spread = jnp.mean(centred * centred, -1, keepdims=True)
    rstd = lax.rsqrt(spread + EPS)
    return centred * rstd, rstd


def norm(h, gain):
    return (norm_parts(h)[0] * gain).astype(BF)


def norm_back(h, gain, cotangent):
    xhat, rstd = norm_parts(h)
    scaled = cotangent * gain
    m1 = jnp.mean(scaled, -1, keepdims=True)
    m2 = jnp.mean(scaled * xhat, -1, keepdims=True)
    return rstd * (scaled - m1 - xhat * m2)


def gelu_parts(u):
    square = u * u
    t = jnp.tanh(u * (SQRT_2_OVER_PI + SQRT_2_OVER_PI * CUBIC * square))
    half = 0.5 + 0.5 * t
    value = u * half
    rate = 2.0 * SQRT_2_OVER_PI + 6.0 * SQRT_2_OVER_PI * CUBIC * square
    return value, half + value * (1.0 - half) * rate


def head_ones(width, size):
    a = lax.broadcasted_iota(jnp.int32, (width, width), 0) // size
    b = lax.broadcasted_iota(jnp.int32, (width, width), 1) // size
    return (a == b).astype(F32).astype(BF)


def head_stack(tokens, size):
    heads = LANES // size
    a = lax.broadcasted_iota(jnp.int32, (heads * tokens, LANES), 0) // tokens
    b = lax.broadcasted_iota(jnp.int32, (heads * tokens, LANES), 1) // size
    return (a == b).astype(F32).astype(BF)


def stacked(x, mask):
    copies = mask.shape[0] // x.shape[0]
    return [
        jnp.concatenate([x[:, t : t + LANES]] * copies, axis=0) * mask
        for t in range(0, x.shape[1], LANES)
    ]


def scores_of(x, blocks):
    return jnp.concatenate(
        [nt(x[:, t * LANES : (t + 1) * LANES], b) for t, b in enumerate(blocks)], axis=1
    )


def mix_of(p, blocks):
    rows = blocks[0].shape[0]
    return jnp.concatenate(
        [nn(p[:, t * rows : (t + 1) * rows], b) for t, b in enumerate(blocks)], axis=1
    )


def side_mask(window_row, threshold, tokens):
    shape = (tokens, HEADS * tokens)
    a = lax.broadcasted_iota(jnp.int32, shape, 0) // WIN
    b = (lax.broadcasted_iota(jnp.int32, shape, 1) % tokens) // WIN
    first = (window_row * WIN + a) >= threshold
    second = (window_row * WIN + b) >= threshold
    return jnp.where(first == second, 1.0, 0.0).astype(F32)


def window(ref, i, w):
    block = ref[i, :, w, :, :]
    return block.reshape(block.shape[0] * block.shape[1], block.shape[2])


def attention_chunk(qkv, scale, ones_ref, mask_ref, allowed, e_ref, o_ref, count, tokens):
    width = qkv.shape[1] // 3
    q = qkv[:, :width].astype(F32)
    k = qkv[:, width : 2 * width].astype(F32)
    v = qkv[:, 2 * width :]
    ones = ones_ref[...]
    qs = (q * lax.rsqrt(nn((q * q).astype(BF), ones) + 1.0) * scale).astype(BF)
    kn = (k * lax.rsqrt(nn((k * k).astype(BF), ones) + 1.0)).astype(BF)
    mask = mask_ref[...]
    for w in range(count):
        part = slice(w * tokens, (w + 1) * tokens)
        expo = jnp.exp(scores_of(qs[part], stacked(kn[part], mask)))
        if allowed is not None:
            expo = expo * allowed
        expo = expo.astype(BF)
        e_ref[part] = expo
        o_ref[part] = mix_of(expo, stacked(v[part], mask))
    total = mix_of(e_ref[...], [mask] * (width // LANES))
    return (o_ref[...] / total).astype(BF)


def attention_chunk_back(
    qkv, d_out, scale, ones_ref, mask_ref, allowed, dq_ref, dk_ref, dv_ref, count, tokens
):
    width = qkv.shape[1] // 3
    size = width // HEADS
    q = qkv[:, :width].astype(F32)
    k = qkv[:, width : 2 * width].astype(F32)
    v = qkv[:, 2 * width :]
    ones = ones_ref[...]
    rq = lax.rsqrt(nn((q * q).astype(BF), ones) + 1.0)
    rk = lax.rsqrt(nn((k * k).astype(BF), ones) + 1.0)
    qs = (q * rq * scale).astype(BF)
    kn = (k * rk).astype(BF)
    mask = mask_ref[...]
    lane_head = lax.broadcasted_iota(jnp.int32, (1, LANES), 1) // size
    per_tile = LANES // size
    for w in range(count):
        part = slice(w * tokens, (w + 1) * tokens)
        kw = kn[part]
        qm = stacked(qs[part], mask)
        dm = stacked(d_out[part], mask)
        expo = jnp.exp(scores_of(kw, qm))
        if allowed is not None:
            expo = expo * allowed
        p = expo * (1.0 / jnp.sum(expo, 0, keepdims=True))
        dp = scores_of(v[part], dm)
        ds = (p * (dp - jnp.sum(p * dp, 0, keepdims=True))).astype(BF)
        dv_ref[part] = mix_of(p.astype(BF), dm)
        dk_ref[part] = mix_of(ds, qm)
        tiles = []
        for tile in range(width // LANES):
            span = per_tile * tokens
            full = tn(
                ds[:, tile * span : (tile + 1) * span], kw[:, tile * LANES : (tile + 1) * LANES]
            )
            total = None
            for s in range(per_tile):
                block = full[s * tokens : (s + 1) * tokens]
                block = jnp.where(lane_head == s, block, 0.0)
                total = block if total is None else total + block
            tiles.append(total)
        dq_ref[part] = jnp.concatenate(tiles, axis=1)
    dqs = dq_ref[...]
    dkn = dk_ref[...]
    dq = scale * rq * (dqs - q * (rq * rq) * nn((q * dqs).astype(BF), ones))
    dk = rk * (dkn - k * (rk * rk) * nn((k * dkn).astype(BF), ones))
    return jnp.concatenate([dq.astype(BF), dk.astype(BF), dv_ref[...].astype(BF)], axis=1)


def split(cap):
    first = max(8, cap // 4)
    return (first, first, cap - 2 * first), min(16, first)


def route_kernel(
    parts, stage, count_ref, owner_ref, point_ref, r_ref, w2_ref, values_ref,
    send1_ref, send2_ref, send3_ref, mixed_ref, y_ref, buf_ref, tgt_ref, tgt_smem, sem,
):
    cap = sum(parts)
    slots = owner_ref.shape[1]
    devices = send1_ref.shape[0]
    stage.need(owner_ref, point_ref)
    owner = owner_ref[...]
    live = lax.broadcasted_iota(jnp.int32, (1, slots), 1) < count_ref[0]
    match = lax.broadcasted_iota(jnp.int32, (devices, slots), 0) == owner
    match = jnp.where(match, 1.0, 0.0).astype(F32)
    a = lax.broadcasted_iota(jnp.int32, (LANES, LANES), 0)
    b = lax.broadcasted_iota(jnp.int32, (LANES, LANES), 1)
    upper = jnp.where(a < b, 1.0, 0.0).astype(BF)
    chunks = slots // LANES
    flat = jnp.concatenate(
        [match[:, c * LANES : (c + 1) * LANES] for c in range(chunks)], axis=0
    )
    before = nn(flat.astype(BF), upper)
    carry = jnp.zeros((devices, 1), F32)
    ranks = []
    dump = devices * cap
    for c in range(chunks):
        here = match[:, c * LANES : (c + 1) * LANES]
        seen = before[c * devices : (c + 1) * devices] + carry
        ranks.append(jnp.sum(here * seen, 0, keepdims=True))
        span = slice(c * LANES, (c + 1) * LANES)
        spot = owner[:, span] * cap + ranks[-1].astype(jnp.int32)
        tgt_ref[c : c + 1, :] = jnp.where(live[:, span], spot, dump)
        carry = carry + jnp.sum(here, 1, keepdims=True)
    rank = jnp.concatenate(ranks, axis=1).astype(jnp.int32)
    copy = pltpu.make_async_copy(tgt_ref, tgt_smem, sem)
    copy.start()
    place = lax.broadcasted_iota(jnp.int32, (cap, slots), 0) == rank
    place = jnp.where(place & live, 1.0, 0.0).astype(BF)
    point = point_ref[...]
    high = (match * (point // LANES + 1).astype(F32)).astype(BF)
    low = (match * (point % LANES).astype(F32)).astype(BF)
    high = nt(high, place)
    low = nt(low, place)
    stage.need(r_ref, w2_ref, values_ref)
    best = lax.Precision.HIGHEST
    dims = (((1,), (1,)), ((), ()))
    m2 = lax.dot_general(
        r_ref[...], w2_ref[...], dims, precision=best, preferred_element_type=F32
    )
    mixed_ref[...] = jnp.dot(
        w2_ref[...], m2, precision=best, preferred_element_type=F32
    ).astype(BF)
    y = nn(values_ref[...].astype(BF), m2.astype(BF))
    y_ref[0, :, :] = y[:, :LANES]
    y_ref[1, :, :] = y[:, LANES:]
    buf_ref[...] = jnp.zeros_like(buf_ref)
    copy.wait()
    unroll = 16

    def move(c, _):
        base = pl.multiple_of(c * LANES, LANES)
        for start in range(0, LANES, unroll):
            spots = [tgt_smem[c, start + u] for u in range(unroll)]
            for half in range(2):
                for u in range(unroll):
                    buf_ref[half, pl.ds(spots[u], 1), :] = y_ref[
                        half, pl.ds(base + start + u, 1), :
                    ]
        return 0

    lax.fori_loop(0, chunks, move, 0)
    for d in range(devices):
        offset = d * cap
        for ref, size in zip((send1_ref, send2_ref, send3_ref), parts):
            for half in range(2):
                ref[d, 0:size, half * LANES : (half + 1) * LANES] = buf_ref[
                    half, offset : offset + size, :
                ].astype(BF)
            offset += size
    fill = ((0, 0), (0, LANES - cap))
    codes = jnp.concatenate([jnp.pad(high, fill), jnp.pad(low, fill)], axis=1)
    for d in range(devices):
        send1_ref[d, parts[0] : parts[0] + EXTRA, :] = jnp.broadcast_to(
            codes[d : d + 1], (EXTRA, 2 * LANES)
        ).astype(BF)


def route(owner, point, count, values, r_inverse, w2, devices, parts):
    slots, channels = values.shape
    cap = sum(parts)
    sizes = (parts[0] + EXTRA,) + tuple(parts[1:])
    return staged(
        functools.partial(route_kernel, parts),
        (count, owner, point, r_inverse, w2, values),
        tuple(jax.ShapeDtypeStruct((devices, n, channels), BF) for n in sizes)
        + (jax.ShapeDtypeStruct(w2.shape, BF),),
        [
            pltpu.VMEM((2, slots, LANES), F32),
            pltpu.VMEM((2, devices * cap + EXTRA, LANES), F32),
            pltpu.VMEM((slots // LANES, LANES), jnp.int32),
            pltpu.SMEM((slots // LANES, LANES), jnp.int32),
            pltpu.SemaphoreType.DMA,
        ],
        1e9,
        smem=(0,),
    )


def load_state(ins, extra):
    source, target, sems = ins[2], extra[0], extra[-1]
    for i in range(source.shape[0]):
        pltpu.make_async_copy(source.at[i], target.at[i], sems.at[i]).start()


def first_kernel(
    stage, scale_ref, order_ref, state_hbm, we_ref, gain_ref, wqkv_ref, wproj_ref, wup_ref, wdown_ref,
    top_ref, left_ref, corner_ref, z1_ref, h1_ref, h0_ref, hm_ref, qkv_ref, gp_ref,
    state_ref, ones_ref, mask_ref, e_ref, o_ref, sems,
):
    rows, _, cols, _, _ = state_ref.shape
    width = we_ref.shape[1]
    tokens = WIN * WIN
    chunk = cols * tokens

    def load(i):
        return pltpu.make_async_copy(state_hbm.at[i], state_ref.at[i], sems.at[i])

    ones_ref[...] = head_ones(width, width // HEADS)
    mask_ref[...] = head_stack(tokens, width // HEADS)
    scale = scale_lanes(scale_ref, 0, width)
    stage.need(we_ref, gain_ref)

    def body(i, _):
        load(i).wait()
        x = jnp.concatenate([window(state_ref, i, w).astype(BF) for w in range(cols)], axis=0)
        h0 = nn(x, we_ref[...])
        here = pl.ds(pl.multiple_of(i * chunk, chunk), chunk)
        h0_ref[here, :] = h0
        stage.emit_part(here, h0_ref)
        stage.need_at(i == 0, wqkv_ref)
        qkv = nn(norm(h0, gain_ref[0, 0:1]), wqkv_ref[...]).astype(BF)
        qkv_ref[here, :] = qkv
        stage.emit_part(here, qkv_ref)
        mixed = attention_chunk(qkv, scale, ones_ref, mask_ref, None, e_ref, o_ref, cols, tokens)
        stage.need_at(i == 0, wproj_ref, wup_ref, wdown_ref)
        hm = h0 + nn(mixed, wproj_ref[...]).astype(BF).astype(F32)
        hm_ref[here, :] = hm
        stage.emit_part(here, hm_ref)
        inner, slope = gelu_parts(nn(norm(hm, gain_ref[0, 1:2]), wup_ref[...]))
        gp_ref[here, :] = slope.astype(BF)
        stage.emit_part(here, gp_ref)
        h1 = hm + nn(inner.astype(BF), wdown_ref[...])
        z1 = norm(h1, gain_ref[1, 0:1]).astype(F32)
        for w in range(cols):
            part = slice(w * tokens, (w + 1) * tokens)
            h1_ref[i, :, w, :, :] = h1[part].reshape(WIN, WIN, width)
            z1_ref[i, :, w, :, :] = z1[part].reshape(WIN, WIN, width)
        stage.emit_part(i, z1_ref, h1_ref)
        return 0

    lax.fori_loop(0, rows, body, 0)
    top_ref[...] = z1_ref[0, 0:SHIFT, :, :, :].astype(BF)
    left_ref[...] = z1_ref[:, :, 0, 0:SHIFT, :].astype(BF)
    corner_ref[...] = z1_ref[0, 0:SHIFT, 0, 0:SHIFT, :].astype(BF)


def first_block(order, state5, we, gains, wqkv, wproj, scale, wup, wdown):
    wr, _, wc, _, _ = state5.shape
    width = we.shape[1]
    tokens = wr * wc * WIN * WIN
    chunk = wc * WIN * WIN
    sh = jax.ShapeDtypeStruct
    outs = (
        sh((SHIFT, wc, WIN, width), BF),
        sh((wr, WIN, SHIFT, width), BF),
        sh((SHIFT, SHIFT, width), BF),
        sh((wr, WIN, wc, WIN, width), F32),
        sh((wr, WIN, wc, WIN, width), F32),
        sh((tokens, width), F32),
        sh((tokens, width), F32),
        sh((tokens, 3 * width), BF),
        sh((tokens, wup.shape[2]), BF),
    )
    return staged(
        first_kernel,
        (scale, order, state5, we, gains, wqkv, wproj, wup, wdown),
        outs,
        [
            pltpu.VMEM(state5.shape, F32),
            pltpu.VMEM((width, width), BF),
            pltpu.VMEM((LANES * HEADS // width * WIN * WIN, LANES), BF),
            pltpu.VMEM((chunk, HEADS * WIN * WIN), BF),
            pltpu.VMEM((chunk, width), F32),
            pltpu.SemaphoreType.DMA((wr,)),
        ],
        2e9,
        smem=(0,),
        raw=(1, 2),
        early=load_state,
        layer={5: 0, 6: 0, 7: 0, 8: 0},
    )


def fill_ahead(pad_ref, own, right_ref, below_ref, corner_ref):
    rows, cols, _ = own.shape
    pad_ref[0:rows, 0:cols, :] = own
    pad_ref[0:rows, cols : cols + SHIFT, :] = right_ref[...].astype(F32)
    pad_ref[rows : rows + SHIFT, 0:cols, :] = below_ref[...].astype(F32)
    pad_ref[rows : rows + SHIFT, cols : cols + SHIFT, :] = corner_ref[...].astype(F32)


def rolled_window(pad_ref, i, w):
    block = pad_ref[
        pl.ds(i * WIN + SHIFT, WIN), SHIFT + w * WIN : SHIFT + (w + 1) * WIN, :
    ]
    return block.reshape(WIN * WIN, block.shape[2])


def emit_behind(out_ref, low_ref, east_ref, corner_ref):
    rows, cols, _ = out_ref.shape
    low_ref[...] = out_ref[rows - SHIFT : rows, :, :].astype(BF)
    east_ref[...] = out_ref[:, cols - SHIFT : cols, :].astype(BF)
    corner_ref[...] = out_ref[rows - SHIFT : rows, cols - SHIFT : cols, :].astype(BF)


def shifted_kernel(
    total_rows, stage, start_ref, scale_ref, z1_ref, right_ref, below_ref, corner_ref, wqkv_ref,
    wproj_ref, ans_ref, low_ref, east_ref, last_ref, qkv_ref,
    pad_ref, ones_ref, mask_ref, e_ref, o_ref,
):
    rows, cols, width = z1_ref.shape
    wr, wc = rows // WIN, cols // WIN
    tokens = WIN * WIN
    chunk = wc * tokens
    ones_ref[...] = head_ones(width, width // HEADS)
    mask_ref[...] = head_stack(tokens, width // HEADS)
    scale = scale_lanes(scale_ref, 1, width)
    stage.need(z1_ref, right_ref, below_ref, corner_ref)
    fill_ahead(pad_ref, z1_ref[...], right_ref, below_ref, corner_ref)
    threshold = total_rows - SHIFT - start_ref[0]

    def body(i, _):
        z = jnp.concatenate([rolled_window(pad_ref, i, w).astype(BF) for w in range(wc)], axis=0)
        stage.need_at(i == 0, wqkv_ref, wproj_ref)
        qkv = nn(z, wqkv_ref[...]).astype(BF)
        here = pl.ds(pl.multiple_of(i * chunk, chunk), chunk)
        qkv_ref[here, :] = qkv
        stage.emit_part(here, qkv_ref)
        allowed = side_mask(i, threshold, tokens)
        mixed = attention_chunk(qkv, scale, ones_ref, mask_ref, allowed, e_ref, o_ref, wc, tokens)
        answer = nn(mixed, wproj_ref[...]).astype(BF).astype(F32)
        for w in range(wc):
            ans_ref[pl.ds(i * WIN, WIN), w * WIN : (w + 1) * WIN, :] = answer[
                w * tokens : (w + 1) * tokens
            ].reshape(WIN, WIN, width)
        stage.emit_part(pl.ds(i * WIN, WIN), ans_ref)
        return 0

    lax.fori_loop(0, wr, body, 0)
    emit_behind(ans_ref, low_ref, east_ref, last_ref)


def behind_shapes(rows, cols, width):
    sh = jax.ShapeDtypeStruct
    return (
        sh((rows, cols, width), F32),
        sh((SHIFT, cols, width), BF),
        sh((rows, SHIFT, width), BF),
        sh((SHIFT, SHIFT, width), BF),
    )


def shifted_forward(start, z1, right, below, corner, wqkv, wproj, scale, total_rows):
    rows, cols, width = z1.shape
    tokens = rows * cols
    chunk = cols * WIN
    outs = behind_shapes(rows, cols, width) + (jax.ShapeDtypeStruct((tokens, 3 * width), BF),)
    return staged(
        functools.partial(shifted_kernel, total_rows),
        (start, scale, z1, right, below, corner, wqkv, wproj),
        outs,
        [
            pltpu.VMEM((rows + SHIFT, cols + WIN, width), F32),
            pltpu.VMEM((width, width), BF),
            pltpu.VMEM((LANES * HEADS // width * WIN * WIN, LANES), BF),
            pltpu.VMEM((chunk, HEADS * WIN * WIN), BF),
            pltpu.VMEM((chunk, width), F32),
        ],
        1e9,
        smem=(0, 1),
        vmem=(3, 4, 5),
        layer={6: 1, 7: 1},
    )


def fill_behind(pad_ref, own, above_ref, west_ref, corner_ref):
    rows, cols, _ = own.shape
    pad_ref[SHIFT : SHIFT + rows, SHIFT : SHIFT + cols, :] = own
    pad_ref[0:SHIFT, SHIFT : SHIFT + cols, :] = above_ref[...].astype(F32)
    pad_ref[SHIFT : SHIFT + rows, 0:SHIFT, :] = west_ref[...].astype(F32)
    pad_ref[0:SHIFT, 0:SHIFT, :] = corner_ref[...].astype(F32)


def group_jobs(cnt_smem, offset, size, group, body):
    devices = cnt_smem.shape[0]

    def each(d, _):
        valid = cnt_smem[d, 0] - offset
        for g in range(0, size, group):

            @pl.when(valid > g)
            def _():
                body(d, offset + g, pl.multiple_of(d * size + g, group))

        return 0

    lax.fori_loop(0, devices, each, 0)


def gather_part(table_ref, found_ref, idx_smem, cnt_smem, offset, size, group):
    def body(d, slot, row):
        for u in range(group):
            found_ref[pl.ds(row + u, 1), :] = table_ref[pl.ds(idx_smem[d, slot + u], 1), :]

    group_jobs(cnt_smem, offset, size, group, body)


def scatter_part(table_ref, found_ref, idx_smem, cnt_smem, dup_smem, offset, size, group):
    def body(d, slot, row):
        @pl.when(dup_smem[d, slot] == 0)
        def _():
            spots = [idx_smem[d, slot + u] for u in range(group)]
            sums = [
                table_ref[pl.ds(spots[u], 1), :] + found_ref[pl.ds(row + u, 1), :]
                for u in range(group)
            ]
            for u in range(group):
                table_ref[pl.ds(spots[u], 1), :] = sums[u]

        @pl.when(dup_smem[d, slot] != 0)
        def _():
            def one(u, _):
                spot = pl.ds(idx_smem[d, slot + u], 1)
                table_ref[spot, :] = table_ref[spot, :] + found_ref[pl.ds(row + u, 1), :]
                return 0

            lax.fori_loop(0, group, one, 0)

    group_jobs(cnt_smem, offset, size, group, body)


def radiance_part(found_ref, obs_ref, mixed_ref, w1_ref, size):
    devices, _, channels = obs_ref.shape
    batch = min(devices, max(1, 512 // size))

    def body(i, _):
        here = pl.ds(pl.multiple_of(i * batch * size, batch * size), batch * size)
        y = obs_ref[pl.ds(i * batch, batch), 0:size, :].astype(F32)
        y = y.reshape(batch * size, channels)
        t = jnp.tanh(nn(found_ref[here, :].astype(BF), w1_ref[...].astype(BF)))
        pulled = (nn(t.astype(BF), mixed_ref[...]) - y) * (1.0 - t * t)
        found_ref[here, :] = nt(pulled.astype(BF), w1_ref[...].astype(BF))
        return 0

    lax.fori_loop(0, devices // batch, body, 0)


def spread(table_ref, moved_ref, i, step, tokens):
    for s in range(PIX):
        there = pl.ds(pl.multiple_of(s * tokens + i * step, WIN), step)
        moved_ref[:, s * VARS : (s + 1) * VARS] = table_ref[there, 0:VARS]


def forecast_kernel(
    parts, group, stage, obs1_ref, h1_ref, ans_ref, above_ref, west_ref, corner_ref, gain_ref,
    wup_ref, wdown_ref, whead_ref, state_ref, w1_in_ref, mixed_ref, obs2_ref, back_ref, inv_ref,
    h2_ref, gp_ref, prior_ref, found3_ref, idx_ref, cnt_ref, dup_ref, pulled_ref, w1_ref,
    pad_ref, table_ref, moved_ref, found1_ref, found2_ref, idx_smem, cnt_smem, dup_smem, sems,
):
    rows, cols, width = h1_ref.shape
    devices = obs1_ref.shape[0]
    tokens = rows * cols
    step = tokens // 2

    stage.need(obs1_ref)
    codes = obs1_ref[:, parts[0] : parts[0] + EXTRA, :].astype(F32)[:, 0, :]
    high = codes[:, :LANES].astype(jnp.int32)
    low = codes[:, LANES : 2 * LANES].astype(jnp.int32)
    point = jnp.where(high > 0, (high - 1) * LANES + low, 0)
    lane = lax.broadcasted_iota(jnp.int32, (devices, LANES), 1)
    idx = jnp.where(
        high > 0, (point % PIX) * tokens + point // PIX, PIX * tokens + lane % group
    )
    idx_ref[...] = idx
    cnt_ref[...] = jnp.broadcast_to(
        jnp.sum(jnp.where(high > 0, 1.0, 0.0), 1, keepdims=True), (devices, LANES)
    ).astype(jnp.int32)
    same = jnp.zeros((devices, LANES), jnp.int32)
    for s in range(1, group):
        hit = (pltpu.roll(idx, s, 1) == idx) & (lane % group >= s)
        same = jnp.maximum(same, jnp.where(hit, 1, 0))
    s = group // 2
    while s:
        same = jnp.maximum(same, pltpu.roll(same, LANES - s, 1))
        s //= 2
    dup_ref[...] = same
    copies = [
        pltpu.make_async_copy(a, b, sems.at[n])
        for n, (a, b) in enumerate(
            ((idx_ref, idx_smem), (cnt_ref, cnt_smem), (dup_ref, dup_smem))
        )
    ]
    for copy in copies:
        copy.start()
    stage.need(h1_ref, ans_ref, above_ref, west_ref, corner_ref)
    fill_behind(pad_ref, ans_ref[...], above_ref, west_ref, corner_ref)
    h2_ref[...] = (h1_ref[...] + pad_ref[0:rows, 0:cols, :]).reshape(tokens, width)
    table_ref[PIX * tokens :, :] = jnp.zeros((group, LANES), F32)
    blank = jnp.zeros((step, LANES - VARS), F32)
    stage.need(gain_ref, wup_ref, wdown_ref)

    def forward(i, _):
        here = pl.ds(pl.multiple_of(i * step, step), step)
        h2 = h2_ref[here, :]
        inner, slope = gelu_parts(nn(norm(h2, gain_ref[1, 1:2]), wup_ref[...]))
        gp_ref[here, :] = slope.astype(BF)
        h3 = (h2 + nn(inner.astype(BF), wdown_ref[...])).astype(BF)
        stage.need_at(i == 0, whead_ref, state_ref)
        moved = state_ref[here, :] + nt(h3, whead_ref[...])
        for s in range(PIX):
            there = pl.ds(pl.multiple_of(s * tokens + i * step, WIN), step)
            table_ref[there, :] = jnp.concatenate(
                [moved[:, s * VARS : (s + 1) * VARS], blank], axis=1
            )
        return 0

    lax.fori_loop(0, 2, forward, 0)
    stage.emit(h2_ref, gp_ref, idx_ref, cnt_ref, dup_ref)
    stage.need(back_ref, inv_ref, w1_in_ref, mixed_ref, obs2_ref)
    w1_ref[...] = jnp.zeros_like(w1_ref)
    w1_ref[0:VARS, :] = w1_in_ref[...]
    w1_ref[...] = w1_ref[...].astype(BF).astype(F32)
    for copy in copies:
        copy.wait()
    offsets = (0, parts[0], parts[0] + parts[1])
    founds = (found1_ref, found2_ref, found3_ref)
    for offset, size, found in zip(offsets, parts, founds):
        gather_part(table_ref, found, idx_smem, cnt_smem, offset, size, group)
    stage.emit(found3_ref)
    table_ref[...] = jnp.zeros_like(table_ref)
    radiance_part(found1_ref, obs1_ref, mixed_ref, w1_ref, parts[0])
    scatter_part(table_ref, found1_ref, idx_smem, cnt_smem, dup_smem, 0, parts[0], group)
    radiance_part(found2_ref, obs2_ref, mixed_ref, w1_ref, parts[1])
    scatter_part(table_ref, found2_ref, idx_smem, cnt_smem, dup_smem, parts[0], parts[1], group)

    def collect(i, _):
        here = pl.ds(pl.multiple_of(i * step, step), step)
        spread(table_ref, moved_ref, i, step, tokens)
        moved = moved_ref[...]
        prior_ref[here, :] = moved + inv_ref[...].reshape(1, -1) * (state_ref[here, :] - back_ref[here, :])
        stage.emit_part(here, prior_ref)
        pulled_ref[here, :] = nn(moved.astype(BF), whead_ref[...])
        stage.emit_part(here, pulled_ref)
        return 0

    lax.fori_loop(0, 2, collect, 0)


def forecast(
    h1, ans, above, west, corner, state, background, inv, obs1, obs2, mixed, gains, wup, wdown,
    whead, w1, parts, group,
):
    rows, cols, width = h1.shape
    tokens = rows * cols
    devices = obs1.shape[0]
    sh = jax.ShapeDtypeStruct
    outs = (
        sh((tokens, width), F32),
        sh((tokens, wup.shape[2]), BF),
        sh(state.shape, F32),
        sh((devices * parts[2], LANES), F32),
        sh((devices, LANES), jnp.int32),
        sh((devices, LANES), jnp.int32),
        sh((devices, LANES), jnp.int32),
        sh((tokens, width), F32),
        sh((LANES, w1.shape[1]), F32),
    )
    return staged(
        functools.partial(forecast_kernel, parts, group),
        (
            obs1, h1, ans, above, west, corner, gains, wup, wdown, whead, state, w1, mixed, obs2,
            background, inv,
        ),
        outs,
        [
            pltpu.VMEM((rows + SHIFT, cols + WIN, width), F32),
            pltpu.VMEM((PIX * tokens + group, LANES), F32),
            pltpu.VMEM((tokens // 2, state.shape[1]), F32),
            pltpu.VMEM((devices * parts[0], LANES), F32),
            pltpu.VMEM((devices * parts[1], LANES), F32),
        ]
        + [pltpu.SMEM((devices, LANES), jnp.int32)] * 3
        + [pltpu.SemaphoreType.DMA((3,))],
        3e9,
        vmem=(0, 3, 4, 5, 13),
        layer={7: 1, 8: 1},
    )


def adjoint_kernel(
    parts, group, stage, idx_smem, cnt_smem, dup_smem, w1_ref, mixed_ref, work_ref, obs3_ref,
    whead_ref, pulled_ref, prior_ref, wdown_ref, gp_ref, wup_ref, h2_ref, gain_ref,
    top_ref, left_ref, edge_ref, third_ref, out_ref, table_ref, moved_ref,
):
    rows, cols, width = third_ref.shape
    tokens = rows * cols
    step = tokens // 2
    table_ref[...] = jnp.zeros_like(table_ref)
    stage.need(idx_smem, cnt_smem, dup_smem, w1_ref, mixed_ref, work_ref, obs3_ref)
    radiance_part(work_ref, obs3_ref, mixed_ref, w1_ref, parts[2])
    scatter_part(
        table_ref, work_ref, idx_smem, cnt_smem, dup_smem, parts[0] + parts[1], parts[2], group
    )
    stage.need(whead_ref, pulled_ref, prior_ref, wdown_ref, gp_ref, wup_ref, h2_ref, gain_ref)
    half = rows // 2

    def backward(i, _):
        here = pl.ds(pl.multiple_of(i * step, step), step)
        spread(table_ref, moved_ref, i, step, tokens)
        moved = moved_ref[...]
        out_ref[here, :] = moved + prior_ref[here, :]
        stage.emit_part(here, out_ref)
        grad = (pulled_ref[here, :] + nn(moved.astype(BF), whead_ref[...])).astype(BF)
        d_inner = nt(grad, wdown_ref[...]) * gp_ref[here, :].astype(F32)
        d_normed = nt(d_inner.astype(BF), wup_ref[...])
        third = grad.astype(F32) + norm_back(h2_ref[here, :], gain_ref[1, 1:2], d_normed)
        third_ref[pl.ds(i * half, half), :, :] = third.reshape(half, cols, width)
        stage.emit_part(pl.ds(i * half, half), third_ref)
        return 0

    lax.fori_loop(0, 2, backward, 0)
    top_ref[...] = third_ref[0:SHIFT, :, :].astype(BF)
    left_ref[...] = third_ref[:, 0:SHIFT, :].astype(BF)
    edge_ref[...] = third_ref[0:SHIFT, 0:SHIFT, :].astype(BF)


def adjoint(
    idx, cnt, dup, found, obs3, mixed, w1, h2, gp, gains, wup, wdown, whead, prior, pulled, parts,
    group, rows, cols,
):
    width = h2.shape[1]
    third, top, left, edge = behind_shapes(rows, cols, width)
    outs = (top, left, edge, third, jax.ShapeDtypeStruct(prior.shape, F32))
    return staged(
        functools.partial(adjoint_kernel, parts, group),
        (idx, cnt, dup, w1, mixed, found, obs3, whead, pulled, prior, wdown, gp, wup, h2, gains),
        outs,
        [
            pltpu.VMEM((PIX * rows * cols + group, LANES), F32),
            pltpu.VMEM((prior.shape[0] // 2, prior.shape[1]), F32),
        ],
        2e9,
        scalars=(0, 1, 2),
        vmem=(6,),
        layer={10: 1, 12: 1},
    )


def shifted_back_kernel(
    total_rows, stage, start_ref, scale_ref, third_ref, right_ref, below_ref, corner_ref,
    wproj_ref, qkv_ref, wqkv_ref, dz_ref, low_ref, east_ref, last_ref,
    pad_ref, ones_ref, mask_ref, dq_ref, dk_ref, dv_ref,
):
    rows, cols, width = third_ref.shape
    wr, wc = rows // WIN, cols // WIN
    tokens = WIN * WIN
    chunk = wc * tokens
    ones_ref[...] = head_ones(width, width // HEADS)
    mask_ref[...] = head_stack(tokens, width // HEADS)
    scale = scale_lanes(scale_ref, 1, width)
    stage.need(third_ref, right_ref, below_ref, corner_ref)
    fill_ahead(pad_ref, third_ref[...], right_ref, below_ref, corner_ref)
    threshold = total_rows - SHIFT - start_ref[0]

    def body(i, _):
        d_answer = jnp.concatenate(
            [rolled_window(pad_ref, i, w).astype(BF) for w in range(wc)], axis=0
        )
        stage.need_at(i == 0, wproj_ref, qkv_ref, wqkv_ref)
        d_out = nt(d_answer, wproj_ref[...]).astype(BF)
        allowed = side_mask(i, threshold, tokens)
        qkv = qkv_ref[pl.ds(pl.multiple_of(i * chunk, chunk), chunk), :]
        d_qkv = attention_chunk_back(
            qkv, d_out, scale, ones_ref, mask_ref, allowed,
            dq_ref, dk_ref, dv_ref, wc, tokens,
        )
        dz = nt(d_qkv, wqkv_ref[...]).astype(BF).astype(F32)
        for w in range(wc):
            dz_ref[pl.ds(i * WIN, WIN), w * WIN : (w + 1) * WIN, :] = dz[
                w * tokens : (w + 1) * tokens
            ].reshape(WIN, WIN, width)
        stage.emit_part(pl.ds(i * WIN, WIN), dz_ref)
        return 0

    lax.fori_loop(0, wr, body, 0)
    emit_behind(dz_ref, low_ref, east_ref, last_ref)


def shifted_backward(start, third, right, below, corner, qkv, wqkv, wproj, scale, total_rows):
    rows, cols, width = third.shape
    chunk = cols * WIN
    outs = behind_shapes(rows, cols, width)
    return staged(
        functools.partial(shifted_back_kernel, total_rows),
        (start, scale, third, right, below, corner, wproj, qkv, wqkv),
        outs,
        [
            pltpu.VMEM((rows + SHIFT, cols + WIN, width), F32),
            pltpu.VMEM((width, width), BF),
            pltpu.VMEM((LANES * HEADS // width * WIN * WIN, LANES), BF),
        ]
        + [pltpu.VMEM((chunk, width), F32)] * 3,
        1e9,
        smem=(0, 1),
        vmem=(3, 4, 5, 6, 7, 8),
        layer={6: 1, 8: 1},
    )


def last_kernel(
    stage, scale_ref, partial_hbm, dz_ref, above_ref, west_ref, corner_ref, third_ref, h1_ref,
    gain_ref, wdown_ref, gp_ref, wup_ref, hm_ref, wproj_ref, qkv_ref, wqkv_ref, h0_ref, we_ref,
    out_hbm,
    pad_ref, ones_ref, mask_ref, dq_ref, dk_ref, dv_ref, out_ref, in_sems, out_sems,
):
    rows, cols, width = dz_ref.shape
    wr, wc = rows // WIN, cols // WIN
    tokens = WIN * WIN
    chunk = wc * tokens

    def rows_of(ref, i):
        return ref.at[pl.ds(i * WIN, WIN)]

    ones_ref[...] = head_ones(width, width // HEADS)
    mask_ref[...] = head_stack(tokens, width // HEADS)
    scale = scale_lanes(scale_ref, 0, width)
    for i in range(wr):
        pltpu.make_async_copy(rows_of(partial_hbm, i), rows_of(out_ref, i), in_sems.at[i]).start()
    stage.need(dz_ref, above_ref, west_ref, corner_ref)
    fill_behind(pad_ref, dz_ref[...], above_ref, west_ref, corner_ref)

    def body(i, _):
        here = pl.ds(pl.multiple_of(i * chunk, chunk), chunk)
        band = pl.ds(i * WIN, WIN)

        def take(ref):
            return jnp.concatenate(
                [
                    ref[band, w * WIN : (w + 1) * WIN, :].reshape(tokens, width)
                    for w in range(wc)
                ],
                axis=0,
            )

        stage.need_at(i == 0, third_ref, h1_ref, gain_ref, wdown_ref, gp_ref, wup_ref)
        second = take(third_ref) + norm_back(take(h1_ref), gain_ref[1, 0:1], take(pad_ref))
        d_inner = nt(second.astype(BF), wdown_ref[...]) * gp_ref[here, :].astype(F32)
        d_normed = nt(d_inner.astype(BF), wup_ref[...])
        stage.need_at(i == 0, hm_ref, wproj_ref, qkv_ref, wqkv_ref, h0_ref, we_ref)
        d_hm = second + norm_back(hm_ref[here, :], gain_ref[0, 1:2], d_normed)
        d_out = nt(d_hm.astype(BF), wproj_ref[...]).astype(BF)
        d_qkv = attention_chunk_back(
            qkv_ref[here, :], d_out, scale, ones_ref, mask_ref, None,
            dq_ref, dk_ref, dv_ref, wc, tokens,
        )
        dz = nt(d_qkv, wqkv_ref[...])
        d_h0 = (d_hm + norm_back(h0_ref[here, :], gain_ref[0, 0:1], dz)).astype(BF)
        pltpu.make_async_copy(rows_of(partial_hbm, i), rows_of(out_ref, i), in_sems.at[i]).wait()
        for w in range(wc):
            grad = nt(d_h0[w * tokens : (w + 1) * tokens], we_ref[...])
            grad = grad.reshape(WIN, WIN, grad.shape[1])
            spot = (band, slice(w * WIN, (w + 1) * WIN), slice(None))
            out_ref[spot] = grad + out_ref[spot]
        pltpu.make_async_copy(rows_of(out_ref, i), rows_of(out_hbm, i), out_sems.at[i]).start()
        return 0

    lax.fori_loop(0, wr, body, 0)
    for i in range(wr):
        pltpu.make_async_copy(rows_of(out_ref, i), rows_of(out_hbm, i), out_sems.at[i]).wait()


def last_block(
    third, dz, above, west, corner, h1, h0, hm, qkv, gp, we, gains, wqkv, wproj, scale,
    wup, wdown, partial,
):
    rows, cols, width = dz.shape
    chunk = cols * WIN
    (result,) = staged(
        last_kernel,
        (
            scale, partial, dz, above, west, corner, third, h1, gains, wdown, gp, wup, hm, wproj,
            qkv, wqkv, h0, we,
        ),
        (jax.ShapeDtypeStruct(partial.shape, F32),),
        [
            pltpu.VMEM((rows + SHIFT, cols + WIN, width), F32),
            pltpu.VMEM((width, width), BF),
            pltpu.VMEM((LANES * HEADS // width * WIN * WIN, LANES), BF),
        ]
        + [pltpu.VMEM((chunk, width), F32)] * 3
        + [
            pltpu.VMEM(partial.shape, F32),
            pltpu.SemaphoreType.DMA((rows // WIN,)),
            pltpu.SemaphoreType.DMA((rows // WIN,)),
        ],
        2e9,
        smem=(0,),
        raw=(1,),
        raw_outs=(0,),
        vmem=(3, 4, 5, 7, 8, 9, 10, 11, 12, 13, 14, 15, 16, 17),
        layer={9: 0, 11: 0, 13: 0, 15: 0},
    )
    return result


def neighbour(x, by_lat, by_lon):
    lat, lon = lax.axis_size("lat"), lax.axis_size("lon")
    pairs = [
        (a * lon + b, ((a + by_lat) % lat) * lon + (b + by_lon) % lon)
        for a in range(lat)
        for b in range(lon)
    ]
    return lax.ppermute(x, ("lat", "lon"), pairs)


def exchange(x):
    return lax.all_to_all(x, ("lat", "lon"), split_axis=0, concat_axis=0, tiled=True)


def local(
    state,
    background,
    inv_background,
    w_embed,
    norm_gain,
    w_qkv,
    w_proj,
    head_scale,
    w_up,
    w_down,
    w_head,
    w_obs1,
    w_obs2,
    r_inverse,
    obs_values,
    obs_owner,
    obs_point,
    obs_count,
):
    rows, cols, patch_values = state.shape
    width = w_embed.shape[1]
    total_rows = rows * lax.axis_size("lat")
    row_start = (lax.axis_index("lat") * rows).astype(jnp.int32).reshape(1)
    devices = lax.axis_size("lat") * lax.axis_size("lon")
    slots = obs_values.shape[0]
    cap = 2 * slots // devices

    parts, group = split(cap)

    send1, send2, send3, mixed = route(
        obs_owner.reshape(1, slots), obs_point.reshape(1, slots), obs_count, obs_values,
        r_inverse, w_obs2, devices, parts,
    )
    obs1 = exchange(send1)
    state5 = state.reshape(rows // WIN, WIN, cols // WIN, WIN, patch_values)
    top, left, corner, z1, h1, h0, hm, qkv0, gp0 = first_block(
        mixed, state5, w_embed, norm_gain, w_qkv, w_proj, head_scale, w_up, w_down
    )
    z1 = z1.reshape(rows, cols, width)
    h1 = h1.reshape(rows, cols, width)
    below = neighbour(top.reshape(SHIFT, cols, width), -1, 0)
    right = neighbour(left.reshape(rows, SHIFT, width), 0, -1)
    corner = neighbour(corner, -1, -1)
    obs1, send2 = lax.optimization_barrier((obs1, send2))
    obs2 = exchange(send2)
    answer, low, east, last, qkv1 = shifted_forward(
        row_start, z1, right, below, corner, w_qkv, w_proj, head_scale, total_rows
    )
    above = neighbour(low, 1, 0)
    west = neighbour(east, 0, 1)
    last = neighbour(last, 1, 1)
    obs2, send3 = lax.optimization_barrier((obs2, send3))
    obs3 = exchange(send3)
    flat = (rows * cols, patch_values)
    h2, gp1, prior, found, idx, cnt, dup, pulled, w1 = forecast(
        h1, answer, above, west, last, state.reshape(flat), background.reshape(flat),
        inv_background, obs1, obs2, mixed, norm_gain, w_up, w_down, w_head.T,
        w_obs1, parts, group,
    )
    top, left, corner, third, partial = adjoint(
        idx, cnt, dup, found, obs3, mixed, w1, h2, gp1, norm_gain, w_up, w_down, w_head.T, prior,
        pulled,
        parts, group, rows, cols,
    )
    below = neighbour(top, -1, 0)
    right = neighbour(left, 0, -1)
    corner = neighbour(corner, -1, -1)
    dz, low, east, last = shifted_backward(
        row_start, third, right, below, corner, qkv1, w_qkv, w_proj, head_scale, total_rows
    )
    above = neighbour(low, 1, 0)
    west = neighbour(east, 0, 1)
    last = neighbour(last, 1, 1)
    return last_block(
        third, dz, above, west, last, h1, h0, hm, qkv0, gp0, w_embed, norm_gain, w_qkv, w_proj,
        head_scale, w_up, w_down, partial.reshape(state.shape),
    )


def solution(mesh):
    placed = (
        P("lat", "lon", None),
        P("lat", "lon", None),
        P(),
        P(),
        P(),
        P(),
        P(),
        P(),
        P(),
        P(),
        P(),
        P(),
        P(),
        P(),
        P(("lat", "lon"), None),
        P(("lat", "lon"), None),
        P(("lat", "lon")),
        P(("lat", "lon")),
    )

    return jax.shard_map(
        local, mesh=mesh, in_specs=placed, out_specs=P("lat", "lon", None), check_vma=False
    )
```

```python
import functools

import jax
import jax.numpy as jnp
from jax import lax
from jax.experimental import pallas as pl
from jax.experimental.pallas import tpu as pltpu
from jax.sharding import PartitionSpec as P


HEADS = 8
VARS = 69
PIX = 16
WIN = 8
SHIFT = 4
LANES = 128
EXTRA = 8
EPS = 1e-05
BF = jnp.bfloat16
F32 = jnp.float32
SQRT_2_OVER_PI = 0.7978845608028654
CUBIC = 0.044715

SMEM = pl.BlockSpec(memory_space=pltpu.SMEM)
VMEM = pl.BlockSpec(memory_space=pltpu.VMEM)
HBM = pl.BlockSpec(memory_space=pltpu.HBM)
MIB = 1024 * 1024
ROOM = 44


class Stage:
    def __init__(self):
        self.inputs = {}
        self.outputs = {}
        self.waited = set()
        self.sent = set()

    def need(self, *refs):
        for ref in refs:
            if id(ref) not in self.waited:
                self.waited.add(id(ref))
                self.inputs[id(ref)].wait()

    def need_at(self, first, *refs):
        pending = [ref for ref in refs if id(ref) not in self.waited]
        self.waited.update(id(ref) for ref in pending)

        @pl.when(first)
        def _():
            for ref in pending:
                self.inputs[id(ref)].wait()

    def emit_part(self, part, *refs):
        for ref in refs:
            self.sent.add(id(ref))
            self.outputs[id(ref)].part(part).start()

    def emit(self, *refs):
        for ref in refs:
            if id(ref) not in self.sent:
                self.sent.add(id(ref))
                self.outputs[id(ref)].start()

    def close(self):
        for key, copy in self.inputs.items():
            if key not in self.waited:
                copy.wait()
        for key, copy in self.outputs.items():
            if key not in self.sent:
                copy.start()
        for copy in self.outputs.values():
            copy.wait()


class Outgoing:
    def __init__(self, source, target, sem):
        self.refs = (source, target, sem)

    def part(self, part):
        source, target, sem = self.refs
        return pltpu.make_async_copy(source.at[part], target.at[part], sem)

    def start(self):
        pltpu.make_async_copy(*self.refs).start()

    def wait(self):
        pltpu.make_async_copy(*self.refs).wait()


def staged(
    body, args, outs, scratch, flops, smem=(), raw=(), raw_outs=(), layer=None, vmem=(),
    early=lambda ins, extra: None,
    scalars=(),
):
    layer = layer or {}
    count = len(args)
    placed = [
        x if i in smem or i in vmem else pltpu.with_memory_space_constraint(x, pltpu.HBM)
        for i, x in enumerate(args)
    ]
    in_buffers = []
    for i, x in enumerate(args):
        if i not in smem and i not in raw and i not in vmem:
            shape = x.shape[1:] if i in layer else x.shape
            space = pltpu.SMEM if i in scalars else pltpu.VMEM
            in_buffers.append((i, space(shape, x.dtype)))
    out_buffers = [
        (j, pltpu.VMEM(o.shape, o.dtype)) for j, o in enumerate(outs) if j not in raw_outs
    ]

    def kernel(*refs):
        ins = [
            ref.at[layer[i]] if i in vmem and i in layer else ref
            for i, ref in enumerate(refs[:count])
        ]
        results = list(refs[count : count + len(outs)])
        rest = list(refs[count + len(outs) :])
        ins_vmem = rest[: len(in_buffers)]
        outs_vmem = rest[len(in_buffers) : len(in_buffers) + len(out_buffers)]
        in_sems, out_sems = rest[-2:]
        extra = rest[len(in_buffers) + len(out_buffers) : -2]
        stage = Stage()
        early(ins, extra)
        stage.waited.update(id(ins[i]) for i in vmem)
        for n, ((i, _), buffer) in enumerate(zip(in_buffers, ins_vmem)):
            source = ins[i].at[layer[i]] if i in layer else ins[i]
            copy = pltpu.make_async_copy(source, buffer, in_sems.at[n])
            copy.start()
            stage.inputs[id(buffer)] = copy
            ins[i] = buffer
        for n, ((j, _), buffer) in enumerate(zip(out_buffers, outs_vmem)):
            stage.outputs[id(buffer)] = Outgoing(buffer, results[j], out_sems.at[n])
            results[j] = buffer
        body(stage, *ins, *results, *extra)
        stage.close()

    return pl.pallas_call(
        kernel,
        out_shape=tuple(pltpu.HBM(o.shape, o.dtype) for o in outs),
        in_specs=[
            SMEM if i in smem else VMEM if i in vmem else HBM for i in range(count)
        ],
        out_specs=(HBM,) * len(outs),
        scratch_shapes=[b for _, b in in_buffers]
        + [b for _, b in out_buffers]
        + list(scratch)
        + [
            pltpu.SemaphoreType.DMA((max(1, len(in_buffers)),)),
            pltpu.SemaphoreType.DMA((max(1, len(out_buffers)),)),
        ],
        compiler_params=pltpu.CompilerParams(vmem_limit_bytes=ROOM * MIB),
        cost_estimate=pl.CostEstimate(
            flops=int(flops), bytes_accessed=8 * MIB, transcendentals=0
        ),
    )(*placed)


def scale_lanes(scale_ref, block, width):
    head = lax.broadcasted_iota(jnp.int32, (1, width), 1) // (width // HEADS)
    row = jnp.zeros((1, width), F32)
    for h in range(HEADS):
        row = jnp.where(head == h, scale_ref[block, h], row)
    return row


def nn(a, b):
    return lax.dot_general(a, b, (((1,), (0,)), ((), ())), preferred_element_type=F32)


def nt(a, b):
    return lax.dot_general(a, b, (((1,), (1,)), ((), ())), preferred_element_type=F32)


def tn(a, b):
    return lax.dot_general(a, b, (((0,), (0,)), ((), ())), preferred_element_type=F32)


def norm_parts(h):
    mean = jnp.mean(h, -1, keepdims=True)
    centred = h - mean
    spread = jnp.mean(centred * centred, -1, keepdims=True)
    rstd = lax.rsqrt(spread + EPS)
    return centred * rstd, rstd


def norm(h, gain):
    return (norm_parts(h)[0] * gain).astype(BF)


def norm_back(h, gain, cotangent):
    xhat, rstd = norm_parts(h)
    scaled = cotangent * gain
    m1 = jnp.mean(scaled, -1, keepdims=True)
    m2 = jnp.mean(scaled * xhat, -1, keepdims=True)
    return rstd * (scaled - m1 - xhat * m2)


def gelu_parts(u):
    square = u * u
    t = jnp.tanh(u * (SQRT_2_OVER_PI + SQRT_2_OVER_PI * CUBIC * square))
    half = 0.5 + 0.5 * t
    value = u * half
    rate = 2.0 * SQRT_2_OVER_PI + 6.0 * SQRT_2_OVER_PI * CUBIC * square
    return value, half + value * (1.0 - half) * rate


def head_ones(width, size):
    a = lax.broadcasted_iota(jnp.int32, (width, width), 0) // size
    b = lax.broadcasted_iota(jnp.int32, (width, width), 1) // size
    return (a == b).astype(F32).astype(BF)


def head_stack(tokens, size):
    heads = LANES // size
    a = lax.broadcasted_iota(jnp.int32, (heads * tokens, LANES), 0) // tokens
    b = lax.broadcasted_iota(jnp.int32, (heads * tokens, LANES), 1) // size
    return (a == b).astype(F32).astype(BF)


def stacked(x, mask):
    copies = mask.shape[0] // x.shape[0]
    return [
        jnp.concatenate([x[:, t : t + LANES]] * copies, axis=0) * mask
        for t in range(0, x.shape[1], LANES)
    ]


def scores_of(x, blocks):
    return jnp.concatenate(
        [nt(x[:, t * LANES : (t + 1) * LANES], b) for t, b in enumerate(blocks)], axis=1
    )


def mix_of(p, blocks):
    rows = blocks[0].shape[0]
    return jnp.concatenate(
        [nn(p[:, t * rows : (t + 1) * rows], b) for t, b in enumerate(blocks)], axis=1
    )


def side_mask(window_row, threshold, tokens):
    shape = (tokens, HEADS * tokens)
    a = lax.broadcasted_iota(jnp.int32, shape, 0) // WIN
    b = (lax.broadcasted_iota(jnp.int32, shape, 1) % tokens) // WIN
    first = (window_row * WIN + a) >= threshold
    second = (window_row * WIN + b) >= threshold
    return jnp.where(first == second, 1.0, 0.0).astype(F32)


def window(ref, i, w):
    block = ref[i, :, w, :, :]
    return block.reshape(block.shape[0] * block.shape[1], block.shape[2])


def attention_chunk(qkv, scale, ones_ref, mask_ref, allowed, e_ref, o_ref, count, tokens):
    width = qkv.shape[1] // 3
    q = qkv[:, :width].astype(F32)
    k = qkv[:, width : 2 * width].astype(F32)
    v = qkv[:, 2 * width :]
    ones = ones_ref[...]
    qs = (q * lax.rsqrt(nn((q * q).astype(BF), ones) + 1.0) * scale).astype(BF)
    kn = (k * lax.rsqrt(nn((k * k).astype(BF), ones) + 1.0)).astype(BF)
    mask = mask_ref[...]
    for w in range(count):
        part = slice(w * tokens, (w + 1) * tokens)
        expo = jnp.exp(scores_of(qs[part], stacked(kn[part], mask)))
        if allowed is not None:
            expo = expo * allowed
        expo = expo.astype(BF)
        e_ref[part] = expo
        o_ref[part] = mix_of(expo, stacked(v[part], mask))
    total = mix_of(e_ref[...], [mask] * (width // LANES))
    return (o_ref[...] / total).astype(BF)


def attention_chunk_back(
    qkv, d_out, scale, ones_ref, mask_ref, allowed, dq_ref, dk_ref, dv_ref, count, tokens
):
    width = qkv.shape[1] // 3
    size = width // HEADS
    q = qkv[:, :width].astype(F32)
    k = qkv[:, width : 2 * width].astype(F32)
    v = qkv[:, 2 * width :]
    ones = ones_ref[...]
    rq = lax.rsqrt(nn((q * q).astype(BF), ones) + 1.0)
    rk = lax.rsqrt(nn((k * k).astype(BF), ones) + 1.0)
    qs = (q * rq * scale).astype(BF)
    kn = (k * rk).astype(BF)
    mask = mask_ref[...]
    lane_head = lax.broadcasted_iota(jnp.int32, (1, LANES), 1) // size
    per_tile = LANES // size
    for w in range(count):
        part = slice(w * tokens, (w + 1) * tokens)
        kw = kn[part]
        qm = stacked(qs[part], mask)
        dm = stacked(d_out[part], mask)
        expo = jnp.exp(scores_of(kw, qm))
        if allowed is not None:
            expo = expo * allowed
        p = expo * (1.0 / jnp.sum(expo, 0, keepdims=True))
        dp = scores_of(v[part], dm)
        ds = (p * (dp - jnp.sum(p * dp, 0, keepdims=True))).astype(BF)
        dv_ref[part] = mix_of(p.astype(BF), dm)
        dk_ref[part] = mix_of(ds, qm)
        tiles = []
        for tile in range(width // LANES):
            span = per_tile * tokens
            full = tn(
                ds[:, tile * span : (tile + 1) * span], kw[:, tile * LANES : (tile + 1) * LANES]
            )
            total = None
            for s in range(per_tile):
                block = full[s * tokens : (s + 1) * tokens]
                block = jnp.where(lane_head == s, block, 0.0)
                total = block if total is None else total + block
            tiles.append(total)
        dq_ref[part] = jnp.concatenate(tiles, axis=1)
    dqs = dq_ref[...]
    dkn = dk_ref[...]
    dq = scale * rq * (dqs - q * (rq * rq) * nn((q * dqs).astype(BF), ones))
    dk = rk * (dkn - k * (rk * rk) * nn((k * dkn).astype(BF), ones))
    return jnp.concatenate([dq.astype(BF), dk.astype(BF), dv_ref[...].astype(BF)], axis=1)


def split(cap):
    first = cap // 2
    return (first, cap - first), min(16, first)


def route_kernel(
    parts, stage, count_ref, owner_ref, point_ref, r_ref, w2_ref, values_ref,
    send1_ref, send2_ref, mixed_ref, y_ref, buf_ref, tgt_ref, tgt_smem, sem,
):
    cap = sum(parts)
    slots = owner_ref.shape[1]
    devices = send1_ref.shape[0]
    stage.need(owner_ref, point_ref)
    owner = owner_ref[...]
    live = lax.broadcasted_iota(jnp.int32, (1, slots), 1) < count_ref[0]
    match = lax.broadcasted_iota(jnp.int32, (devices, slots), 0) == owner
    match = jnp.where(match, 1.0, 0.0).astype(F32)
    a = lax.broadcasted_iota(jnp.int32, (LANES, LANES), 0)
    b = lax.broadcasted_iota(jnp.int32, (LANES, LANES), 1)
    upper = jnp.where(a < b, 1.0, 0.0).astype(BF)
    chunks = slots // LANES
    flat = jnp.concatenate(
        [match[:, c * LANES : (c + 1) * LANES] for c in range(chunks)], axis=0
    )
    before = nn(flat.astype(BF), upper)
    carry = jnp.zeros((devices, 1), F32)
    ranks = []
    dump = devices * cap
    for c in range(chunks):
        here = match[:, c * LANES : (c + 1) * LANES]
        seen = before[c * devices : (c + 1) * devices] + carry
        ranks.append(jnp.sum(here * seen, 0, keepdims=True))
        span = slice(c * LANES, (c + 1) * LANES)
        spot = owner[:, span] * cap + ranks[-1].astype(jnp.int32)
        tgt_ref[c : c + 1, :] = jnp.where(live[:, span], spot, dump)
        carry = carry + jnp.sum(here, 1, keepdims=True)
    rank = jnp.concatenate(ranks, axis=1).astype(jnp.int32)
    copy = pltpu.make_async_copy(tgt_ref, tgt_smem, sem)
    copy.start()
    place = lax.broadcasted_iota(jnp.int32, (cap, slots), 0) == rank
    place = jnp.where(place & live, 1.0, 0.0).astype(BF)
    point = point_ref[...]
    high = (match * (point // LANES + 1).astype(F32)).astype(BF)
    low = (match * (point % LANES).astype(F32)).astype(BF)
    high = nt(high, place)
    low = nt(low, place)
    stage.need(r_ref, w2_ref, values_ref)
    best = lax.Precision.HIGHEST
    dims = (((1,), (1,)), ((), ()))
    m2 = lax.dot_general(
        r_ref[...], w2_ref[...], dims, precision=best, preferred_element_type=F32
    )
    mixed_ref[...] = jnp.dot(
        w2_ref[...], m2, precision=best, preferred_element_type=F32
    ).astype(BF)
    y = nn(values_ref[...].astype(BF), m2.astype(BF))
    y_ref[0, :, :] = y[:, :LANES]
    y_ref[1, :, :] = y[:, LANES:]
    buf_ref[...] = jnp.zeros_like(buf_ref)
    copy.wait()
    unroll = 16

    def move(c, _):
        base = pl.multiple_of(c * LANES, LANES)
        for start in range(0, LANES, unroll):
            spots = [tgt_smem[c, start + u] for u in range(unroll)]
            for half in range(2):
                for u in range(unroll):
                    buf_ref[half, pl.ds(spots[u], 1), :] = y_ref[
                        half, pl.ds(base + start + u, 1), :
                    ]
        return 0

    lax.fori_loop(0, chunks, move, 0)
    fill = ((0, 0), (0, LANES - cap))
    codes = jnp.concatenate([jnp.pad(high, fill), jnp.pad(low, fill)], axis=1)
    stage.emit(mixed_ref)
    for d in range(devices):
        offset = d * cap
        for ref, size in zip((send1_ref, send2_ref), parts):
            for half in range(2):
                ref[d, 0:size, half * LANES : (half + 1) * LANES] = buf_ref[
                    half, offset : offset + size, :
                ].astype(BF)
            offset += size
        send1_ref[d, parts[0] : parts[0] + EXTRA, :] = jnp.broadcast_to(
            codes[d : d + 1], (EXTRA, 2 * LANES)
        ).astype(BF)
        if (d + 1) % 8 == 0:
            stage.emit_part(pl.ds(d - 7, 8), send1_ref, send2_ref)


def route(owner, point, count, values, r_inverse, w2, devices, parts):
    slots, channels = values.shape
    cap = sum(parts)
    sizes = (parts[0] + EXTRA,) + tuple(parts[1:])
    return staged(
        functools.partial(route_kernel, parts),
        (count, owner, point, r_inverse, w2, values),
        tuple(jax.ShapeDtypeStruct((devices, n, channels), BF) for n in sizes)
        + (jax.ShapeDtypeStruct(w2.shape, BF),),
        [
            pltpu.VMEM((2, slots, LANES), F32),
            pltpu.VMEM((2, devices * cap + EXTRA, LANES), F32),
            pltpu.VMEM((slots // LANES, LANES), jnp.int32),
            pltpu.SMEM((slots // LANES, LANES), jnp.int32),
            pltpu.SemaphoreType.DMA,
        ],
        1e9,
        smem=(0,),
    )


def load_state(ins, extra):
    source, target, sems = ins[2], extra[0], extra[-1]
    for i in range(source.shape[0]):
        pltpu.make_async_copy(source.at[i], target.at[i], sems.at[i]).start()


def first_kernel(
    stage, scale_ref, order_ref, state_hbm, we_ref, gain_ref, wqkv_ref, wproj_ref, wup_ref, wdown_ref,
    top_ref, left_ref, corner_ref, z1_ref, h1_ref, h0_ref, hm_ref, qkv_ref, gp_ref,
    state_ref, ones_ref, mask_ref, e_ref, o_ref, sems,
):
    rows, _, cols, _, _ = state_ref.shape
    width = we_ref.shape[1]
    tokens = WIN * WIN
    chunk = cols * tokens

    def load(i):
        return pltpu.make_async_copy(state_hbm.at[i], state_ref.at[i], sems.at[i])

    ones_ref[...] = head_ones(width, width // HEADS)
    mask_ref[...] = head_stack(tokens, width // HEADS)
    scale = scale_lanes(scale_ref, 0, width)
    stage.need(we_ref, gain_ref)

    def body(i, _):
        load(i).wait()
        x = jnp.concatenate([window(state_ref, i, w).astype(BF) for w in range(cols)], axis=0)
        h0 = nn(x, we_ref[...])
        here = pl.ds(pl.multiple_of(i * chunk, chunk), chunk)
        h0_ref[here, :] = h0
        stage.emit_part(here, h0_ref)
        stage.need_at(i == 0, wqkv_ref)
        qkv = nn(norm(h0, gain_ref[0, 0:1]), wqkv_ref[...]).astype(BF)
        qkv_ref[here, :] = qkv
        stage.emit_part(here, qkv_ref)
        mixed = attention_chunk(qkv, scale, ones_ref, mask_ref, None, e_ref, o_ref, cols, tokens)
        stage.need_at(i == 0, wproj_ref, wup_ref, wdown_ref)
        hm = h0 + nn(mixed, wproj_ref[...]).astype(BF).astype(F32)
        hm_ref[here, :] = hm
        stage.emit_part(here, hm_ref)
        inner, slope = gelu_parts(nn(norm(hm, gain_ref[0, 1:2]), wup_ref[...]))
        gp_ref[here, :] = slope.astype(BF)
        stage.emit_part(here, gp_ref)
        h1 = hm + nn(inner.astype(BF), wdown_ref[...])
        z1 = norm(h1, gain_ref[1, 0:1]).astype(F32)
        for w in range(cols):
            part = slice(w * tokens, (w + 1) * tokens)
            h1_ref[i, :, w, :, :] = h1[part].reshape(WIN, WIN, width)
            z1_ref[i, :, w, :, :] = z1[part].reshape(WIN, WIN, width)
        stage.emit_part(i, z1_ref, h1_ref)
        return 0

    lax.fori_loop(0, rows, body, 0)
    top_ref[...] = z1_ref[0, 0:SHIFT, :, :, :].astype(BF)
    left_ref[...] = z1_ref[:, :, 0, 0:SHIFT, :].astype(BF)
    corner_ref[...] = z1_ref[0, 0:SHIFT, 0, 0:SHIFT, :].astype(BF)


def first_block(order, state5, we, gains, wqkv, wproj, scale, wup, wdown):
    wr, _, wc, _, _ = state5.shape
    width = we.shape[1]
    tokens = wr * wc * WIN * WIN
    chunk = wc * WIN * WIN
    sh = jax.ShapeDtypeStruct
    outs = (
        sh((SHIFT, wc, WIN, width), BF),
        sh((wr, WIN, SHIFT, width), BF),
        sh((SHIFT, SHIFT, width), BF),
        sh((wr, WIN, wc, WIN, width), F32),
        sh((wr, WIN, wc, WIN, width), F32),
        sh((tokens, width), F32),
        sh((tokens, width), F32),
        sh((tokens, 3 * width), BF),
        sh((tokens, wup.shape[2]), BF),
    )
    return staged(
        first_kernel,
        (scale, order, state5, we, gains, wqkv, wproj, wup, wdown),
        outs,
        [
            pltpu.VMEM(state5.shape, F32),
            pltpu.VMEM((width, width), BF),
            pltpu.VMEM((LANES * HEADS // width * WIN * WIN, LANES), BF),
            pltpu.VMEM((chunk, HEADS * WIN * WIN), BF),
            pltpu.VMEM((chunk, width), F32),
            pltpu.SemaphoreType.DMA((wr,)),
        ],
        2e9,
        smem=(0,),
        raw=(1, 2),
        early=load_state,
        layer={5: 0, 6: 0, 7: 0, 8: 0},
    )


def fill_ahead(pad_ref, own, right_ref, below_ref, corner_ref):
    rows, cols, _ = own.shape
    pad_ref[0:rows, 0:cols, :] = own
    pad_ref[0:rows, cols : cols + SHIFT, :] = right_ref[...].astype(F32)
    pad_ref[rows : rows + SHIFT, 0:cols, :] = below_ref[...].astype(F32)
    pad_ref[rows : rows + SHIFT, cols : cols + SHIFT, :] = corner_ref[...].astype(F32)


def rolled_window(pad_ref, i, w):
    block = pad_ref[
        pl.ds(i * WIN + SHIFT, WIN), SHIFT + w * WIN : SHIFT + (w + 1) * WIN, :
    ]
    return block.reshape(WIN * WIN, block.shape[2])


def emit_behind(out_ref, low_ref, east_ref, corner_ref):
    rows, cols, _ = out_ref.shape
    low_ref[...] = out_ref[rows - SHIFT : rows, :, :].astype(BF)
    east_ref[...] = out_ref[:, cols - SHIFT : cols, :].astype(BF)
    corner_ref[...] = out_ref[rows - SHIFT : rows, cols - SHIFT : cols, :].astype(BF)


def shifted_kernel(
    total_rows, stage, start_ref, scale_ref, z1_ref, right_ref, below_ref, corner_ref, wqkv_ref,
    wproj_ref, ans_ref, low_ref, east_ref, last_ref, qkv_ref,
    pad_ref, ones_ref, mask_ref, e_ref, o_ref,
):
    rows, cols, width = z1_ref.shape
    wr, wc = rows // WIN, cols // WIN
    tokens = WIN * WIN
    chunk = wc * tokens
    ones_ref[...] = head_ones(width, width // HEADS)
    mask_ref[...] = head_stack(tokens, width // HEADS)
    scale = scale_lanes(scale_ref, 1, width)
    stage.need(z1_ref, right_ref, below_ref, corner_ref)
    fill_ahead(pad_ref, z1_ref[...], right_ref, below_ref, corner_ref)
    threshold = total_rows - SHIFT - start_ref[0]

    def body(i, _):
        z = jnp.concatenate([rolled_window(pad_ref, i, w).astype(BF) for w in range(wc)], axis=0)
        stage.need_at(i == 0, wqkv_ref, wproj_ref)
        qkv = nn(z, wqkv_ref[...]).astype(BF)
        here = pl.ds(pl.multiple_of(i * chunk, chunk), chunk)
        qkv_ref[here, :] = qkv
        stage.emit_part(here, qkv_ref)
        allowed = side_mask(i, threshold, tokens)
        mixed = attention_chunk(qkv, scale, ones_ref, mask_ref, allowed, e_ref, o_ref, wc, tokens)
        answer = nn(mixed, wproj_ref[...]).astype(BF).astype(F32)
        for w in range(wc):
            ans_ref[pl.ds(i * WIN, WIN), w * WIN : (w + 1) * WIN, :] = answer[
                w * tokens : (w + 1) * tokens
            ].reshape(WIN, WIN, width)
        stage.emit_part(pl.ds(i * WIN, WIN), ans_ref)
        return 0

    lax.fori_loop(0, wr, body, 0)
    emit_behind(ans_ref, low_ref, east_ref, last_ref)


def behind_shapes(rows, cols, width):
    sh = jax.ShapeDtypeStruct
    return (
        sh((rows, cols, width), F32),
        sh((SHIFT, cols, width), BF),
        sh((rows, SHIFT, width), BF),
        sh((SHIFT, SHIFT, width), BF),
    )


def shifted_forward(start, z1, right, below, corner, wqkv, wproj, scale, total_rows):
    rows, cols, width = z1.shape
    tokens = rows * cols
    chunk = cols * WIN
    outs = behind_shapes(rows, cols, width) + (jax.ShapeDtypeStruct((tokens, 3 * width), BF),)
    return staged(
        functools.partial(shifted_kernel, total_rows),
        (start, scale, z1, right, below, corner, wqkv, wproj),
        outs,
        [
            pltpu.VMEM((rows + SHIFT, cols + WIN, width), F32),
            pltpu.VMEM((width, width), BF),
            pltpu.VMEM((LANES * HEADS // width * WIN * WIN, LANES), BF),
            pltpu.VMEM((chunk, HEADS * WIN * WIN), BF),
            pltpu.VMEM((chunk, width), F32),
        ],
        1e9,
        smem=(0, 1),
        vmem=(3, 4, 5),
        layer={6: 1, 7: 1},
    )


def fill_behind(pad_ref, own, above_ref, west_ref, corner_ref):
    rows, cols, _ = own.shape
    pad_ref[SHIFT : SHIFT + rows, SHIFT : SHIFT + cols, :] = own
    pad_ref[0:SHIFT, SHIFT : SHIFT + cols, :] = above_ref[...].astype(F32)
    pad_ref[SHIFT : SHIFT + rows, 0:SHIFT, :] = west_ref[...].astype(F32)
    pad_ref[0:SHIFT, 0:SHIFT, :] = corner_ref[...].astype(F32)


def group_jobs(cnt_smem, offset, size, group, body):
    devices = cnt_smem.shape[0]

    def each(d, _):
        valid = cnt_smem[d, 0] - offset
        for g in range(0, size, group):

            @pl.when(valid > g)
            def _():
                body(d, offset + g, pl.multiple_of(d * size + g, group))

        return 0

    lax.fori_loop(0, devices, each, 0)


def gather_part(table_ref, found_ref, idx_smem, cnt_smem, offset, size, group):
    def body(d, slot, row):
        for u in range(group):
            found_ref[pl.ds(row + u, 1), :] = table_ref[pl.ds(idx_smem[d, slot + u], 1), :]

    group_jobs(cnt_smem, offset, size, group, body)


def scatter_part(table_ref, found_ref, idx_smem, cnt_smem, dup_smem, offset, size, group):
    def body(d, slot, row):
        @pl.when(dup_smem[d, slot] == 0)
        def _():
            spots = [idx_smem[d, slot + u] for u in range(group)]
            sums = [
                table_ref[pl.ds(spots[u], 1), :] + found_ref[pl.ds(row + u, 1), :]
                for u in range(group)
            ]
            for u in range(group):
                table_ref[pl.ds(spots[u], 1), :] = sums[u]

        @pl.when(dup_smem[d, slot] != 0)
        def _():
            def one(u, _):
                spot = pl.ds(idx_smem[d, slot + u], 1)
                table_ref[spot, :] = table_ref[spot, :] + found_ref[pl.ds(row + u, 1), :]
                return 0

            lax.fori_loop(0, group, one, 0)

    group_jobs(cnt_smem, offset, size, group, body)


def radiance_part(found_ref, obs_ref, mixed_ref, w1_ref, size):
    devices, _, channels = obs_ref.shape
    batch = min(devices, max(1, 512 // size))

    def body(i, _):
        here = pl.ds(pl.multiple_of(i * batch * size, batch * size), batch * size)
        y = obs_ref[pl.ds(i * batch, batch), 0:size, :].astype(F32)
        y = y.reshape(batch * size, channels)
        t = jnp.tanh(nn(found_ref[here, :].astype(BF), w1_ref[...].astype(BF)))
        pulled = (nn(t.astype(BF), mixed_ref[...]) - y) * (1.0 - t * t)
        found_ref[here, :] = nt(pulled.astype(BF), w1_ref[...].astype(BF))
        return 0

    lax.fori_loop(0, devices // batch, body, 0)


def spread(table_ref, moved_ref, i, step, tokens):
    for s in range(PIX):
        there = pl.ds(pl.multiple_of(s * tokens + i * step, WIN), step)
        moved_ref[:, s * VARS : (s + 1) * VARS] = table_ref[there, 0:VARS]


def forecast_kernel(
    parts, group, stage, obs1_ref, h1_ref, ans_ref, above_ref, west_ref, corner_ref, gain_ref,
    wup_ref, wdown_ref, whead_ref, state_ref, w1_in_ref, mixed_ref, back_ref, inv_ref,
    h2_ref, gp_ref, prior_ref, found2_ref, idx_ref, cnt_ref, dup_ref, pulled_ref, w1_ref,
    pad_ref, table_ref, moved_ref, found1_ref, idx_smem, cnt_smem, dup_smem, sems,
):
    rows, cols, width = h1_ref.shape
    devices = obs1_ref.shape[0]
    tokens = rows * cols
    step = tokens // 2

    stage.need(obs1_ref)
    codes = obs1_ref[:, parts[0] : parts[0] + EXTRA, :].astype(F32)[:, 0, :]
    high = codes[:, :LANES].astype(jnp.int32)
    low = codes[:, LANES : 2 * LANES].astype(jnp.int32)
    point = jnp.where(high > 0, (high - 1) * LANES + low, 0)
    lane = lax.broadcasted_iota(jnp.int32, (devices, LANES), 1)
    idx = jnp.where(
        high > 0, (point % PIX) * tokens + point // PIX, PIX * tokens + lane % group
    )
    idx_ref[...] = idx
    cnt_ref[...] = jnp.broadcast_to(
        jnp.sum(jnp.where(high > 0, 1.0, 0.0), 1, keepdims=True), (devices, LANES)
    ).astype(jnp.int32)
    same = jnp.zeros((devices, LANES), jnp.int32)
    for s in range(1, group):
        hit = (pltpu.roll(idx, s, 1) == idx) & (lane % group >= s)
        same = jnp.maximum(same, jnp.where(hit, 1, 0))
    s = group // 2
    while s:
        same = jnp.maximum(same, pltpu.roll(same, LANES - s, 1))
        s //= 2
    dup_ref[...] = same
    copies = [
        pltpu.make_async_copy(a, b, sems.at[n])
        for n, (a, b) in enumerate(
            ((idx_ref, idx_smem), (cnt_ref, cnt_smem), (dup_ref, dup_smem))
        )
    ]
    for copy in copies:
        copy.start()
    stage.need(h1_ref, ans_ref, above_ref, west_ref, corner_ref)
    fill_behind(pad_ref, ans_ref[...], above_ref, west_ref, corner_ref)
    h2_ref[...] = (h1_ref[...] + pad_ref[0:rows, 0:cols, :]).reshape(tokens, width)
    table_ref[PIX * tokens :, :] = jnp.zeros((group, LANES), F32)
    blank = jnp.zeros((step, LANES - VARS), F32)
    stage.need(gain_ref, wup_ref, wdown_ref)

    def forward(i, _):
        here = pl.ds(pl.multiple_of(i * step, step), step)
        h2 = h2_ref[here, :]
        inner, slope = gelu_parts(nn(norm(h2, gain_ref[1, 1:2]), wup_ref[...]))
        gp_ref[here, :] = slope.astype(BF)
        h3 = (h2 + nn(inner.astype(BF), wdown_ref[...])).astype(BF)
        stage.need_at(i == 0, whead_ref, state_ref)
        moved = state_ref[here, :] + nt(h3, whead_ref[...])
        for s in range(PIX):
            there = pl.ds(pl.multiple_of(s * tokens + i * step, WIN), step)
            table_ref[there, :] = jnp.concatenate(
                [moved[:, s * VARS : (s + 1) * VARS], blank], axis=1
            )
        return 0

    lax.fori_loop(0, 2, forward, 0)
    stage.emit(h2_ref, gp_ref, idx_ref, cnt_ref, dup_ref)
    stage.need(back_ref, inv_ref, w1_in_ref, mixed_ref)
    w1_ref[...] = jnp.zeros_like(w1_ref)
    w1_ref[0:VARS, :] = w1_in_ref[...]
    w1_ref[...] = w1_ref[...].astype(BF).astype(F32)
    for copy in copies:
        copy.wait()
    offsets = (0, parts[0])
    founds = (found1_ref, found2_ref)
    for offset, size, found in zip(offsets, parts, founds):
        gather_part(table_ref, found, idx_smem, cnt_smem, offset, size, group)
    stage.emit(found2_ref)
    table_ref[...] = jnp.zeros_like(table_ref)
    radiance_part(found1_ref, obs1_ref, mixed_ref, w1_ref, parts[0])
    scatter_part(table_ref, found1_ref, idx_smem, cnt_smem, dup_smem, 0, parts[0], group)

    def collect(i, _):
        here = pl.ds(pl.multiple_of(i * step, step), step)
        spread(table_ref, moved_ref, i, step, tokens)
        moved = moved_ref[...]
        prior_ref[here, :] = moved + inv_ref[...].reshape(1, -1) * (state_ref[here, :] - back_ref[here, :])
        stage.emit_part(here, prior_ref)
        pulled_ref[here, :] = nn(moved.astype(BF), whead_ref[...])
        stage.emit_part(here, pulled_ref)
        return 0

    lax.fori_loop(0, 2, collect, 0)


def forecast(
    h1, ans, above, west, corner, state, background, inv, obs1, mixed, gains, wup, wdown, whead,
    w1, parts, group,
):
    rows, cols, width = h1.shape
    tokens = rows * cols
    devices = obs1.shape[0]
    sh = jax.ShapeDtypeStruct
    outs = (
        sh((tokens, width), F32),
        sh((tokens, wup.shape[2]), BF),
        sh(state.shape, F32),
        sh((devices * parts[1], LANES), F32),
        sh((devices, LANES), jnp.int32),
        sh((devices, LANES), jnp.int32),
        sh((devices, LANES), jnp.int32),
        sh((tokens, width), F32),
        sh((LANES, w1.shape[1]), F32),
    )
    return staged(
        functools.partial(forecast_kernel, parts, group),
        (
            obs1, h1, ans, above, west, corner, gains, wup, wdown, whead, state, w1, mixed,
            background, inv,
        ),
        outs,
        [
            pltpu.VMEM((rows + SHIFT, cols + WIN, width), F32),
            pltpu.VMEM((PIX * tokens + group, LANES), F32),
            pltpu.VMEM((tokens // 2, state.shape[1]), F32),
            pltpu.VMEM((devices * parts[0], LANES), F32),
        ]
        + [pltpu.SMEM((devices, LANES), jnp.int32)] * 3
        + [pltpu.SemaphoreType.DMA((3,))],
        3e9,
        vmem=(0, 3, 4, 5),
        layer={7: 1, 8: 1},
    )


def adjoint_kernel(
    parts, group, stage, idx_smem, cnt_smem, dup_smem, w1_ref, mixed_ref, work_ref, obs2_ref,
    whead_ref, pulled_ref, prior_ref, wdown_ref, gp_ref, wup_ref, h2_ref, gain_ref,
    top_ref, left_ref, edge_ref, third_ref, out_ref, table_ref, moved_ref,
):
    rows, cols, width = third_ref.shape
    tokens = rows * cols
    step = tokens // 2
    table_ref[...] = jnp.zeros_like(table_ref)
    stage.need(idx_smem, cnt_smem, dup_smem, w1_ref, mixed_ref, work_ref, obs2_ref)
    radiance_part(work_ref, obs2_ref, mixed_ref, w1_ref, parts[1])
    scatter_part(
        table_ref, work_ref, idx_smem, cnt_smem, dup_smem, parts[0], parts[1], group
    )
    stage.need(whead_ref, pulled_ref, prior_ref, wdown_ref, gp_ref, wup_ref, h2_ref, gain_ref)
    half = rows // 2

    def backward(i, _):
        here = pl.ds(pl.multiple_of(i * step, step), step)
        spread(table_ref, moved_ref, i, step, tokens)
        moved = moved_ref[...]
        out_ref[here, :] = moved + prior_ref[here, :]
        stage.emit_part(here, out_ref)
        grad = (pulled_ref[here, :] + nn(moved.astype(BF), whead_ref[...])).astype(BF)
        d_inner = nt(grad, wdown_ref[...]) * gp_ref[here, :].astype(F32)
        d_normed = nt(d_inner.astype(BF), wup_ref[...])
        third = grad.astype(F32) + norm_back(h2_ref[here, :], gain_ref[1, 1:2], d_normed)
        third_ref[pl.ds(i * half, half), :, :] = third.reshape(half, cols, width)
        stage.emit_part(pl.ds(i * half, half), third_ref)
        return 0

    lax.fori_loop(0, 2, backward, 0)
    top_ref[...] = third_ref[0:SHIFT, :, :].astype(BF)
    left_ref[...] = third_ref[:, 0:SHIFT, :].astype(BF)
    edge_ref[...] = third_ref[0:SHIFT, 0:SHIFT, :].astype(BF)


def adjoint(
    idx, cnt, dup, found, obs2, mixed, w1, h2, gp, gains, wup, wdown, whead, prior, pulled, parts,
    group, rows, cols,
):
    width = h2.shape[1]
    third, top, left, edge = behind_shapes(rows, cols, width)
    outs = (top, left, edge, third, jax.ShapeDtypeStruct(prior.shape, F32))
    return staged(
        functools.partial(adjoint_kernel, parts, group),
        (idx, cnt, dup, w1, mixed, found, obs2, whead, pulled, prior, wdown, gp, wup, h2, gains),
        outs,
        [
            pltpu.VMEM((PIX * rows * cols + group, LANES), F32),
            pltpu.VMEM((prior.shape[0] // 2, prior.shape[1]), F32),
        ],
        2e9,
        scalars=(0, 1, 2),
        vmem=(6,),
        layer={10: 1, 12: 1},
    )


def shifted_back_kernel(
    total_rows, stage, start_ref, scale_ref, third_ref, right_ref, below_ref, corner_ref,
    wproj_ref, qkv_ref, wqkv_ref, dz_ref, low_ref, east_ref, last_ref,
    pad_ref, ones_ref, mask_ref, dq_ref, dk_ref, dv_ref,
):
    rows, cols, width = third_ref.shape
    wr, wc = rows // WIN, cols // WIN
    tokens = WIN * WIN
    chunk = wc * tokens
    ones_ref[...] = head_ones(width, width // HEADS)
    mask_ref[...] = head_stack(tokens, width // HEADS)
    scale = scale_lanes(scale_ref, 1, width)
    stage.need(third_ref, right_ref, below_ref, corner_ref)
    fill_ahead(pad_ref, third_ref[...], right_ref, below_ref, corner_ref)
    threshold = total_rows - SHIFT - start_ref[0]

    def body(i, _):
        d_answer = jnp.concatenate(
            [rolled_window(pad_ref, i, w).astype(BF) for w in range(wc)], axis=0
        )
        stage.need_at(i == 0, wproj_ref, qkv_ref, wqkv_ref)
        d_out = nt(d_answer, wproj_ref[...]).astype(BF)
        allowed = side_mask(i, threshold, tokens)
        qkv = qkv_ref[pl.ds(pl.multiple_of(i * chunk, chunk), chunk), :]
        d_qkv = attention_chunk_back(
            qkv, d_out, scale, ones_ref, mask_ref, allowed,
            dq_ref, dk_ref, dv_ref, wc, tokens,
        )
        dz = nt(d_qkv, wqkv_ref[...]).astype(BF).astype(F32)
        for w in range(wc):
            dz_ref[pl.ds(i * WIN, WIN), w * WIN : (w + 1) * WIN, :] = dz[
                w * tokens : (w + 1) * tokens
            ].reshape(WIN, WIN, width)
        stage.emit_part(pl.ds(i * WIN, WIN), dz_ref)
        return 0

    lax.fori_loop(0, wr, body, 0)
    emit_behind(dz_ref, low_ref, east_ref, last_ref)


def shifted_backward(start, third, right, below, corner, qkv, wqkv, wproj, scale, total_rows):
    rows, cols, width = third.shape
    chunk = cols * WIN
    outs = behind_shapes(rows, cols, width)
    return staged(
        functools.partial(shifted_back_kernel, total_rows),
        (start, scale, third, right, below, corner, wproj, qkv, wqkv),
        outs,
        [
            pltpu.VMEM((rows + SHIFT, cols + WIN, width), F32),
            pltpu.VMEM((width, width), BF),
            pltpu.VMEM((LANES * HEADS // width * WIN * WIN, LANES), BF),
        ]
        + [pltpu.VMEM((chunk, width), F32)] * 3,
        1e9,
        smem=(0, 1),
        vmem=(3, 4, 5, 6, 7, 8),
        layer={6: 1, 8: 1},
    )


def last_kernel(
    stage, scale_ref, partial_hbm, dz_ref, above_ref, west_ref, corner_ref, third_ref, h1_ref,
    gain_ref, wdown_ref, gp_ref, wup_ref, hm_ref, wproj_ref, qkv_ref, wqkv_ref, h0_ref, we_ref,
    out_hbm,
    pad_ref, ones_ref, mask_ref, dq_ref, dk_ref, dv_ref, out_ref, in_sems, out_sems,
):
    rows, cols, width = dz_ref.shape
    wr, wc = rows // WIN, cols // WIN
    tokens = WIN * WIN
    chunk = wc * tokens

    def rows_of(ref, i):
        return ref.at[pl.ds(i * WIN, WIN)]

    ones_ref[...] = head_ones(width, width // HEADS)
    mask_ref[...] = head_stack(tokens, width // HEADS)
    scale = scale_lanes(scale_ref, 0, width)
    for i in range(wr):
        pltpu.make_async_copy(rows_of(partial_hbm, i), rows_of(out_ref, i), in_sems.at[i]).start()
    stage.need(dz_ref, above_ref, west_ref, corner_ref)
    fill_behind(pad_ref, dz_ref[...], above_ref, west_ref, corner_ref)

    def body(i, _):
        here = pl.ds(pl.multiple_of(i * chunk, chunk), chunk)
        band = pl.ds(i * WIN, WIN)

        def take(ref):
            return jnp.concatenate(
                [
                    ref[band, w * WIN : (w + 1) * WIN, :].reshape(tokens, width)
                    for w in range(wc)
                ],
                axis=0,
            )

        stage.need_at(i == 0, third_ref, h1_ref, gain_ref, wdown_ref, gp_ref, wup_ref)
        second = take(third_ref) + norm_back(take(h1_ref), gain_ref[1, 0:1], take(pad_ref))
        d_inner = nt(second.astype(BF), wdown_ref[...]) * gp_ref[here, :].astype(F32)
        d_normed = nt(d_inner.astype(BF), wup_ref[...])
        stage.need_at(i == 0, hm_ref, wproj_ref, qkv_ref, wqkv_ref, h0_ref, we_ref)
        d_hm = second + norm_back(hm_ref[here, :], gain_ref[0, 1:2], d_normed)
        d_out = nt(d_hm.astype(BF), wproj_ref[...]).astype(BF)
        d_qkv = attention_chunk_back(
            qkv_ref[here, :], d_out, scale, ones_ref, mask_ref, None,
            dq_ref, dk_ref, dv_ref, wc, tokens,
        )
        dz = nt(d_qkv, wqkv_ref[...])
        d_h0 = (d_hm + norm_back(h0_ref[here, :], gain_ref[0, 0:1], dz)).astype(BF)
        pltpu.make_async_copy(rows_of(partial_hbm, i), rows_of(out_ref, i), in_sems.at[i]).wait()
        for w in range(wc):
            grad = nt(d_h0[w * tokens : (w + 1) * tokens], we_ref[...])
            grad = grad.reshape(WIN, WIN, grad.shape[1])
            spot = (band, slice(w * WIN, (w + 1) * WIN), slice(None))
            out_ref[spot] = grad + out_ref[spot]
        pltpu.make_async_copy(rows_of(out_ref, i), rows_of(out_hbm, i), out_sems.at[i]).start()
        return 0

    lax.fori_loop(0, wr, body, 0)
    for i in range(wr):
        pltpu.make_async_copy(rows_of(out_ref, i), rows_of(out_hbm, i), out_sems.at[i]).wait()


def last_block(
    third, dz, above, west, corner, h1, h0, hm, qkv, gp, we, gains, wqkv, wproj, scale,
    wup, wdown, partial,
):
    rows, cols, width = dz.shape
    chunk = cols * WIN
    (result,) = staged(
        last_kernel,
        (
            scale, partial, dz, above, west, corner, third, h1, gains, wdown, gp, wup, hm, wproj,
            qkv, wqkv, h0, we,
        ),
        (jax.ShapeDtypeStruct(partial.shape, F32),),
        [
            pltpu.VMEM((rows + SHIFT, cols + WIN, width), F32),
            pltpu.VMEM((width, width), BF),
            pltpu.VMEM((LANES * HEADS // width * WIN * WIN, LANES), BF),
        ]
        + [pltpu.VMEM((chunk, width), F32)] * 3
        + [
            pltpu.VMEM(partial.shape, F32),
            pltpu.SemaphoreType.DMA((rows // WIN,)),
            pltpu.SemaphoreType.DMA((rows // WIN,)),
        ],
        2e9,
        smem=(0,),
        raw=(1,),
        raw_outs=(0,),
        vmem=(3, 4, 5, 7, 8, 9, 10, 11, 12, 13, 14, 15, 16, 17),
        layer={9: 0, 11: 0, 13: 0, 15: 0},
    )
    return result


def neighbour(x, by_lat, by_lon):
    lat, lon = lax.axis_size("lat"), lax.axis_size("lon")
    pairs = [
        (a * lon + b, ((a + by_lat) % lat) * lon + (b + by_lon) % lon)
        for a in range(lat)
        for b in range(lon)
    ]
    return lax.ppermute(x, ("lat", "lon"), pairs)


def exchange(x):
    return lax.all_to_all(x, ("lat", "lon"), split_axis=0, concat_axis=0, tiled=True)


def local(
    state,
    background,
    inv_background,
    w_embed,
    norm_gain,
    w_qkv,
    w_proj,
    head_scale,
    w_up,
    w_down,
    w_head,
    w_obs1,
    w_obs2,
    r_inverse,
    obs_values,
    obs_owner,
    obs_point,
    obs_count,
):
    rows, cols, patch_values = state.shape
    width = w_embed.shape[1]
    total_rows = rows * lax.axis_size("lat")
    row_start = (lax.axis_index("lat") * rows).astype(jnp.int32).reshape(1)
    devices = lax.axis_size("lat") * lax.axis_size("lon")
    slots = obs_values.shape[0]
    cap = 2 * slots // devices

    parts, group = split(cap)

    send1, send2, mixed = route(
        obs_owner.reshape(1, slots), obs_point.reshape(1, slots), obs_count, obs_values,
        r_inverse, w_obs2, devices, parts,
    )
    obs1 = exchange(send1)
    state5 = state.reshape(rows // WIN, WIN, cols // WIN, WIN, patch_values)
    top, left, corner, z1, h1, h0, hm, qkv0, gp0 = first_block(
        mixed, state5, w_embed, norm_gain, w_qkv, w_proj, head_scale, w_up, w_down
    )
    z1 = z1.reshape(rows, cols, width)
    h1 = h1.reshape(rows, cols, width)
    below = neighbour(top.reshape(SHIFT, cols, width), -1, 0)
    right = neighbour(left.reshape(rows, SHIFT, width), 0, -1)
    corner = neighbour(corner, -1, -1)
    answer, low, east, last, qkv1 = shifted_forward(
        row_start, z1, right, below, corner, w_qkv, w_proj, head_scale, total_rows
    )
    above = neighbour(low, 1, 0)
    west = neighbour(east, 0, 1)
    last = neighbour(last, 1, 1)
    obs1, send2 = lax.optimization_barrier((obs1, send2))
    obs2 = exchange(send2)
    flat = (rows * cols, patch_values)
    h2, gp1, prior, found, idx, cnt, dup, pulled, w1 = forecast(
        h1, answer, above, west, last, state.reshape(flat), background.reshape(flat),
        inv_background, obs1, mixed, norm_gain, w_up, w_down, w_head.T,
        w_obs1, parts, group,
    )
    top, left, corner, third, partial = adjoint(
        idx, cnt, dup, found, obs2, mixed, w1, h2, gp1, norm_gain, w_up, w_down, w_head.T, prior,
        pulled,
        parts, group, rows, cols,
    )
    below = neighbour(top, -1, 0)
    right = neighbour(left, 0, -1)
    corner = neighbour(corner, -1, -1)
    dz, low, east, last = shifted_backward(
        row_start, third, right, below, corner, qkv1, w_qkv, w_proj, head_scale, total_rows
    )
    above = neighbour(low, 1, 0)
    west = neighbour(east, 0, 1)
    last = neighbour(last, 1, 1)
    return last_block(
        third, dz, above, west, last, h1, h0, hm, qkv0, gp0, w_embed, norm_gain, w_qkv, w_proj,
        head_scale, w_up, w_down, partial.reshape(state.shape),
    )


def solution(mesh):
    placed = (
        P("lat", "lon", None),
        P("lat", "lon", None),
        P(),
        P(),
        P(),
        P(),
        P(),
        P(),
        P(),
        P(),
        P(),
        P(),
        P(),
        P(),
        P(("lat", "lon"), None),
        P(("lat", "lon"), None),
        P(("lat", "lon")),
        P(("lat", "lon")),
    )

    return jax.shard_map(
        local, mesh=mesh, in_specs=placed, out_specs=P("lat", "lon", None), check_vma=False
    )
```
